32 devices in a mesh: groups: 2 (over x), rows: 16 (over z, y, core).
Axes of the slice: x: 2, y: 2, z: 4, core: 2. Of those that a mesh axis runs over, the one named last changes fastest.
Arguments:
- phase: float32 [512, 2048], P(('groups', 'rows')), parts along dimension 0, may hold values from -3.140625 to 3.140625
Outputs:
- filtered: float32 [2, 512, 2048], P(None, ('groups', 'rows')), parts along dimension 1
- profile: float32 [6, 16], P('groups'), parts along dimension 0
The draws below stay inside these ranges and needn't reach their ends.
There are 2 independent parts, one for each index of `groups`. The reference program is written for one: setup_inputs(seed, part) draws one part's arguments, and reference() takes and returns one part's arrays. A program takes and returns all parts, laid end to end along the dimension named above; each array names one. Nothing has to cross between parts.
All inputs are finite; a program needn't handle non-finite values.
Results may differ from the reference program's by a relative error of at most 0.00012.
Values sent between devices are 32-bit elements; how exact they have to be, the bound alone decides.
No kernel may reach another device: no remote copies, remote signals or barrier semaphores. Data moves between devices by JAX's collectives and lax.ppermute only.
A program may use at most 64 MiB of HBM per device.

```python
import jax
import jax.numpy as jnp
from jax import lax

COLS = 2048
ITERS = 3
NR = 256


def setup_inputs(seed: int = 0, part: int = 0) -> dict:
    streams_of = jax.random.split(jax.random.key(seed), 2)
    part_splits = jax.random.split(jax.random.fold_in(streams_of[1], part), 2)
    phase = jnp.clip(jax.random.uniform(part_splits[0], (NR, COLS), jnp.float32, -3.140625, 3.140625), -3.140625, 3.140625)
    return {"phase": phase}


EPS = 1e-6


def residue_sums(padded_rows):
    padded = jnp.pad(padded_rows, ((0, 0), (0, 0), (0, 1)))
    first = padded[:, :-1, :-1]
    second = padded[:, :-1, 1:]
    third = padded[:, 1:, 1:]
    fourth = padded[:, 1:, :-1]

    def cross(left, right):
        return left[1] * right[0] - left[0] * right[1]

    loop = cross(first, second) + cross(second, third) + cross(third, fourth) + cross(fourth, first)
    height = loop.shape[0]
    return jnp.sum((loop * loop).reshape(height, COLS // 128, 128), axis=(0, 2))


def goldstein(field, taper):
    extended = jnp.pad(field, ((0, 0), (0, 16), (0, 16)))
    blocks = extended.reshape(2, NR // 16 + 1, 16, COLS // 16 + 1, 16)

    def one_row(start):
        strip = lax.dynamic_slice_in_dim(blocks, start, 2, 1).reshape(2, 32, COLS // 16 + 1, 16)
        windows = jnp.concatenate([strip[:, :, :-1], strip[:, :, 1:]], axis=3)
        signal = windows[0] + 1j * windows[1]
        spectrum = jnp.fft.fft2(signal, axes=(0, 2))
        power = spectrum.real ** 2 + spectrum.imag ** 2
        average = jnp.mean(power, axis=(0, 2), keepdims=True)
        result = jnp.fft.ifft2(spectrum * (power / (average + EPS)) ** 0.25, axes=(0, 2)) * taper
        return jnp.stack([result.real, result.imag])

    pieces = lax.map(one_row, jnp.arange(NR // 16, dtype=jnp.int32))
    righty = jnp.pad(pieces[..., 16:], ((0, 0), (0, 0), (0, 0), (1, 0), (0, 0)))[:, :, :, :-1]
    columns = (pieces[..., :16] + righty).reshape(NR // 16, 2, 32, COLS)
    lower = jnp.pad(columns[:, :, 16:], ((1, 0), (0, 0), (0, 0), (0, 0)))[:-1]
    joined = columns[:, :, :16] + lower
    return joined.transpose(1, 0, 2, 3).reshape(2, NR, COLS)


def reference(phase):
    field = jnp.stack([jnp.cos(phase), jnp.sin(phase)])
    offsets = jnp.arange(32, dtype=jnp.float32)
    ramp = 1.0 - jnp.abs(offsets - 15.5) / 16.0
    taper = ramp[:, None, None] * ramp[None, None, :]
    reports = []
    for step in range(ITERS):
        padded_rows = jnp.pad(field, ((0, 0), (0, 1), (0, 0)))
        reports.append(residue_sums(padded_rows) / (NR * 128.0))
        field = goldstein(field, taper)
    return field, jnp.stack(reports)
```

```python
import functools
import math

import jax
import jax.numpy as jnp
from jax import lax
from jax.experimental import pallas as pl
from jax.experimental.pallas import tpu as pltpu
from jax.sharding import PartitionSpec as P

ITERS = 3
EPS = 1e-06
LANES = 128
HALO = 3

SIN = (1.000000000e+00, -1.666666662e-01, 8.333330977e-03, -1.984086143e-04, 2.752528078e-06, -2.388938418e-08)
COS = (9.999999998e-01, -4.999999936e-01, 4.166663620e-02, -1.388836069e-03, 2.476012736e-05, -2.605092951e-07)


def rotated(value, k, size, sign):
    re, im = value
    half = math.sqrt(0.5)
    if k == 0:
        return re, im
    if 4 * k == size:
        return (im, -re) if sign < 0 else (-im, re)
    if 8 * k == size:
        return ((re + im) * half, (im - re) * half) if sign < 0 else ((re - im) * half, (im + re) * half)
    if 8 * k == 3 * size:
        return ((im - re) * half, (re + im) * -half) if sign < 0 else ((re + im) * -half, (re - im) * half)
    c = math.cos(2 * math.pi * k / size)
    s = sign * math.sin(2 * math.pi * k / size)
    return re * c - im * s, im * c + re * s


def plus(a, b):
    return a[0] + b[0], a[1] + b[1]


def minus(a, b):
    return a[0] - b[0], a[1] - b[1]


def fft(values, sign):
    size = len(values)
    if size == 1:
        return values
    even = fft(values[0::2], sign)
    odd = fft(values[1::2], sign)
    turned = [rotated(odd[k], k, size, sign) for k in range(size // 2)]
    return [plus(e, o) for e, o in zip(even, turned)] + [minus(e, o) for e, o in zip(even, turned)]


def polynomial(coefficients, w):
    result = jnp.full_like(w, coefficients[-1])
    for c in coefficients[-2::-1]:
        result = result * w + c
    return result


def cos_sin(x):
    u = (jnp.abs(x) - jnp.float32(math.pi / 2)) + jnp.float32(4.371139e-08)
    w = u * u
    cosine = -(u * polynomial(SIN, w))
    sine = polynomial(COS, w)
    return cosine, jnp.where(x < 0, -sine, sine)


def swap_bits(values, lane):
    values = list(values)
    bit = 1
    while bit < len(values):
        clear = (lane & bit) == 0
        for p in range(len(values)):
            if p & bit == 0:
                low, high = values[p], values[p | bit]
                values[p] = jnp.where(clear, low, pltpu.roll(high, bit, 1))
                values[p | bit] = jnp.where(clear, pltpu.roll(low, LANES - bit, 1), high)
        bit *= 2
    return values


def ramp(t):
    return 1.0 - abs(t - 15.5) / 16.0


def filter_kernel(slabs, blocks, tiles, packed, in_ref, out_ref, zr, zi, yr, yi, wr, wi, gain):
    tile = lax.axis_index("rows")
    per_tile = LANES // slabs
    lane = lax.broadcasted_iota(jnp.int32, (8, LANES), 1)
    sub = lax.broadcasted_iota(jnp.int32, (8, LANES), 0)
    slab = lane % slabs
    not_last = slab != slabs - 1
    not_first = slab != 0
    place = lane // slabs

    def inside(h, step):
        position = (h * per_tile + place + step) % (tiles * per_tile)
        relative = jnp.where(position < blocks + HALO, position, position - tiles * per_tile)
        column = tile * blocks + relative
        return jnp.where((column >= 0) & (column < slabs * blocks), 1.0, 0.0)

    here = [inside(h, 0) for h in range(tiles)]
    both = [here[h] * inside(h, 1) for h in range(tiles)]

    def right(values):
        if per_tile == 1:
            return [values[(h + 1) % tiles] for h in range(tiles)]
        moved = [pltpu.roll(v, LANES - slabs, 1) for v in values]
        return [jnp.where(lane < LANES - slabs, moved[h], moved[(h + 1) % tiles]) for h in range(tiles)]

    def left(values):
        if per_tile == 1:
            return [values[h - 1] for h in range(tiles)]
        moved = [pltpu.roll(v, slabs, 1) for v in values]
        return [jnp.where(lane < slabs, moved[h - 1], moved[h]) for h in range(tiles)]

    def below(value):
        return jnp.where(not_last, pltpu.roll(value, LANES - 1, 1), 0.0)

    def above(value):
        return jnp.where(not_first, pltpu.roll(value, 1, 1), 0.0)

    for h in range(tiles):
        for g in range(2):
            if packed:
                phases = swap_bits([in_ref[a, h * 16 + g * 8 : h * 16 + g * 8 + 8, :] for a in range(16)], lane)
            else:
                phases = [in_ref[h, s, g * 8 : g * 8 + 8, :] for s in range(16)]
            for s in range(16):
                cosine, sine = cos_sin(phases[s])
                zr[h * 16 + s, g * 8 : g * 8 + 8, :] = cosine * here[h]
                zi[h * 16 + s, g * 8 : g * 8 + 8, :] = sine * here[h]

    def measure_z():
        total = jnp.zeros((8, LANES), jnp.float32)
        energy = [jnp.zeros((8, LANES), jnp.float32) for _ in range(tiles)]
        for h in range(1, tiles):
            for s in range(16):
                for g in range(2):
                    re = zr[h * 16 + s, g * 8 : g * 8 + 8, :]
                    im = zi[h * 16 + s, g * 8 : g * 8 + 8, :]
                    energy[h] = energy[h] + (re * re + im * im)

        def column(s, shifted):
            halves = []
            for ref in (zr, zi):
                top = ref[s, 0:8, :]
                low = ref[s, 8:16, :]
                if shifted:
                    top = right([ref[h * 16, 0:8, :] for h in range(tiles)])[0]
                    low = right([ref[h * 16, 8:16, :] for h in range(tiles)])[0]
                turned = [pltpu.roll(v, 7, 0) for v in (top, low, below(top))]
                halves.append((top, low, jnp.where(sub < 7, turned[0], turned[1]), jnp.where(sub < 7, turned[1], turned[2])))
            (r0, r1, r0d, r1d), (i0, i1, i0d, i1d) = halves
            vertical = (i0 * r0d - r0 * i0d, i1 * r1d - r1 * i1d)
            return (r0, i0, r0d, i0d), (r1, i1, r1d, i1d), vertical

        current = column(0, False)
        for s in range(16):
            following = column(s + 1, False) if s < 15 else column(0, True)
            for g in range(2):
                r, i, rd, idn = current[g]
                rn, in_, rdn, idnn = following[g]
                energy[0] = energy[0] + (r * r + i * i)
                across = i * rn - r * in_
                across_down = idn * rdn - rd * idnn
                loop = (across - across_down) + (following[2][g] - current[2][g])
                total = total + loop * loop
            current = following
        summed = [jnp.broadcast_to(jnp.sum(e, axis=0, keepdims=True), (8, LANES)) for e in energy]
        tall = [e + below(e) for e in summed]
        wide = right(tall)
        for h in range(tiles):
            gain[h * 8 : h * 8 + 8, :] = 1.0 / ((tall[h] + wide[h]) + EPS)
        return jnp.sum(total)

    def forward_columns(g):
        rows = pl.ds(pl.multiple_of(g * 8, 8), 8)
        first = [[None] * 16 for _ in range(tiles)]
        second = [[None] * 16 for _ in range(tiles)]
        for s in range(16):
            re = [zr[h * 16 + s, rows, :] for h in range(tiles)]
            im = [zi[h * 16 + s, rows, :] for h in range(tiles)]
            for h, (a, b) in enumerate(zip(right(re), right(im))):
                first[h][s] = (re[h], im[h])
                second[h][s] = (a, b)
        for h in range(tiles):
            sums = [plus(a, b) for a, b in zip(first[h], second[h])]
            differences = [rotated(minus(a, b), s, 32, -1) for s, (a, b) in enumerate(zip(first[h], second[h]))]
            for parity, half in enumerate((sums, differences)):
                for m, (re, im) in enumerate(fft(half, -1)):
                    at = pl.ds((h * 32 + 2 * m + parity) * 17 + g * 8, 8)
                    yr[at, :] = re
                    yi[at, :] = im

    def windows(unit):
        h = unit // 4
        q = unit % 4
        base = (h * 32 + q * 8) * 17
        scale = gain[pl.ds(pl.multiple_of(h * 8, 8), 8), :]
        first = []
        second = []
        for t in range(16):
            at = pl.ds(base + t, 8, stride=17)
            re = yr[at, :]
            im = yi[at, :]
            first.append((re, im))
            second.append((below(re), below(im)))
        sums = [plus(a, b) for a, b in zip(first, second)]
        differences = [rotated(minus(a, b), t, 32, -1) for t, (a, b) in enumerate(zip(first, second))]
        back = []
        for half in (sums, differences):
            filtered = []
            for re, im in fft(half, -1):
                power = (re * re + im * im) * scale
                factor = lax.rsqrt(lax.rsqrt(power))
                filtered.append((re * factor, im * factor))
            back.append(fft(filtered, 1))
        for t in range(16):
            even = back[0][t]
            odd = rotated(back[1][t], t, 32, 1)
            upper = plus(even, odd)
            lower = minus(even, odd)
            at = pl.ds((h * 16 + t) * 33 + q * 8, 8)
            wr[at, :] = upper[0] * (ramp(t) / 32) + above(lower[0] * (ramp(t + 16) / 32))
            wi[at, :] = upper[1] * (ramp(t) / 32) + above(lower[1] * (ramp(t + 16) / 32))

    def inverse_columns(g):
        rows = pl.ds(pl.multiple_of(g * 8, 8), 8)
        kept = []
        passed = []
        for h in range(tiles):
            back = []
            for parity in range(2):
                values = []
                for m in range(16):
                    at = pl.ds((h * 16 + g * 8) * 33 + 2 * m + parity, 8, stride=33)
                    values.append((wr[at, :], wi[at, :]))
                back.append(fft(values, 1))
            own = []
            other = []
            for s in range(16):
                odd = rotated(back[1][s], s, 32, 1)
                near = here[h] * (ramp(s) / 32)
                far = both[h] * (ramp(s + 16) / 32)
                a = plus(back[0][s], odd)
                b = minus(back[0][s], odd)
                own.append((a[0] * near, a[1] * near))
                other.append((b[0] * far, b[1] * far))
            kept.append(own)
            passed.append(other)
        for s in range(16):
            for part, ref in enumerate((zr, zi)):
                arrived = left([passed[h][s][part] for h in range(tiles)])
                for h in range(tiles):
                    ref[h * 16 + s, rows, :] = kept[h][s][part] + arrived[h]

    def run(count, body):
        lax.fori_loop(0, count, lambda i, c: (body(i), c)[1], 0)

    def iteration(step, carry):
        total = measure_z()
        out_ref_row(step, total)
        run(2, forward_columns)
        run(4 * tiles, windows)
        run(2, inverse_columns)
        return carry

    if packed:

        def out_ref_row(step, total):
            for a in range(16):
                out_ref[a, pl.ds(32 + step, 1), :] = jnp.full((1, LANES), total)

    else:

        def out_ref_row(step, total):
            out_ref[32, pl.ds(step, 1), :] = jnp.full((1, LANES), total)

    lax.fori_loop(0, ITERS, iteration, 0)

    for part, ref in enumerate((zr, zi)):
        for g in range(2):
            values = [ref[s, g * 8 : g * 8 + 8, :] for s in range(16)]
            if packed:
                for a, value in enumerate(swap_bits(values, lane)):
                    out_ref[a, part * 16 + g * 8 : part * 16 + g * 8 + 8, :] = value
            else:
                for s, value in enumerate(values):
                    out_ref[part * 16 + s, g * 8 : g * 8 + 8, :] = value


def filter_tiles(slabs, blocks, tiles, packed, data):
    shape = (16, 40, LANES) if packed else (33, 16, LANES)
    body = functools.partial(filter_kernel, slabs, blocks, tiles, packed)
    return pl.pallas_call(
        body,
        out_shape=jax.ShapeDtypeStruct(shape, jnp.float32),
        in_specs=[pl.BlockSpec(memory_space=pltpu.VMEM)],
        out_specs=pl.BlockSpec(memory_space=pltpu.VMEM),
        scratch_shapes=[pltpu.VMEM((tiles * 16, 16, LANES), jnp.float32)] * 2
        + [pltpu.VMEM((tiles * 32 * 17 + 8, LANES), jnp.float32)] * 2
        + [pltpu.VMEM((tiles * 16 * 33 + 8, LANES), jnp.float32)] * 2
        + [pltpu.VMEM((tiles * 8, LANES), jnp.float32)],
        name="filter_tiles",
    )(data)


def ring_of_blocks(phase, devices, blocks, tiles):
    per_tile = LANES // devices
    ring = tiles * per_tile
    width = phase.shape[1]
    padded = jnp.pad(phase, ((0, 0), (HALO * 16, (ring + HALO) * 16)))
    pieces = []
    for d in range(devices):
        start = d * blocks * 16
        ahead = padded[:, start + HALO * 16 : start + (blocks + 2 * HALO) * 16]
        behind = padded[:, start : start + HALO * 16]
        gap = jnp.zeros((16, (ring - blocks - 2 * HALO) * 16), phase.dtype)
        pieces.append(jnp.concatenate([ahead, gap, behind], axis=1))
    return jnp.stack(pieces)


def per_device(phase):
    devices = lax.axis_size("rows")
    height, width = phase.shape
    blocks = width // (16 * devices)
    per_tile = LANES // devices
    if height != 16 or LANES % devices or blocks * 16 * devices != width or blocks != per_tile:
        raise ValueError("unsupported sizes")
    scale = 1.0 / (height * devices * 128.0)
    if devices == 16:
        tiles = 2
        columns = phase.reshape(16, devices, LANES).transpose(1, 0, 2)
        empty = jnp.zeros((1, 16, LANES), phase.dtype)
        after = jnp.concatenate([columns[1:], empty])
        before = jnp.concatenate([empty, columns[:-1]])
        lane = lax.broadcasted_iota(jnp.int32, columns.shape, 2)
        data = jnp.concatenate([columns, jnp.where(lane < LANES // 2, after, before)], axis=1)
        data = lax.all_to_all(data, "rows", 0, 0)
        result = filter_tiles(devices, blocks, tiles, True, data)
        result = lax.all_to_all(result, "rows", 0, 0)
        field = result[:, :32].reshape(devices, 2, 16, LANES).transpose(1, 2, 0, 3).reshape(2, 16, width)
        profile = result[:, 32 : 32 + ITERS, 0].T
        return field, profile * scale
    tiles = -(-(blocks + 2 * HALO) // per_tile)
    data = lax.all_to_all(ring_of_blocks(phase, devices, blocks, tiles), "rows", 0, 0)
    data = data.reshape(devices, 16, tiles, per_tile, 16).transpose(2, 4, 1, 3, 0)
    result = filter_tiles(devices, blocks, tiles, False, data.reshape(tiles, 16, 16, LANES))
    field = result[:32].reshape(2, 16, 16, per_tile, devices).transpose(4, 0, 2, 3, 1)
    field = field.reshape(devices, 32, per_tile * 16)
    sums = jnp.broadcast_to(result[32, :ITERS, : per_tile * 16][None], (devices, ITERS, per_tile * 16))
    result = lax.all_to_all(jnp.concatenate([field, sums], axis=1), "rows", 0, 0)
    field = result[:, :32].reshape(devices, 2, 16, per_tile * 16).transpose(1, 2, 0, 3).reshape(2, 16, width)
    profile = result[:, 32:, 0].reshape(width // 128, -1, ITERS).sum(1).T
    return field, profile * scale


def solution(mesh):
    return jax.shard_map(
        per_device,
        mesh=mesh,
        in_specs=(P(("groups", "rows"), None),),
        out_specs=(P(None, ("groups", "rows"), None), P("groups", None)),
        check_vma=False,
    )
```

```python
import functools
import math

import jax
import jax.numpy as jnp
from jax import lax
from jax.experimental import pallas as pl
from jax.experimental.pallas import tpu as pltpu
from jax.sharding import PartitionSpec as P

ITERS = 3
EPS = 1e-06
LANES = 128
HALO = 3

SIN = (1.000000000e+00, -1.666666662e-01, 8.333330977e-03, -1.984086143e-04, 2.752528078e-06, -2.388938418e-08)
COS = (9.999999998e-01, -4.999999936e-01, 4.166663620e-02, -1.388836069e-03, 2.476012736e-05, -2.605092951e-07)


def rotated(value, k, size, sign):
    re, im = value
    half = math.sqrt(0.5)
    if k == 0:
        return re, im
    if 4 * k == size:
        return (im, -re) if sign < 0 else (-im, re)
    if 8 * k == size:
        return ((re + im) * half, (im - re) * half) if sign < 0 else ((re - im) * half, (im + re) * half)
    if 8 * k == 3 * size:
        return ((im - re) * half, (re + im) * -half) if sign < 0 else ((re + im) * -half, (re - im) * half)
    c = math.cos(2 * math.pi * k / size)
    s = sign * math.sin(2 * math.pi * k / size)
    return re * c - im * s, im * c + re * s


def plus(a, b):
    return a[0] + b[0], a[1] + b[1]


def minus(a, b):
    return a[0] - b[0], a[1] - b[1]


def fft(values, sign):
    size = len(values)
    if size == 1:
        return values
    even = fft(values[0::2], sign)
    odd = fft(values[1::2], sign)
    turned = [rotated(odd[k], k, size, sign) for k in range(size // 2)]
    return [plus(e, o) for e, o in zip(even, turned)] + [minus(e, o) for e, o in zip(even, turned)]


def polynomial(coefficients, w):
    result = jnp.full_like(w, coefficients[-1])
    for c in coefficients[-2::-1]:
        result = result * w + c
    return result


def cos_sin(x):
    u = (jnp.abs(x) - jnp.float32(math.pi / 2)) + jnp.float32(4.371139e-08)
    w = u * u
    cosine = -(u * polynomial(SIN, w))
    sine = polynomial(COS, w)
    return cosine, jnp.where(x < 0, -sine, sine)


def swap_bits(values, lane):
    values = list(values)
    bit = 1
    while bit < len(values):
        clear = (lane & bit) == 0
        for p in range(len(values)):
            if p & bit == 0:
                low, high = values[p], values[p | bit]
                values[p] = jnp.where(clear, low, pltpu.roll(high, bit, 1))
                values[p | bit] = jnp.where(clear, pltpu.roll(low, LANES - bit, 1), high)
        bit *= 2
    return values


def ramp(t):
    return 1.0 - abs(t - 15.5) / 16.0


def filter_kernel(slabs, blocks, tiles, packed, in_ref, out_ref, zr, zi, ur, ui, vr, vi, pr, pi, qr, qi, gain, turn):
    tile = lax.axis_index("rows")
    per_tile = LANES // slabs
    ring = tiles * per_tile
    lane = lax.broadcasted_iota(jnp.int32, (8, LANES), 1)
    sub = lax.broadcasted_iota(jnp.int32, (8, LANES), 0)
    not_last = lane % slabs != slabs - 1
    not_first = lane % slabs != 0
    place = lane // slabs

    def inside(h, step):
        position = (h * per_tile + place + step) % ring
        relative = jnp.where(position < blocks + HALO, position, position - ring)
        column = tile * blocks + relative
        return jnp.where((column >= 0) & (column < slabs * blocks), 1.0, 0.0)

    here = [inside(h, 0) for h in range(tiles)]
    both = [here[h] * inside(h, 1) for h in range(tiles)]

    def right(values, active):
        if per_tile == 1:
            return [values[(h + 1) % tiles] for h in active]
        moved = [pltpu.roll(v, LANES - slabs, 1) for v in values]
        return [jnp.where(lane < LANES - slabs, moved[h], moved[(h + 1) % tiles]) for h in active]

    def left(values):
        if per_tile == 1:
            return [values[h - 1] for h in range(tiles)]
        moved = [pltpu.roll(v, slabs, 1) for v in values]
        return [jnp.where(lane < slabs, moved[h - 1], moved[h]) for h in range(tiles)]

    def below(value):
        return jnp.where(not_last, pltpu.roll(value, LANES - 1, 1), 0.0)

    def above(value):
        return jnp.where(not_first, pltpu.roll(value, 1, 1), 0.0)

    for h in range(tiles):
        for g in range(2):
            if packed:
                phases = swap_bits([in_ref[a, h * 16 + g * 8 : h * 16 + g * 8 + 8, :] for a in range(16)], lane)
            else:
                phases = [in_ref[h, s, g * 8 : g * 8 + 8, :] for s in range(16)]
            for s in range(16):
                cosine, sine = cos_sin(phases[s])
                zr[h * 16 + s, g * 8 : g * 8 + 8, :] = cosine * here[h]
                zi[h * 16 + s, g * 8 : g * 8 + 8, :] = sine * here[h]

    def measure_z(active):
        total = jnp.zeros((8, LANES), jnp.float32)
        energy = [jnp.zeros((8, LANES), jnp.float32) for _ in range(tiles)]
        for h in range(1, tiles):
            for s in range(16):
                for g in range(2):
                    re = zr[h * 16 + s, g * 8 : g * 8 + 8, :]
                    im = zi[h * 16 + s, g * 8 : g * 8 + 8, :]
                    energy[h] = energy[h] + (re * re + im * im)

        def column(s):
            halves = []
            for ref in (zr, zi):
                if s < 16:
                    top = ref[s, 0:8, :]
                    low = ref[s, 8:16, :]
                else:
                    top = right([ref[h * 16, 0:8, :] for h in range(tiles)], (0,))[0]
                    low = right([ref[h * 16, 8:16, :] for h in range(tiles)], (0,))[0]
                moved = [pltpu.roll(v, 7, 0) for v in (top, low, below(top))]
                halves.append((top, low, jnp.where(sub < 7, moved[0], moved[1]), jnp.where(sub < 7, moved[1], moved[2])))
            (r0, r1, r0d, r1d), (i0, i1, i0d, i1d) = halves
            vertical = (i0 * r0d - r0 * i0d, i1 * r1d - r1 * i1d)
            return (r0, i0, r0d, i0d), (r1, i1, r1d, i1d), vertical

        current = column(0)
        for s in range(16):
            following = column(s + 1)
            for g in range(2):
                r, i, rd, idn = current[g]
                rn, in_, rdn, idnn = following[g]
                energy[0] = energy[0] + (r * r + i * i)
                across = i * rn - r * in_
                across_down = idn * rdn - rd * idnn
                loop = (across - across_down) + (following[2][g] - current[2][g])
                total = total + loop * loop
            current = following
        summed = [jnp.broadcast_to(jnp.sum(e, axis=0, keepdims=True), (8, LANES)) for e in energy]
        tall = [e + below(e) for e in summed]
        wide = right(tall, active)
        return jnp.sum(total), [1.0 / ((tall[h] + w) + EPS) for h, w in zip(active, wide)]

    def sharing(h, needed):
        places = {w % ring - h * per_tile for w in needed}
        places = {p for p in places if 0 <= p < per_tile}
        group = 1
        for k in (2, 4):
            if per_tile % k == 0:
                taken = {(p + j * (per_tile // k)) % per_tile for p in places for j in range(k)}
                group = k if len(taken) == k * len(places) else group
        masks = []
        for k in range(1, group):
            mask = place < 0
            for p in places:
                mask = mask | (place == (p + k * (per_tile // group)) % per_tile)
            masks.append(mask)
        return masks

    def merged(values, masks):
        result = values[0]
        for k, mask in enumerate(masks):
            result = jnp.where(mask, pltpu.roll(values[k + 1], (k + 1) * LANES // (len(masks) + 1), 1), result)
        return result

    def forward_columns(plans, g):
        rows = pl.ds(pl.multiple_of(g * 8, 8), 8)
        active = [h for h, _ in plans]
        near = {h: [] for h in active}
        far = {h: [] for h in active}
        for s in range(16):
            re = [zr[h * 16 + s, rows, :] for h in range(tiles)]
            im = [zi[h * 16 + s, rows, :] for h in range(tiles)]
            for h, a, b in zip(active, right(re, active), right(im, active)):
                near[h].append((re[h], im[h]))
                far[h].append((a, b))
        for h, masks in plans:
            group = len(masks) + 1
            even = fft([plus(a, b) for a, b in zip(near[h], far[h])], -1)
            odd = fft([rotated(minus(a, b), s, 32, -1) for s, (a, b) in enumerate(zip(near[h], far[h]))], -1)
            for row in range(32 // group):
                sources = [(row // 8 * group + k) * 8 + row % 8 for k in range(group)]
                values = [(even, odd)[l % 2][l // 2] for l in sources]
                value = tuple(merged([v[part] for v in values], masks) for part in range(2))
                following = (below(value[0]), below(value[1]))
                at = pl.ds((h * 32 + row) * 17 + g * 8, 8)
                ur[at, :], ui[at, :] = plus(value, following)
                vr[at, :], vi[at, :] = minus(value, following)

    def windows(h, unit):
        scale = gain[h * 8 : h * 8 + 8, :]
        at = [pl.ds((h * 32 + unit * 8) * 17 + t, 8, stride=17) for t in range(16)]
        back = []
        for parity, (a, b) in enumerate(((ur, ui), (vr, vi))):
            values = [(a[x, :], b[x, :]) for x in at]
            if parity:
                values = [rotated(v, t, 32, -1) for t, v in enumerate(values)]
            filtered = []
            for re, im in fft(values, -1):
                factor = lax.rsqrt(lax.rsqrt((re * re + im * im) * scale))
                filtered.append((re * factor, im * factor))
            back.append(fft(filtered, 1))
        for t in range(16):
            odd = rotated(back[1][t], t, 32, 1)
            upper = plus(back[0][t], odd)
            lower = minus(back[0][t], odd)
            at = pl.ds((h * 16 + t) * 33 + unit * 8, 8)
            pr[at, :], pi[at, :] = (v * (ramp(t) / 32) for v in upper)
            qr[at, :], qi[at, :] = (v * (ramp(t + 16) / 32) for v in lower)

    def inverse_columns(plans, g):
        rows = pl.ds(pl.multiple_of(g * 8, 8), 8)
        kept = []
        passed = []
        for h, masks in plans:
            group = len(masks) + 1
            values = [None] * 32
            for row in range(32 // group):
                at = pl.ds((h * 16 + g * 8) * 33 + row, 8, stride=33)
                value = (pr[at, :] + above(qr[at, :]), pi[at, :] + above(qi[at, :]))
                for k in range(group):
                    l = (row // 8 * group + k) * 8 + row % 8
                    values[l] = tuple(pltpu.roll(v, LANES - k * LANES // group, 1) if k else v for v in value)
            even = fft(values[0::2], 1)
            odd = fft(values[1::2], 1)
            own = []
            other = []
            for s in range(16):
                turned = rotated(odd[s], s, 32, 1)
                weight = here[h] * (ramp(s) / 32)
                own.append(tuple(v * weight for v in plus(even[s], turned)))
                weight = both[h] * (ramp(s + 16) / 32)
                other.append(tuple(v * weight for v in minus(even[s], turned)))
            kept.append(own)
            passed.append(other)
        for s in range(16):
            for part, ref in enumerate((zr, zi)):
                if len(plans) == tiles:
                    arrived = left([passed[h][s][part] for h in range(tiles)])
                    for h in range(tiles):
                        ref[h * 16 + s, rows, :] = kept[h][s][part] + arrived[h]
                else:
                    ref[s, rows, :] = kept[0][s][part]
                    ref[16 + s, rows, :] = pltpu.roll(passed[0][s][part], slabs, 1)

    def run(count, body):
        lax.fori_loop(0, count, lambda i, c: (body(i), c)[1], 0)

    totals = []
    for step in range(ITERS):
        before = ITERS - step - (1 if packed else 0)
        needed = range(-before, blocks + ITERS - 1 - step)
        active = range(1 if packed and step == ITERS - 1 else tiles)
        plans = [(h, sharing(h, needed)) for h in active]
        total, gains = measure_z(active)
        totals.append(total)
        for (h, masks), value in zip(plans, gains):
            gain[h * 8 : h * 8 + 8, :] = merged([value] * 4, masks)
        run(2, functools.partial(forward_columns, plans))
        for h, masks in plans:
            run(4 // (len(masks) + 1), functools.partial(windows, h))
        run(2, functools.partial(inverse_columns, plans))

    if not packed:
        for step, total in enumerate(totals):
            out_ref[32, step : step + 1, :] = jnp.full((1, LANES), total)
        for part, ref in enumerate((zr, zi)):
            for s in range(16):
                out_ref[part * 16 + s, :, :] = ref[s, :, :]
        return

    spill = []
    for part, ref in enumerate((zr, zi)):
        for g in range(2):
            own = [ref[s, g * 8 : g * 8 + 8, :] for s in range(16)]
            other = [ref[16 + s, g * 8 : g * 8 + 8, :] for s in range(16)]
            values = [a + jnp.where(place > 0, b, 0.0) for a, b in zip(own, other)]
            for a, value in enumerate(swap_bits(values, lane)):
                out_ref[a, part * 16 + g * 8 : part * 16 + g * 8 + 8, :] = value
            for q in range(2):
                pack = other[8 * q]
                for j in range(1, 8):
                    pack = jnp.where(place == j, pltpu.roll(other[8 * q + j], j * slabs, 1), pack)
                spill.append(pack)
    turned = jnp.concatenate(spill + spill, axis=0).T
    for j in range(8):
        turn[j * 17 : j * 17 + 16, :] = turned[j * 16 : j * 16 + 16, :]
    sums = jnp.zeros((8, LANES), jnp.float32)
    for step, total in enumerate(totals):
        sums = jnp.where((sub == step) & (lane == 64 + tile), total, sums)
    for a in range(16):
        out_ref[a, 32:40, :] = jnp.where(lane < 64, turn[pl.ds(a, 8, stride=17), :], sums)


def filter_tiles(slabs, blocks, tiles, packed, data):
    shape = (16, 40, LANES) if packed else (33, 16, LANES)
    body = functools.partial(filter_kernel, slabs, blocks, tiles, packed)
    return pl.pallas_call(
        body,
        out_shape=jax.ShapeDtypeStruct(shape, jnp.float32),
        in_specs=[pl.BlockSpec(memory_space=pltpu.VMEM)],
        out_specs=pl.BlockSpec(memory_space=pltpu.VMEM),
        scratch_shapes=[pltpu.VMEM((tiles * 16, 16, LANES), jnp.float32)] * 2
        + [pltpu.VMEM((tiles * 32 * 17 + 8, LANES), jnp.float32)] * 4
        + [pltpu.VMEM((tiles * 16 * 33 + 8, LANES), jnp.float32)] * 4
        + [pltpu.VMEM((tiles * 8, LANES), jnp.float32), pltpu.VMEM((136, LANES), jnp.float32)],
        compiler_params=pltpu.CompilerParams(vmem_limit_bytes=16 << 20),
        name="filter_tiles",
    )(data)


def finish_kernel(scale, in_ref, field_ref, profile_ref):
    lane = lax.broadcasted_iota(jnp.int32, (8, LANES), 1)
    extras = [in_ref[c, 32:40, :] for c in range(16)]
    sums = functools.reduce(jnp.add, extras)
    profile_ref[...] = pltpu.roll(sums, 64, 1)[:ITERS, :16] * scale
    turned = jnp.concatenate(extras, axis=0).T
    low = (lane & 8) == 0
    for part in range(2):
        for g in range(2):
            first = (part * 2 + g) * 16
            a = turned[first : first + 8]
            b = turned[first + 8 : first + 16]
            pairs = (jnp.where(low, a, pltpu.roll(b, 8, 1)), jnp.where(low, pltpu.roll(a, LANES - 8, 1), b))
            for c in range(16):
                value = in_ref[c, part * 16 + g * 8 : part * 16 + g * 8 + 8, :]
                if c:
                    spill = pltpu.roll(pairs[(c - 1) % 2], (LANES - (c - 1) // 2 * 16) % LANES, 1)
                    value = value + jnp.where(lane < 16, spill, 0.0)
                field_ref[part, g * 8 : g * 8 + 8, c * LANES : (c + 1) * LANES] = value


def finish(scale, data):
    return pl.pallas_call(
        functools.partial(finish_kernel, scale),
        out_shape=(
            jax.ShapeDtypeStruct((2, 16, 16 * LANES), jnp.float32),
            jax.ShapeDtypeStruct((ITERS, 16), jnp.float32),
        ),
        in_specs=[pl.BlockSpec(memory_space=pltpu.VMEM)],
        out_specs=[pl.BlockSpec(memory_space=pltpu.VMEM)] * 2,
        compiler_params=pltpu.CompilerParams(vmem_limit_bytes=8 << 20),
        name="finish",
    )(data)


def ring_of_blocks(phase, devices, blocks, tiles):
    per_tile = LANES // devices
    ring = tiles * per_tile
    width = phase.shape[1]
    padded = jnp.pad(phase, ((0, 0), (HALO * 16, (ring + HALO) * 16)))
    pieces = []
    for d in range(devices):
        start = d * blocks * 16
        ahead = padded[:, start + HALO * 16 : start + (blocks + 2 * HALO) * 16]
        behind = padded[:, start : start + HALO * 16]
        gap = jnp.zeros((16, (ring - blocks - 2 * HALO) * 16), phase.dtype)
        pieces.append(jnp.concatenate([ahead, gap, behind], axis=1))
    return jnp.stack(pieces)


def per_device(phase):
    devices = lax.axis_size("rows")
    height, width = phase.shape
    blocks = width // (16 * devices)
    per_tile = LANES // devices
    if height != 16 or LANES % devices or blocks * 16 * devices != width or blocks != per_tile:
        raise ValueError("unsupported sizes")
    scale = 1.0 / (height * devices * 128.0)
    if devices == 16:
        tiles = 2
        columns = phase.reshape(16, devices, LANES).transpose(1, 0, 2)
        empty = jnp.zeros((1, 16, LANES), phase.dtype)
        after = jnp.concatenate([columns[1:], empty])
        before = jnp.concatenate([empty, columns[:-1]])
        lane = lax.broadcasted_iota(jnp.int32, columns.shape, 2)
        data = jnp.concatenate([columns, jnp.where(lane < LANES // 2, after, before)], axis=1)
        data = lax.all_to_all(data, "rows", 0, 0)
        result = filter_tiles(devices, blocks, tiles, True, data)
        result = lax.all_to_all(result, "rows", 0, 0)
        return finish(scale, result)
    tiles = -(-(blocks + 2 * HALO) // per_tile)
    data = lax.all_to_all(ring_of_blocks(phase, devices, blocks, tiles), "rows", 0, 0)
    data = data.reshape(devices, 16, tiles, per_tile, 16).transpose(2, 4, 1, 3, 0)
    result = filter_tiles(devices, blocks, tiles, False, data.reshape(tiles, 16, 16, LANES))
    field = result[:32].reshape(2, 16, 16, per_tile, devices).transpose(4, 0, 2, 3, 1)
    field = field.reshape(devices, 32, per_tile * 16)
    sums = jnp.broadcast_to(result[32, :ITERS, : per_tile * 16][None], (devices, ITERS, per_tile * 16))
    result = lax.all_to_all(jnp.concatenate([field, sums], axis=1), "rows", 0, 0)
    field = result[:, :32].reshape(devices, 2, 16, per_tile * 16).transpose(1, 2, 0, 3).reshape(2, 16, width)
    profile = result[:, 32:, 0].reshape(width // 128, -1, ITERS).sum(1).T
    return field, profile * scale


def solution(mesh):
    return jax.shard_map(
        per_device,
        mesh=mesh,
        in_specs=(P(("groups", "rows"), None),),
        out_specs=(P(None, ("groups", "rows"), None), P("groups", None)),
        check_vma=False,
    )
```

```python
import functools
import math

import jax
import jax.numpy as jnp
from jax import lax
from jax.experimental import pallas as pl
from jax.experimental.pallas import tpu as pltpu
from jax.sharding import PartitionSpec as P

ITERS = 3
EPS = 1e-06
LANES = 128
HALO = 3

SIN = (1.000000000e+00, -1.666666662e-01, 8.333330977e-03, -1.984086143e-04, 2.752528078e-06, -2.388938418e-08)
COS = (9.999999998e-01, -4.999999936e-01, 4.166663620e-02, -1.388836069e-03, 2.476012736e-05, -2.605092951e-07)


def rotated(value, k, size, sign):
    re, im = value
    half = math.sqrt(0.5)
    if k == 0:
        return re, im
    if 4 * k == size:
        return (im, -re) if sign < 0 else (-im, re)
    if 8 * k == size:
        return ((re + im) * half, (im - re) * half) if sign < 0 else ((re - im) * half, (im + re) * half)
    if 8 * k == 3 * size:
        return ((im - re) * half, (re + im) * -half) if sign < 0 else ((re + im) * -half, (re - im) * half)
    c = math.cos(2 * math.pi * k / size)
    s = sign * math.sin(2 * math.pi * k / size)
    return re * c - im * s, im * c + re * s


def plus(a, b):
    return a[0] + b[0], a[1] + b[1]


def minus(a, b):
    return a[0] - b[0], a[1] - b[1]


def fft(values, sign):
    size = len(values)
    if size == 1:
        return values
    even = fft(values[0::2], sign)
    odd = fft(values[1::2], sign)
    turned = [rotated(odd[k], k, size, sign) for k in range(size // 2)]
    return [plus(e, o) for e, o in zip(even, turned)] + [minus(e, o) for e, o in zip(even, turned)]


def polynomial(coefficients, w):
    result = jnp.full_like(w, coefficients[-1])
    for c in coefficients[-2::-1]:
        result = result * w + c
    return result


def cos_sin(x):
    u = (jnp.abs(x) - jnp.float32(math.pi / 2)) + jnp.float32(4.371139e-08)
    w = u * u
    cosine = -(u * polynomial(SIN, w))
    sine = polynomial(COS, w)
    return cosine, jnp.where(x < 0, -sine, sine)


def swap_bits(values, lane):
    values = list(values)
    bit = 1
    while bit < len(values):
        clear = (lane & bit) == 0
        for p in range(len(values)):
            if p & bit == 0:
                low, high = values[p], values[p | bit]
                values[p] = jnp.where(clear, low, pltpu.roll(high, bit, 1))
                values[p | bit] = jnp.where(clear, pltpu.roll(low, LANES - bit, 1), high)
        bit *= 2
    return values


def ramp(t):
    return 1.0 - abs(t - 15.5) / 16.0


def filter_kernel(
    slabs, blocks, tiles, packed, in_ref, out_ref, zr, zi, yr, yi, ur, ui, vr, vi, wr, wi, pr, pi, qr, qi, energy, gain, sums, turn
):
    tile = lax.axis_index("rows")
    per_tile = LANES // slabs
    ring = tiles * per_tile
    lane = lax.broadcasted_iota(jnp.int32, (8, LANES), 1)
    sub = lax.broadcasted_iota(jnp.int32, (8, LANES), 0)
    not_last = lane % slabs != slabs - 1
    not_first = lane % slabs != 0
    place = lane // slabs

    def inside(h, step):
        position = (h * per_tile + place + step) % ring
        relative = jnp.where(position < blocks + HALO, position, position - ring)
        column = tile * blocks + relative
        return jnp.where((column >= 0) & (column < slabs * blocks), 1.0, 0.0)

    here = [inside(h, 0) for h in range(tiles)]
    both = [here[h] * inside(h, 1) for h in range(tiles)]

    def right(values, active):
        if per_tile == 1:
            return [values[(h + 1) % tiles] for h in active]
        moved = [pltpu.roll(v, LANES - slabs, 1) for v in values]
        return [jnp.where(lane < LANES - slabs, moved[h], moved[(h + 1) % tiles]) for h in active]

    def left(values):
        if per_tile == 1:
            return [values[h - 1] for h in range(tiles)]
        moved = [pltpu.roll(v, slabs, 1) for v in values]
        return [jnp.where(lane < slabs, moved[h - 1], moved[h]) for h in range(tiles)]

    def below(value):
        return jnp.where(not_last, pltpu.roll(value, LANES - 1, 1), 0.0)

    def above(value):
        return jnp.where(not_first, pltpu.roll(value, 1, 1), 0.0)

    def keep(h, s, g, value, power):
        for part, ref in enumerate((zr, zi)):
            ref[h * 16 + s, pl.ds(g * 8, 8), :] = value[part]
            if h == 0 or s == 0:
                ref[h * 16 + s, pl.ds(16 + g, 1), :] = below(value[part])[0:1]
        return power + (value[0] * value[0] + value[1] * value[1])

    for h in range(tiles):
        for g in range(2):
            if packed:
                phases = swap_bits([in_ref[a, h * 16 + g * 8 : h * 16 + g * 8 + 8, :] for a in range(16)], lane)
            else:
                phases = [in_ref[h, s, g * 8 : g * 8 + 8, :] for s in range(16)]
            power = jnp.zeros((8, LANES), jnp.float32)
            for s in range(16):
                cosine, sine = cos_sin(phases[s])
                power = keep(h, s, g, (cosine * here[h], sine * here[h]), power)
            energy[h * 16 + g * 8 : h * 16 + g * 8 + 8, :] = power

    def sharing(h, needed):
        places = {w % ring - h * per_tile for w in needed}
        places = {p for p in places if 0 <= p < per_tile}
        group = 1
        for k in (2, 4):
            if per_tile % k == 0:
                taken = {(p + j * (per_tile // k)) % per_tile for p in places for j in range(k)}
                group = k if len(taken) == k * len(places) else group
        masks = []
        for k in range(1, group):
            mask = place < 0
            for p in places:
                mask = mask | (place == (p + k * (per_tile // group)) % per_tile)
            masks.append(mask)
        return masks

    def merged(values, masks):
        result = values[0]
        for k, mask in enumerate(masks):
            result = jnp.where(mask, pltpu.roll(values[k + 1], (k + 1) * LANES // (len(masks) + 1), 1), result)
        return result

    def window_gains(plans):
        both_rows = [energy[h * 16 : h * 16 + 8, :] + energy[h * 16 + 8 : h * 16 + 16, :] for h in range(tiles)]
        blockwise = [jnp.broadcast_to(jnp.sum(e, axis=0, keepdims=True), (8, LANES)) for e in both_rows]
        tall = [e + below(e) for e in blockwise]
        for unit, ((h, masks, first, count), wide) in enumerate(zip(plans, right(tall, [p[0] for p in plans]))):
            value = merged([1.0 / ((tall[h] + wide) + EPS)] * 4, masks)
            for j in range(count):
                gain[(first + j) * 8 : (first + j) * 8 + 8, :] = value

    def forward_columns(step, plans, g):
        rows = pl.ds(pl.multiple_of(g * 8, 8), 8)
        under = pl.ds(g * 8 + 1, 8)
        active = [p[0] for p in plans]
        window_gains(plans)
        near = {h: [] for h in active}
        far = {h: [] for h in active}
        for s in range(16):
            re = [zr[h * 16 + s, rows, :] for h in range(tiles)]
            im = [zi[h * 16 + s, rows, :] for h in range(tiles)]
            for h, a, b in zip(active, right(re, active), right(im, active)):
                near[h].append((re[h], im[h]))
                far[h].append((a, b))
        for h, masks, first, count in plans:
            group = len(masks) + 1
            even = fft([plus(a, b) for a, b in zip(near[h], far[h])], -1)
            odd = fft([rotated(minus(a, b), s, 32, -1) for s, (a, b) in enumerate(zip(near[h], far[h]))], -1)
            for row in range(8 * count):
                sources = [(row // 8 * group + k) * 8 + row % 8 for k in range(group)]
                values = [(even, odd)[l % 2][l // 2] for l in sources]
                value = tuple(merged([v[part] for v in values], masks) for part in range(2))
                at = pl.ds((first * 8 + row) * 17 + g * 8, 8)
                if first == 0 and row < 8:
                    following = (below(value[0]), below(value[1]))
                    ur[at, :], ui[at, :] = plus(value, following)
                    vr[at, :], vi[at, :] = minus(value, following)
                else:
                    yr[at, :], yi[at, :] = value

        def corner(s):
            if s < 16:
                return near[0][s], (zr[s, under, :], zi[s, under, :])
            moved = [right([ref[h * 16, under, :] for h in range(tiles)], (0,))[0] for ref in (zr, zi)]
            return far[0][0], tuple(moved)

        def cross(a, b):
            return a[1] * b[0] - a[0] * b[1]

        total = jnp.zeros((8, LANES), jnp.float32)
        here_, under_ = corner(0)
        down = cross(here_, under_)
        for s in range(16):
            next_, next_under = corner(s + 1)
            next_down = cross(next_, next_under)
            loop = (cross(here_, next_) - cross(under_, next_under)) + (next_down - down)
            total = total + loop * loop
            here_, under_, down = next_, next_under, next_down
        sums[pl.ds(pl.multiple_of(step * 16 + g * 8, 8), 8), :] = total

    def split_rows(unit):
        for row in range(8):
            for g in range(2):
                source = pl.ds((unit * 8 + row) * 17 + g * 8, 8)
                at = pl.ds(row * 17 + g * 8, 8)
                value = (yr[source, :], yi[source, :])
                following = (below(value[0]), below(value[1]))
                ur[at, :], ui[at, :] = plus(value, following)
                vr[at, :], vi[at, :] = minus(value, following)

    def join_rows(unit):
        for t in range(16):
            source = pl.ds(t * 9, 8)
            at = pl.ds((unit * 16 + t) * 9, 8)
            wr[at, :] = pr[source, :] + above(qr[source, :])
            wi[at, :] = pi[source, :] + above(qi[source, :])

    def windows(unit):
        join_rows(jnp.maximum(unit - 1, 0))
        scale = gain[pl.ds(pl.multiple_of(unit * 8, 8), 8), :]
        at = [pl.ds(t, 8, stride=17) for t in range(16)]
        back = []
        for parity, (a, b) in enumerate(((ur, ui), (vr, vi))):
            values = [(a[x, :], b[x, :]) for x in at]
            if parity:
                values = [rotated(v, t, 32, -1) for t, v in enumerate(values)]
            filtered = []
            for re, im in fft(values, -1):
                factor = lax.rsqrt(lax.rsqrt((re * re + im * im) * scale))
                filtered.append((re * factor, im * factor))
            back.append(fft(filtered, 1))
        split_rows(unit + 1)
        for t in range(16):
            odd = rotated(back[1][t], t, 32, 1)
            upper = plus(back[0][t], odd)
            lower = minus(back[0][t], odd)
            at = pl.ds(t * 9, 8)
            pr[at, :], pi[at, :] = (v * (ramp(t) / 32) for v in upper)
            qr[at, :], qi[at, :] = (v * (ramp(t + 16) / 32) for v in lower)

    def inverse_columns(plans, units, g):
        rows = pl.ds(pl.multiple_of(g * 8, 8), 8)
        kept = []
        passed = []
        for h, masks, first, count in plans:
            group = len(masks) + 1
            values = [None] * 32
            for row in range(8 * count):
                unit = first + row // 8
                if unit == units - 1:
                    at = pl.ds(g * 72 + row % 8, 8, stride=9)
                    value = (pr[at, :] + above(qr[at, :]), pi[at, :] + above(qi[at, :]))
                else:
                    at = pl.ds(unit * 144 + g * 72 + row % 8, 8, stride=9)
                    value = (wr[at, :], wi[at, :])
                for k in range(group):
                    l = (row // 8 * group + k) * 8 + row % 8
                    values[l] = tuple(pltpu.roll(v, LANES - k * LANES // group, 1) if k else v for v in value)
            even = fft(values[0::2], 1)
            odd = fft(values[1::2], 1)
            own = []
            other = []
            for s in range(16):
                turned = rotated(odd[s], s, 32, 1)
                weight = here[h] * (ramp(s) / 32)
                own.append(tuple(v * weight for v in plus(even[s], turned)))
                weight = both[h] * (ramp(s + 16) / 32)
                other.append(tuple(v * weight for v in minus(even[s], turned)))
            kept.append(own)
            passed.append(other)
        if len(plans) == tiles:
            power = [jnp.zeros((8, LANES), jnp.float32) for _ in range(tiles)]
            for s in range(16):
                arrived = [left([passed[h][s][part] for h in range(tiles)]) for part in range(2)]
                for h in range(tiles):
                    value = tuple(kept[h][s][part] + arrived[part][h] for part in range(2))
                    power[h] = keep(h, s, g, value, power[h])
            for h in range(tiles):
                energy[pl.ds(pl.multiple_of(h * 16 + g * 8, 8), 8), :] = power[h]
            return
        for s in range(16):
            for part, ref in enumerate((zr, zi)):
                ref[s, rows, :] = kept[0][s][part]
                ref[16 + s, rows, :] = pltpu.roll(passed[0][s][part], slabs, 1)

    def run(count, body):
        lax.fori_loop(0, count, lambda i, c: (body(i), c)[1], 0)

    for step in range(ITERS):
        before = ITERS - step - (1 if packed else 0)
        needed = range(-before, blocks + ITERS - 1 - step)
        plans = []
        units = 0
        for h in range(1 if packed and step == ITERS - 1 else tiles):
            masks = sharing(h, needed)
            plans.append((h, masks, units, 4 // (len(masks) + 1)))
            units += 4 // (len(masks) + 1)
        run(2, functools.partial(forward_columns, step, plans))
        run(units, windows)
        run(2, functools.partial(inverse_columns, plans, units))
    totals = [jnp.sum(sums[step * 16 : step * 16 + 8, :] + sums[step * 16 + 8 : step * 16 + 16, :]) for step in range(ITERS)]

    if not packed:
        for step, total in enumerate(totals):
            out_ref[32, step : step + 1, :] = jnp.full((1, LANES), total)
        for part, ref in enumerate((zr, zi)):
            for s in range(16):
                out_ref[part * 16 + s, :, :] = ref[s, 0:16, :]
        return

    spill = []
    for part, ref in enumerate((zr, zi)):
        for g in range(2):
            own = [ref[s, g * 8 : g * 8 + 8, :] for s in range(16)]
            other = [ref[16 + s, g * 8 : g * 8 + 8, :] for s in range(16)]
            values = [a + jnp.where(place > 0, b, 0.0) for a, b in zip(own, other)]
            for a, value in enumerate(swap_bits(values, lane)):
                out_ref[a, part * 16 + g * 8 : part * 16 + g * 8 + 8, :] = value
            for q in range(2):
                pack = other[8 * q]
                for j in range(1, 8):
                    pack = jnp.where(place == j, pltpu.roll(other[8 * q + j], j * slabs, 1), pack)
                spill.append(pack)
    turned = jnp.concatenate(spill + spill, axis=0).T
    for j in range(8):
        turn[j * 17 : j * 17 + 16, :] = turned[j * 16 : j * 16 + 16, :]
    report = jnp.zeros((8, LANES), jnp.float32)
    for step, total in enumerate(totals):
        report = jnp.where((sub == step) & (lane == 64 + tile), total, report)
    for a in range(16):
        out_ref[a, 32:40, :] = jnp.where(lane < 64, turn[pl.ds(a, 8, stride=17), :], report)


def filter_tiles(slabs, blocks, tiles, packed, data):
    shape = (16, 40, LANES) if packed else (33, 16, LANES)
    body = functools.partial(filter_kernel, slabs, blocks, tiles, packed)
    return pl.pallas_call(
        body,
        out_shape=jax.ShapeDtypeStruct(shape, jnp.float32),
        in_specs=[pl.BlockSpec(memory_space=pltpu.VMEM)],
        out_specs=pl.BlockSpec(memory_space=pltpu.VMEM),
        scratch_shapes=[pltpu.VMEM((tiles * 16, 24, LANES), jnp.float32)] * 2
        + [pltpu.VMEM(((tiles * 4 + 1) * 136, LANES), jnp.float32)] * 2
        + [pltpu.VMEM((136, LANES), jnp.float32)] * 4
        + [pltpu.VMEM((tiles * 4 * 144, LANES), jnp.float32)] * 2
        + [pltpu.VMEM((144, LANES), jnp.float32)] * 4
        + [pltpu.VMEM((rows, LANES), jnp.float32) for rows in (tiles * 16, tiles * 32, ITERS * 16, 136)],
        compiler_params=pltpu.CompilerParams(vmem_limit_bytes=16 << 20),
        name="filter_tiles",
    )(data)


def finish_kernel(scale, in_ref, field_ref, profile_ref):
    lane = lax.broadcasted_iota(jnp.int32, (8, LANES), 1)
    extras = [in_ref[c, 32:40, :] for c in range(16)]
    sums = functools.reduce(jnp.add, extras)
    profile_ref[...] = pltpu.roll(sums, 64, 1)[:ITERS, :16] * scale
    turned = jnp.concatenate(extras, axis=0).T
    low = (lane & 8) == 0
    for part in range(2):
        for g in range(2):
            first = (part * 2 + g) * 16
            a = turned[first : first + 8]
            b = turned[first + 8 : first + 16]
            pairs = (jnp.where(low, a, pltpu.roll(b, 8, 1)), jnp.where(low, pltpu.roll(a, LANES - 8, 1), b))
            for c in range(16):
                value = in_ref[c, part * 16 + g * 8 : part * 16 + g * 8 + 8, :]
                if c:
                    spill = pltpu.roll(pairs[(c - 1) % 2], (LANES - (c - 1) // 2 * 16) % LANES, 1)
                    value = value + jnp.where(lane < 16, spill, 0.0)
                field_ref[part, g * 8 : g * 8 + 8, c * LANES : (c + 1) * LANES] = value


def finish(scale, data):
    return pl.pallas_call(
        functools.partial(finish_kernel, scale),
        out_shape=(
            jax.ShapeDtypeStruct((2, 16, 16 * LANES), jnp.float32),
            jax.ShapeDtypeStruct((ITERS, 16), jnp.float32),
        ),
        in_specs=[pl.BlockSpec(memory_space=pltpu.VMEM)],
        out_specs=[pl.BlockSpec(memory_space=pltpu.VMEM)] * 2,
        compiler_params=pltpu.CompilerParams(vmem_limit_bytes=8 << 20),
        name="finish",
    )(data)


def ring_of_blocks(phase, devices, blocks, tiles):
    per_tile = LANES // devices
    ring = tiles * per_tile
    width = phase.shape[1]
    padded = jnp.pad(phase, ((0, 0), (HALO * 16, (ring + HALO) * 16)))
    pieces = []
    for d in range(devices):
        start = d * blocks * 16
        ahead = padded[:, start + HALO * 16 : start + (blocks + 2 * HALO) * 16]
        behind = padded[:, start : start + HALO * 16]
        gap = jnp.zeros((16, (ring - blocks - 2 * HALO) * 16), phase.dtype)
        pieces.append(jnp.concatenate([ahead, gap, behind], axis=1))
    return jnp.stack(pieces)


def per_device(phase):
    devices = lax.axis_size("rows")
    height, width = phase.shape
    blocks = width // (16 * devices)
    per_tile = LANES // devices
    if height != 16 or LANES % devices or blocks * 16 * devices != width or blocks != per_tile:
        raise ValueError("unsupported sizes")
    scale = 1.0 / (height * devices * 128.0)
    if devices == 16:
        tiles = 2
        columns = phase.reshape(16, devices, LANES).transpose(1, 0, 2)
        empty = jnp.zeros((1, 16, LANES), phase.dtype)
        after = jnp.concatenate([columns[1:], empty])
        before = jnp.concatenate([empty, columns[:-1]])
        lane = lax.broadcasted_iota(jnp.int32, columns.shape, 2)
        data = jnp.concatenate([columns, jnp.where(lane < LANES // 2, after, before)], axis=1)
        data = lax.all_to_all(data, "rows", 0, 0)
        result = filter_tiles(devices, blocks, tiles, True, data)
        result = lax.all_to_all(result, "rows", 0, 0)
        return finish(scale, result)
    tiles = -(-(blocks + 2 * HALO) // per_tile)
    data = lax.all_to_all(ring_of_blocks(phase, devices, blocks, tiles), "rows", 0, 0)
    data = data.reshape(devices, 16, tiles, per_tile, 16).transpose(2, 4, 1, 3, 0)
    result = filter_tiles(devices, blocks, tiles, False, data.reshape(tiles, 16, 16, LANES))
    field = result[:32].reshape(2, 16, 16, per_tile, devices).transpose(4, 0, 2, 3, 1)
    field = field.reshape(devices, 32, per_tile * 16)
    sums = jnp.broadcast_to(result[32, :ITERS, : per_tile * 16][None], (devices, ITERS, per_tile * 16))
    result = lax.all_to_all(jnp.concatenate([field, sums], axis=1), "rows", 0, 0)
    field = result[:, :32].reshape(devices, 2, 16, per_tile * 16).transpose(1, 2, 0, 3).reshape(2, 16, width)
    profile = result[:, 32:, 0].reshape(width // 128, -1, ITERS).sum(1).T
    return field, profile * scale


def solution(mesh):
    return jax.shard_map(
        per_device,
        mesh=mesh,
        in_specs=(P(("groups", "rows"), None),),
        out_specs=(P(None, ("groups", "rows"), None), P("groups", None)),
        check_vma=False,
    )
```

```python
import functools
import math

import jax
import jax.numpy as jnp
from jax import lax
from jax.experimental import pallas as pl
from jax.experimental.pallas import tpu as pltpu
from jax.sharding import PartitionSpec as P

ITERS = 3
EPS = 1e-06
LANES = 128
HALO = 3

SIN = (9.99999996e-01, -1.66666580e-01, 8.33305053e-03, -1.98090400e-04, 2.60515161e-06)
COS = (9.99999953e-01, -4.99999050e-01, 4.16635780e-02, -1.38536600e-03, 2.31530144e-05)


def rotated(value, k, size, sign):
    re, im = value
    half = math.sqrt(0.5)
    if k == 0:
        return re, im
    if 4 * k == size:
        return (im, -re) if sign < 0 else (-im, re)
    if 8 * k == size:
        return ((re + im) * half, (im - re) * half) if sign < 0 else ((re - im) * half, (im + re) * half)
    if 8 * k == 3 * size:
        return ((im - re) * half, (re + im) * -half) if sign < 0 else ((re + im) * -half, (re - im) * half)
    if 2 * k > size:
        return rotated((-re, -im), k - size // 2, size, sign)
    c = math.cos(2 * math.pi * k / size)
    s = sign * math.sin(2 * math.pi * k / size)
    return re * c - im * s, im * c + re * s


def plus(a, b):
    return a[0] + b[0], a[1] + b[1]


def minus(a, b):
    return a[0] - b[0], a[1] - b[1]


def quarter_turn(a, sign):
    return (-a[1], a[0]) if sign > 0 else (a[1], -a[0])


def join(one, three, size, sign):
    quarter = size // 4
    one = [rotated(one[k], k, size, sign) for k in range(quarter)]
    three = [rotated(three[k], 3 * k, size, sign) for k in range(quarter)]
    turned = [quarter_turn(minus(a, b), sign) for a, b in zip(one, three)]
    return [plus(a, b) for a, b in zip(one, three)] + turned


def fft(values, sign):
    size = len(values)
    if size == 1:
        return values
    if size == 2:
        return [plus(*values), minus(*values)]
    even = fft(values[0::2], sign)
    odd = join(fft(values[1::4], sign), fft(values[3::4], sign), size, sign)
    return [plus(e, o) for e, o in zip(even, odd)] + [minus(e, o) for e, o in zip(even, odd)]


def odd_outputs(differences):
    one = []
    three = []
    for k in range(8):
        turned = quarter_turn(differences[k + 8], -1)
        one.append(rotated(plus(differences[k], turned), k, 32, -1))
        three.append(rotated(minus(differences[k], turned), 3 * k, 32, -1))
    pairs = zip(fft(one, -1), fft(three, -1))
    return [value for pair in pairs for value in pair]


def polynomial(coefficients, w):
    result = jnp.full_like(w, coefficients[-1])
    for c in coefficients[-2::-1]:
        result = result * w + c
    return result


def cos_sin(x):
    u = (jnp.abs(x) - jnp.float32(math.pi / 2)) + jnp.float32(4.371139e-08)
    w = u * u
    cosine = -(u * polynomial(SIN, w))
    sine = polynomial(COS, w)
    return cosine, jnp.where(x < 0, -sine, sine)


def ramp(t):
    return 1.0 - abs(t - 15.5) / 16.0


def filter_kernel(
    slabs, blocks, tiles, in_ref, out_ref, zr, zi, yr, yi, ur, ui, vr, vi, wr, wi, pr, pi, qr, qi, energy, gain, sums
):
    tile = lax.axis_index("rows")
    per_tile = LANES // slabs
    ring = tiles * per_tile
    lane = lax.broadcasted_iota(jnp.int32, (8, LANES), 1)
    sub = lax.broadcasted_iota(jnp.int32, (8, LANES), 0)
    not_last = lane % slabs != slabs - 1
    not_first = lane % slabs != 0
    place = lane // slabs

    def inside(h, step):
        position = (h * per_tile + place + step) % ring
        relative = jnp.where(position < blocks + HALO, position, position - ring)
        column = tile * blocks + relative
        return jnp.where((column >= 0) & (column < slabs * blocks), 1.0, 0.0)

    here = [inside(h, 0) for h in range(tiles)]
    both = [here[h] * inside(h, 1) for h in range(tiles)]

    def right(values, active):
        if per_tile == 1:
            return [values[(h + 1) % tiles] for h in active]
        moved = [pltpu.roll(v, LANES - slabs, 1) for v in values]
        return [jnp.where(lane < LANES - slabs, moved[h], moved[(h + 1) % tiles]) for h in active]

    def left(values):
        if per_tile == 1:
            return [values[h - 1] for h in range(tiles)]
        moved = [pltpu.roll(v, slabs, 1) for v in values]
        return [jnp.where(lane < slabs, moved[h - 1], moved[h]) for h in range(tiles)]

    def below(value):
        return jnp.where(not_last, pltpu.roll(value, LANES - 1, 1), 0.0)

    def above(value):
        return jnp.where(not_first, pltpu.roll(value, 1, 1), 0.0)

    def keep(h, s, g, value, power):
        for part, ref in enumerate((zr, zi)):
            ref[h * 16 + s, pl.ds(g * 8, 8), :] = value[part]
            if h == 0 or s == 0:
                ref[h * 16 + s, pl.ds(16 + g, 1), :] = below(value[part])[0:1]
        return power + (value[0] * value[0] + value[1] * value[1])

    for h in range(tiles):
        for g in range(2):
            phases = [in_ref[h, s, g * 8 : g * 8 + 8, :] for s in range(16)]
            power = jnp.zeros((8, LANES), jnp.float32)
            for s in range(16):
                cosine, sine = cos_sin(phases[s])
                power = keep(h, s, g, (cosine * here[h], sine * here[h]), power)
            energy[h * 16 + g * 8 : h * 16 + g * 8 + 8, :] = power

    def sharing(h, needed):
        places = {w % ring - h * per_tile for w in needed}
        places = {p for p in places if 0 <= p < per_tile}
        group = 1
        for k in (2, 4):
            if per_tile % k == 0:
                taken = {(p + j * (per_tile // k)) % per_tile for p in places for j in range(k)}
                group = k if len(taken) == k * len(places) else group
        masks = []
        for k in range(1, group):
            mask = place < 0
            for p in places:
                mask = mask | (place == (p + k * (per_tile // group)) % per_tile)
            masks.append(mask)
        return masks

    def merged(values, masks):
        result = values[0]
        for k, mask in enumerate(masks):
            result = jnp.where(mask, pltpu.roll(values[k + 1], (k + 1) * LANES // (len(masks) + 1), 1), result)
        return result

    def window_gains(plans):
        both_rows = [energy[h * 16 : h * 16 + 8, :] + energy[h * 16 + 8 : h * 16 + 16, :] for h in range(tiles)]
        blockwise = [jnp.broadcast_to(jnp.sum(e, axis=0, keepdims=True), (8, LANES)) for e in both_rows]
        tall = [e + below(e) for e in blockwise]
        for unit, ((h, masks, first, count), wide) in enumerate(zip(plans, right(tall, [p[0] for p in plans]))):
            value = merged([1.0 / ((tall[h] + wide) + EPS)] * 4, masks)
            for j in range(count):
                gain[(first + j) * 8 : (first + j) * 8 + 8, :] = value

    def forward_columns(step, plans, g):
        rows = pl.ds(pl.multiple_of(g * 8, 8), 8)
        under = pl.ds(g * 8 + 1, 8)
        active = [p[0] for p in plans]
        window_gains(plans)
        near = {h: [] for h in active}
        far = {h: [] for h in active}
        for s in range(16):
            re = [zr[h * 16 + s, rows, :] for h in range(tiles)]
            im = [zi[h * 16 + s, rows, :] for h in range(tiles)]
            for h, a, b in zip(active, right(re, active), right(im, active)):
                near[h].append((re[h], im[h]))
                far[h].append((a, b))
        for h, masks, first, count in plans:
            group = len(masks) + 1
            even = fft([plus(a, b) for a, b in zip(near[h], far[h])], -1)
            odd = fft([rotated(minus(a, b), s, 32, -1) for s, (a, b) in enumerate(zip(near[h], far[h]))], -1)
            for row in range(8 * count):
                sources = [(row // 8 * group + k) * 8 + row % 8 for k in range(group)]
                values = [(even, odd)[l % 2][l // 2] for l in sources]
                value = tuple(merged([v[part] for v in values], masks) for part in range(2))
                at = pl.ds((first * 8 + row) * 17 + g * 8, 8)
                if first == 0 and row < 8:
                    following = (below(value[0]), below(value[1]))
                    ur[at, :], ui[at, :] = plus(value, following)
                    vr[at, :], vi[at, :] = minus(value, following)
                else:
                    yr[at, :], yi[at, :] = value

        def corner(s):
            if s < 16:
                return near[0][s], (zr[s, under, :], zi[s, under, :])
            moved = [right([ref[h * 16, under, :] for h in range(tiles)], (0,))[0] for ref in (zr, zi)]
            return far[0][0], tuple(moved)

        def cross(a, b):
            return a[1] * b[0] - a[0] * b[1]

        total = jnp.zeros((8, LANES), jnp.float32)
        here_, under_ = corner(0)
        down = cross(here_, under_)
        for s in range(16):
            next_, next_under = corner(s + 1)
            next_down = cross(next_, next_under)
            loop = (cross(here_, next_) - cross(under_, next_under)) + (next_down - down)
            total = total + loop * loop
            here_, under_, down = next_, next_under, next_down
        sums[pl.ds(pl.multiple_of(step * 16 + g * 8, 8), 8), :] = total

    def split_rows(unit):
        for row in range(8):
            for g in range(2):
                source = pl.ds((unit * 8 + row) * 17 + g * 8, 8)
                at = pl.ds(row * 17 + g * 8, 8)
                value = (yr[source, :], yi[source, :])
                following = (below(value[0]), below(value[1]))
                ur[at, :], ui[at, :] = plus(value, following)
                vr[at, :], vi[at, :] = minus(value, following)

    def join_rows(unit):
        for t in range(16):
            source = pl.ds(t * 9, 8)
            at = pl.ds((unit * 16 + t) * 9, 8)
            wr[at, :] = pr[source, :] + above(qr[source, :])
            wi[at, :] = pi[source, :] + above(qi[source, :])

    def windows(unit):
        join_rows(jnp.maximum(unit - 1, 0))
        scale = gain[pl.ds(pl.multiple_of(unit * 8, 8), 8), :]
        at = [pl.ds(t, 8, stride=17) for t in range(16)]
        back = []
        for parity, (a, b) in enumerate(((ur, ui), (vr, vi))):
            values = [(a[x, :], b[x, :]) for x in at]
            if parity:
                values = [rotated(v, t, 32, -1) for t, v in enumerate(values)]
            filtered = []
            for re, im in fft(values, -1):
                factor = lax.rsqrt(lax.rsqrt((re * re + im * im) * scale))
                filtered.append((re * factor, im * factor))
            back.append(fft(filtered, 1))
        split_rows(unit + 1)
        for t in range(16):
            odd = rotated(back[1][t], t, 32, 1)
            upper = plus(back[0][t], odd)
            lower = minus(back[0][t], odd)
            at = pl.ds(t * 9, 8)
            pr[at, :], pi[at, :] = (v * (ramp(t) / 32) for v in upper)
            qr[at, :], qi[at, :] = (v * (ramp(t + 16) / 32) for v in lower)

    def inverse_columns(plans, units, g):
        rows = pl.ds(pl.multiple_of(g * 8, 8), 8)
        kept = []
        passed = []
        for h, masks, first, count in plans:
            group = len(masks) + 1
            values = [None] * 32
            for row in range(8 * count):
                unit = first + row // 8
                if unit == units - 1:
                    at = pl.ds(g * 72 + row % 8, 8, stride=9)
                    value = (pr[at, :] + above(qr[at, :]), pi[at, :] + above(qi[at, :]))
                else:
                    at = pl.ds(unit * 144 + g * 72 + row % 8, 8, stride=9)
                    value = (wr[at, :], wi[at, :])
                for k in range(group):
                    l = (row // 8 * group + k) * 8 + row % 8
                    values[l] = tuple(pltpu.roll(v, LANES - k * LANES // group, 1) if k else v for v in value)
            even = fft(values[0::2], 1)
            odd = fft(values[1::2], 1)
            own = []
            other = []
            for s in range(16):
                turned = rotated(odd[s], s, 32, 1)
                weight = here[h] * (ramp(s) / 32)
                own.append(tuple(v * weight for v in plus(even[s], turned)))
                weight = both[h] * (ramp(s + 16) / 32)
                other.append(tuple(v * weight for v in minus(even[s], turned)))
            kept.append(own)
            passed.append(other)
        power = [jnp.zeros((8, LANES), jnp.float32) for _ in range(tiles)]
        for s in range(16):
            arrived = [left([passed[h][s][part] for h in range(tiles)]) for part in range(2)]
            for h in range(tiles):
                value = tuple(kept[h][s][part] + arrived[part][h] for part in range(2))
                power[h] = keep(h, s, g, value, power[h])
        for h in range(tiles):
            energy[pl.ds(pl.multiple_of(h * 16 + g * 8, 8), 8), :] = power[h]

    def run(count, body):
        lax.fori_loop(0, count, lambda i, c: (body(i), c)[1], 0)

    for step in range(ITERS):
        needed = range(step - ITERS, blocks + ITERS - 1 - step)
        plans = []
        units = 0
        for h in range(tiles):
            masks = sharing(h, needed)
            plans.append((h, masks, units, 4 // (len(masks) + 1)))
            units += 4 // (len(masks) + 1)
        run(2, functools.partial(forward_columns, step, plans))
        run(units, windows)
        run(2, functools.partial(inverse_columns, plans, units))
    totals = [jnp.sum(sums[step * 16 : step * 16 + 8, :] + sums[step * 16 + 8 : step * 16 + 16, :]) for step in range(ITERS)]

    for step, total in enumerate(totals):
        out_ref[32, step : step + 1, :] = jnp.full((1, LANES), total)
    for part, ref in enumerate((zr, zi)):
        for s in range(16):
            out_ref[part * 16 + s, :, :] = ref[s, 0:16, :]


def filter_tiles(slabs, blocks, tiles, data):
    body = functools.partial(filter_kernel, slabs, blocks, tiles)
    return pl.pallas_call(
        body,
        out_shape=jax.ShapeDtypeStruct((33, 16, LANES), jnp.float32),
        in_specs=[pl.BlockSpec(memory_space=pltpu.VMEM)],
        out_specs=pl.BlockSpec(memory_space=pltpu.VMEM),
        scratch_shapes=[pltpu.VMEM((tiles * 16, 24, LANES), jnp.float32)] * 2
        + [pltpu.VMEM(((tiles * 4 + 1) * 136, LANES), jnp.float32)] * 2
        + [pltpu.VMEM((136, LANES), jnp.float32)] * 4
        + [pltpu.VMEM((tiles * 4 * 144, LANES), jnp.float32)] * 2
        + [pltpu.VMEM((144, LANES), jnp.float32)] * 4
        + [pltpu.VMEM((rows, LANES), jnp.float32) for rows in (tiles * 16, tiles * 32, ITERS * 16)],
        compiler_params=pltpu.CompilerParams(vmem_limit_bytes=16 << 20),
        name="filter_tiles",
    )(data)


def column_kernel(in_ref, out_ref, *scratch):
    zr, zi, yr, yi, wr, wi, shift_r, shift_i, gain, turn = scratch[:10]
    buffers = [scratch[10 + 6 * k : 16 + 6 * k] for k in range(2)]
    final = scratch[22:25]
    tile = lax.axis_index("rows")
    lane = lax.broadcasted_iota(jnp.int32, (8, LANES), 1)
    sub = lax.broadcasted_iota(jnp.int32, (8, LANES), 0)
    in_slab = lane & 7

    def inside(first):
        column = tile * 8 + (first - 2) + sub
        return jnp.where((column >= 0) & (column < 128), 1.0, 0.0)

    def block(body):
        pl.when(tile >= 0)(body)

    def run(count, body):
        lax.fori_loop(0, count, lambda i, c: (body(i), c)[1], 0)

    zero = jnp.zeros((8, LANES), jnp.float32)
    for vr, vi, pr, pi, qr, qi in buffers:
        for ref in (vr, vi):
            for row in (272, 280, 288):
                ref[row : row + 8, :] = zero
        for ref in (qr, qi):
            for t in range(16):
                ref[t * 17 : t * 17 + 1, :] = zero[0:1]

    for g in range(2):
        for h in range(2):
            stacked = jnp.concatenate([in_ref[a, h * 16 + g * 8 : h * 16 + g * 8 + 8, :] for a in range(16)], axis=0)
            base = (g * 2 + h) * 136
            turned = stacked.T
            for b in range(8):
                turn[base + b * 17 : base + b * 17 + 16, :] = turned[b * 16 : b * 16 + 16]
    halo = jnp.where(sub < 3, inside(10), jnp.where(sub > 5, inside(-6), 0.0))
    for g in range(2):
        for h, mask in enumerate((None, halo)):
            for s in range(16):
                value = cos_sin(turn[pl.ds((g * 2 + h) * 136 + s, 8, stride=17), :])
                for ref, v in zip((zr, zi), value):
                    if h == 0:
                        ref[g * 16 + s, 2:10, :] = v
                    else:
                        ref[g * 16 + s, 10:13, :] = (v * mask)[0:3]
                        ref[g * 16 + s, 0:2, :] = (v * mask)[6:8]

    def forward_columns(first, width, g):
        energies = []
        for j in range(-(-width // 8)):
            rows = min(8, width - 8 * j)
            at = first + 8 * j
            near = [(zr[g * 16 + s, at : at + 8, :], zi[g * 16 + s, at : at + 8, :]) for s in range(16)]
            far = [(zr[g * 16 + s, at + 1 : at + 9, :], zi[g * 16 + s, at + 1 : at + 9, :]) for s in range(16)]
            power = zero
            for a, b in zip(near, far):
                power = power + ((a[0] * a[0] + a[1] * a[1]) + (b[0] * b[0] + b[1] * b[1]))
            energies.append(power)
            even = fft([plus(a, b) for a, b in zip(near, far)], -1)
            odd = odd_outputs([minus(a, b) for a, b in zip(near, far)])
            for l in range(32):
                re, im = (even, odd)[l % 2][l // 2]
                to = pl.ds(g * 400 + l * width + 8 * j, rows)
                yr[to, :] = re[0:rows]
                yi[to, :] = im[0:rows]
        for j, power in enumerate(energies):
            gain[pl.ds(pl.multiple_of(48 + g * 16 + j * 8, 8), 8), :] = power

    def turn_in(chunk):
        vr, vi = buffers[chunk % 2][:2]
        for source, ref in ((yr, vr), (yi, vi)):
            for g in range(2):
                turned = source[g * 400 + chunk * 128 : g * 400 + chunk * 128 + 128, :].T
                for a in range(16):
                    ref[a * 17 + g * 8 : a * 17 + g * 8 + 8, :] = turned[a * 8 : a * 8 + 8]

    def turn_out(chunk):
        pr, pi, qr, qi = buffers[chunk % 2][2:]
        for p, q, target in ((pr, qr, wr), (pi, qi, wi)):
            for g in range(2):
                parts = []
                for a in range(16):
                    at = pl.ds(g * 136 + a, 8, stride=17)
                    parts.append(p[at, :] + q[at, :])
                target[g * 400 + chunk * 128 : g * 400 + chunk * 128 + 128, :] = jnp.concatenate(parts, axis=0).T

    def window_gains(width, chunks):
        power = [gain[48 + j * 8 : 56 + j * 8, :] + gain[64 + j * 8 : 72 + j * 8, :] for j in range(2)]
        power[1] = jnp.where(sub < width - 8, power[1], 0.0)
        row = lax.broadcasted_iota(jnp.int32, (16, LANES), 0)
        slab = lax.broadcasted_iota(jnp.int32, (16, LANES), 1) // 8
        pick = jnp.where((slab == row) | (slab == row + 1), 1.0, 0.0)
        exact = dict(precision=lax.Precision.HIGHEST, preferred_element_type=jnp.float32)
        mean = lax.dot_general(pick, jnp.concatenate(power, axis=0), (((1,), (1,)), ((), ())), **exact)
        column = lax.broadcasted_iota(jnp.int32, (16, chunks * 128), 1)
        column = column - width * ((column.astype(jnp.float32) + 0.5) * (1.0 / width)).astype(jnp.int32)
        spread = jnp.where(column == lax.broadcasted_iota(jnp.int32, (16, chunks * 128), 0), 1.0, 0.0)
        value = lax.dot_general(1.0 / (mean + EPS), spread, (((1,), (0,)), ((), ())), **exact)
        for c in range(chunks):
            gain[c * 16 : c * 16 + 16, :] = value[:, c * 128 : c * 128 + 128]

    def residues():
        def corner(s):
            at = 2 if s < 16 else 3
            result = []
            for ref in (zr, zi):
                top = ref[s % 16, at : at + 8, :]
                low = ref[16 + s % 16, at : at + 8, :]
                top_left = pltpu.roll(top, LANES - 1, 1)
                low_left = pltpu.roll(low, LANES - 1, 1)
                top_under = jnp.where(in_slab < 7, top_left, pltpu.roll(low, 7, 1))
                low_under = jnp.where(in_slab < 7, low_left, jnp.where(lane < LANES - 1, top_left, 0.0))
                result.append((top, low, top_under, low_under))
            return [((result[0][g], result[1][g]), (result[0][2 + g], result[1][2 + g])) for g in range(2)]

        def cross(a, b):
            return a[1] * b[0] - a[0] * b[1]

        total = zero
        here = corner(0)
        down = [cross(*pair) for pair in here]
        for s in range(16):
            following = corner(s + 1)
            following_down = [cross(*pair) for pair in following]
            for g in range(2):
                across = cross(here[g][0], following[g][0]) - cross(here[g][1], following[g][1])
                loop = across + (following_down[g] - down[g])
                total = total + loop * loop
            here, down = following, following_down
        return total

    def windows(chunk, half):
        vr, vi, pr, pi, qr, qi = buffers[chunk % 2]
        scale = gain[chunk * 16 + half * 8 : chunk * 16 + half * 8 + 8, :]
        sums = []
        differences = []
        for t in range(16):
            at = pl.ds(half * 136 + t, 8, stride=17)
            after = pl.ds(half * 136 + 17 + t, 8, stride=17)
            near = (vr[at, :], vi[at, :])
            far = (vr[after, :], vi[after, :])
            sums.append(plus(near, far))
            differences.append(minus(near, far))
        back = []
        for spectrum in (lambda: fft(sums, -1), lambda: odd_outputs(differences)):
            filtered = []
            for re, im in spectrum():
                factor = lax.rsqrt(lax.rsqrt((re * re + im * im) * scale))
                filtered.append((re * factor, im * factor))
            back.append(filtered)
        back = fft(back[0], 1), join(fft(back[1][0::2], 1), fft(back[1][1::2], 1), 32, 1)
        for t in range(16):
            upper = plus(back[0][t], back[1][t])
            lower = minus(back[0][t], back[1][t])
            at = pl.ds(t * 17 + half * 8, 8)
            pr[at, :], pi[at, :] = (v * (ramp(t) / 32) for v in upper)
            at = pl.ds(t * 17 + half * 8 + 1, 8)
            qr[at, :], qi[at, :] = (v * (ramp(t + 16) / 32) for v in lower)

    def inverse_columns(first, width, last, g):
        groups = range(-(-width // 8))
        kept = []
        for j in groups:
            here = inside(first + 8 * j)
            both = here * inside(first + 8 * j + 1)
            values = []
            for l in range(32):
                at = pl.ds(g * 400 + l * width + 8 * j, 8)
                values.append((wr[at, :], wi[at, :]))
            even = fft(values[0::2], 1)
            odd = join(fft(values[1::4], 1), fft(values[3::4], 1), 32, 1)
            for s in range(16):
                weight = here * (ramp(s) / 32)
                own = [v * weight for v in plus(even[s], odd[s])]
                weight = both * (ramp(s + 16) / 32)
                other = [v * weight for v in minus(even[s], odd[s])]
                if last:
                    for part in range(2):
                        base = (part * 2 + g) * 144 + s * 9
                        final[0][pl.ds(base, 8), :] = own[part]
                        final[1][pl.ds(base + 1, 8), :] = other[part]
                else:
                    kept.append(own)
                    shift_r[s * 24 + 8 * j + 1 : s * 24 + 8 * j + 9, :] = other[0]
                    shift_i[s * 24 + 8 * j + 1 : s * 24 + 8 * j + 9, :] = other[1]
        if last:
            return
        for j in groups:
            rows = min(8, width - 8 * j)
            for s in range(16):
                for part, (ref, shift) in enumerate(((zr, shift_r), (zi, shift_i))):
                    value = kept[j * 16 + s][part] + shift[s * 24 + 8 * j : s * 24 + 8 * j + 8, :]
                    ref[g * 16 + s, first + 8 * j : first + 8 * j + rows, :] = value[0:rows]

    for k in range(4):
        for s in range(16):
            final[1][k * 144 + s * 9 : k * 144 + s * 9 + 1, :] = zero[0:1]

    for step in range(ITERS):
        first = step
        width = 12 - 2 * step
        chunks = -(-width // 4)
        last = step == ITERS - 1
        run(2, functools.partial(forward_columns, first, width))

        @block
        def _():
            window_gains(width, chunks)
            turn_in(0)
            final[2][step * 8 : step * 8 + 8, :] = residues()

        for chunk in range(chunks):

            @block
            def _():
                if chunk + 1 < chunks:
                    turn_in(chunk + 1)
                windows(chunk, 0)
                windows(chunk, 1)
                if chunk:
                    turn_out(chunk - 1)

        block(lambda: turn_out(chunks - 1))
        run(2, functools.partial(inverse_columns, first, width, last))

    spill = []
    for part in range(2):
        for g in range(2):
            base = (part * 2 + g) * 144
            rows = []
            for b in range(8):
                for s in (0, 8):
                    at = pl.ds(base + s * 9 + b, 8, stride=9)
                    rows.append(final[0][at, :] + final[1][at, :])
            turned = jnp.concatenate(rows, axis=0).T
            for a in range(16):
                out_ref[a, part * 16 + g * 8 : part * 16 + g * 8 + 8, :] = turned[a * 8 : a * 8 + 8]
            spill += [final[1][pl.ds(base + s * 9 + 8, 8, stride=9), :] for s in (0, 8)]
    turned = jnp.concatenate(spill + spill, axis=0).T
    report = zero
    for step in range(ITERS):
        total = jnp.sum(final[2][step * 8 : step * 8 + 8, :])
        report = jnp.where((sub == step) & (lane == 64 + tile), total, report)
    for a in range(16):
        out_ref[a, 32:40, :] = jnp.where(lane < 64, turned[a * 8 : a * 8 + 8], report)


def filter_columns(data):
    def rows(count):
        return pltpu.VMEM((count, LANES), jnp.float32)

    return pl.pallas_call(
        column_kernel,
        out_shape=jax.ShapeDtypeStruct((16, 40, LANES), jnp.float32),
        in_specs=[pl.BlockSpec(memory_space=pltpu.VMEM)],
        out_specs=pl.BlockSpec(memory_space=pltpu.VMEM),
        scratch_shapes=[pltpu.VMEM((32, 24, LANES), jnp.float32)] * 2
        + [rows(800)] * 4
        + [rows(384)] * 2
        + [rows(80), rows(544)]
        + ([rows(296)] * 2 + [rows(280)] * 4) * 2
        + [rows(584), rows(584), rows(ITERS * 8)],
        compiler_params=pltpu.CompilerParams(vmem_limit_bytes=16 << 20),
        name="filter_columns",
    )(data)


def finish_kernel(scale, in_ref, field_ref, profile_ref):
    lane = lax.broadcasted_iota(jnp.int32, (8, LANES), 1)
    extras = [in_ref[c, 32:40, :] for c in range(16)]
    sums = functools.reduce(jnp.add, extras)
    profile_ref[...] = pltpu.roll(sums, 64, 1)[:ITERS, :16] * scale
    for part in range(2):
        for g in range(2):
            offset = (part * 2 + g) * 16
            for c in range(16):
                value = in_ref[c, part * 16 + g * 8 : part * 16 + g * 8 + 8, :]
                if c:
                    spill = pltpu.roll(extras[c - 1], LANES - offset, 1) if offset else extras[c - 1]
                    value = value + jnp.where(lane < 16, spill, 0.0)
                field_ref[part, g * 8 : g * 8 + 8, c * LANES : (c + 1) * LANES] = value


def finish(scale, data):
    return pl.pallas_call(
        functools.partial(finish_kernel, scale),
        out_shape=(
            jax.ShapeDtypeStruct((2, 16, 16 * LANES), jnp.float32),
            jax.ShapeDtypeStruct((ITERS, 16), jnp.float32),
        ),
        in_specs=[pl.BlockSpec(memory_space=pltpu.VMEM)],
        out_specs=[pl.BlockSpec(memory_space=pltpu.VMEM)] * 2,
        compiler_params=pltpu.CompilerParams(vmem_limit_bytes=8 << 20),
        name="finish",
    )(data)


def ring_of_blocks(phase, devices, blocks, tiles):
    per_tile = LANES // devices
    ring = tiles * per_tile
    width = phase.shape[1]
    padded = jnp.pad(phase, ((0, 0), (HALO * 16, (ring + HALO) * 16)))
    pieces = []
    for d in range(devices):
        start = d * blocks * 16
        ahead = padded[:, start + HALO * 16 : start + (blocks + 2 * HALO) * 16]
        behind = padded[:, start : start + HALO * 16]
        gap = jnp.zeros((16, (ring - blocks - 2 * HALO) * 16), phase.dtype)
        pieces.append(jnp.concatenate([ahead, gap, behind], axis=1))
    return jnp.stack(pieces)


def per_device(phase):
    devices = lax.axis_size("rows")
    height, width = phase.shape
    blocks = width // (16 * devices)
    per_tile = LANES // devices
    if height != 16 or LANES % devices or blocks * 16 * devices != width or blocks != per_tile:
        raise ValueError("unsupported sizes")
    scale = 1.0 / (height * devices * 128.0)
    if devices == 16:
        columns = phase.reshape(16, devices, LANES).transpose(1, 0, 2)
        empty = jnp.zeros((1, 16, LANES), phase.dtype)
        after = jnp.concatenate([columns[1:], empty])
        before = jnp.concatenate([empty, columns[:-1]])
        lane = lax.broadcasted_iota(jnp.int32, columns.shape, 2)
        data = jnp.concatenate([columns, jnp.where(lane < LANES // 2, after, before)], axis=1)
        data = lax.all_to_all(data, "rows", 0, 0)
        result = filter_columns(data)
        result = lax.all_to_all(result, "rows", 0, 0)
        return finish(scale, result)
    tiles = -(-(blocks + 2 * HALO) // per_tile)
    data = lax.all_to_all(ring_of_blocks(phase, devices, blocks, tiles), "rows", 0, 0)
    data = data.reshape(devices, 16, tiles, per_tile, 16).transpose(2, 4, 1, 3, 0)
    result = filter_tiles(devices, blocks, tiles, data.reshape(tiles, 16, 16, LANES))
    field = result[:32].reshape(2, 16, 16, per_tile, devices).transpose(4, 0, 2, 3, 1)
    field = field.reshape(devices, 32, per_tile * 16)
    sums = jnp.broadcast_to(result[32, :ITERS, : per_tile * 16][None], (devices, ITERS, per_tile * 16))
    result = lax.all_to_all(jnp.concatenate([field, sums], axis=1), "rows", 0, 0)
    field = result[:, :32].reshape(devices, 2, 16, per_tile * 16).transpose(1, 2, 0, 3).reshape(2, 16, width)
    profile = result[:, 32:, 0].reshape(width // 128, -1, ITERS).sum(1).T
    return field, profile * scale


def solution(mesh):
    return jax.shard_map(
        per_device,
        mesh=mesh,
        in_specs=(P(("groups", "rows"), None),),
        out_specs=(P(None, ("groups", "rows"), None), P("groups", None)),
        check_vma=False,
    )
```

```python
import functools
import math

import jax
import jax.numpy as jnp
from jax import lax
from jax.experimental import pallas as pl
from jax.experimental.pallas import tpu as pltpu
from jax.sharding import PartitionSpec as P

ITERS = 3
EPS = 1e-06
LANES = 128
IN_ROWS = 26
OUT_ROWS = 37
HALO = 3

SIN = (9.99999996e-01, -1.66666580e-01, 8.33305053e-03, -1.98090400e-04, 2.60515161e-06)
COS = (9.99999953e-01, -4.99999050e-01, 4.16635780e-02, -1.38536600e-03, 2.31530144e-05)


def rotated(value, k, size, sign):
    re, im = value
    half = math.sqrt(0.5)
    if k == 0:
        return re, im
    if 4 * k == size:
        return (im, -re) if sign < 0 else (-im, re)
    if 8 * k == size:
        return ((re + im) * half, (im - re) * half) if sign < 0 else ((re - im) * half, (im + re) * half)
    if 8 * k == 3 * size:
        return ((im - re) * half, (re + im) * -half) if sign < 0 else ((re + im) * -half, (re - im) * half)
    if 2 * k > size:
        return rotated((-re, -im), k - size // 2, size, sign)
    c = math.cos(2 * math.pi * k / size)
    s = sign * math.sin(2 * math.pi * k / size)
    return re * c - im * s, im * c + re * s


def plus(a, b):
    return a[0] + b[0], a[1] + b[1]


def minus(a, b):
    return a[0] - b[0], a[1] - b[1]


def quarter_turn(a, sign):
    return (-a[1], a[0]) if sign > 0 else (a[1], -a[0])


def join(one, three, size, sign):
    quarter = size // 4
    one = [rotated(one[k], k, size, sign) for k in range(quarter)]
    three = [rotated(three[k], 3 * k, size, sign) for k in range(quarter)]
    turned = [quarter_turn(minus(a, b), sign) for a, b in zip(one, three)]
    return [plus(a, b) for a, b in zip(one, three)] + turned


def fft(values, sign):
    size = len(values)
    if size == 1:
        return values
    if size == 2:
        return [plus(*values), minus(*values)]
    even = fft(values[0::2], sign)
    odd = join(fft(values[1::4], sign), fft(values[3::4], sign), size, sign)
    return [plus(e, o) for e, o in zip(even, odd)] + [minus(e, o) for e, o in zip(even, odd)]


def odd_outputs(differences):
    one = []
    three = []
    for k in range(8):
        turned = quarter_turn(differences[k + 8], -1)
        one.append(rotated(plus(differences[k], turned), k, 32, -1))
        three.append(rotated(minus(differences[k], turned), 3 * k, 32, -1))
    pairs = zip(fft(one, -1), fft(three, -1))
    return [value for pair in pairs for value in pair]


def polynomial(coefficients, w):
    result = jnp.full_like(w, coefficients[-1])
    for c in coefficients[-2::-1]:
        result = result * w + c
    return result


def cos_sin(x):
    u = (jnp.abs(x) - jnp.float32(math.pi / 2)) + jnp.float32(4.371139e-08)
    w = u * u
    cosine = -(u * polynomial(SIN, w))
    sine = polynomial(COS, w)
    return cosine, jnp.where(x < 0, -sine, sine)


def ramp(t):
    return 1.0 - abs(t - 15.5) / 16.0


def filter_kernel(
    slabs, blocks, tiles, in_ref, out_ref, zr, zi, yr, yi, ur, ui, vr, vi, wr, wi, pr, pi, qr, qi, energy, gain, sums
):
    tile = lax.axis_index("rows")
    per_tile = LANES // slabs
    ring = tiles * per_tile
    lane = lax.broadcasted_iota(jnp.int32, (8, LANES), 1)
    sub = lax.broadcasted_iota(jnp.int32, (8, LANES), 0)
    not_last = lane % slabs != slabs - 1
    not_first = lane % slabs != 0
    place = lane // slabs

    def inside(h, step):
        position = (h * per_tile + place + step) % ring
        relative = jnp.where(position < blocks + HALO, position, position - ring)
        column = tile * blocks + relative
        return jnp.where((column >= 0) & (column < slabs * blocks), 1.0, 0.0)

    here = [inside(h, 0) for h in range(tiles)]
    both = [here[h] * inside(h, 1) for h in range(tiles)]

    def right(values, active):
        if per_tile == 1:
            return [values[(h + 1) % tiles] for h in active]
        moved = [pltpu.roll(v, LANES - slabs, 1) for v in values]
        return [jnp.where(lane < LANES - slabs, moved[h], moved[(h + 1) % tiles]) for h in active]

    def left(values):
        if per_tile == 1:
            return [values[h - 1] for h in range(tiles)]
        moved = [pltpu.roll(v, slabs, 1) for v in values]
        return [jnp.where(lane < slabs, moved[h - 1], moved[h]) for h in range(tiles)]

    def below(value):
        return jnp.where(not_last, pltpu.roll(value, LANES - 1, 1), 0.0)

    def above(value):
        return jnp.where(not_first, pltpu.roll(value, 1, 1), 0.0)

    def keep(h, s, g, value, power):
        for part, ref in enumerate((zr, zi)):
            ref[h * 16 + s, pl.ds(g * 8, 8), :] = value[part]
            if h == 0 or s == 0:
                ref[h * 16 + s, pl.ds(16 + g, 1), :] = below(value[part])[0:1]
        return power + (value[0] * value[0] + value[1] * value[1])

    for h in range(tiles):
        for g in range(2):
            phases = [in_ref[h, s, g * 8 : g * 8 + 8, :] for s in range(16)]
            power = jnp.zeros((8, LANES), jnp.float32)
            for s in range(16):
                cosine, sine = cos_sin(phases[s])
                power = keep(h, s, g, (cosine * here[h], sine * here[h]), power)
            energy[h * 16 + g * 8 : h * 16 + g * 8 + 8, :] = power

    def sharing(h, needed):
        places = {w % ring - h * per_tile for w in needed}
        places = {p for p in places if 0 <= p < per_tile}
        group = 1
        for k in (2, 4):
            if per_tile % k == 0:
                taken = {(p + j * (per_tile // k)) % per_tile for p in places for j in range(k)}
                group = k if len(taken) == k * len(places) else group
        masks = []
        for k in range(1, group):
            mask = place < 0
            for p in places:
                mask = mask | (place == (p + k * (per_tile // group)) % per_tile)
            masks.append(mask)
        return masks

    def merged(values, masks):
        result = values[0]
        for k, mask in enumerate(masks):
            result = jnp.where(mask, pltpu.roll(values[k + 1], (k + 1) * LANES // (len(masks) + 1), 1), result)
        return result

    def window_gains(plans):
        both_rows = [energy[h * 16 : h * 16 + 8, :] + energy[h * 16 + 8 : h * 16 + 16, :] for h in range(tiles)]
        blockwise = [jnp.broadcast_to(jnp.sum(e, axis=0, keepdims=True), (8, LANES)) for e in both_rows]
        tall = [e + below(e) for e in blockwise]
        for unit, ((h, masks, first, count), wide) in enumerate(zip(plans, right(tall, [p[0] for p in plans]))):
            value = merged([1.0 / ((tall[h] + wide) + EPS)] * 4, masks)
            for j in range(count):
                gain[(first + j) * 8 : (first + j) * 8 + 8, :] = value

    def forward_columns(step, plans, g):
        rows = pl.ds(pl.multiple_of(g * 8, 8), 8)
        under = pl.ds(g * 8 + 1, 8)
        active = [p[0] for p in plans]
        window_gains(plans)
        near = {h: [] for h in active}
        far = {h: [] for h in active}
        for s in range(16):
            re = [zr[h * 16 + s, rows, :] for h in range(tiles)]
            im = [zi[h * 16 + s, rows, :] for h in range(tiles)]
            for h, a, b in zip(active, right(re, active), right(im, active)):
                near[h].append((re[h], im[h]))
                far[h].append((a, b))
        for h, masks, first, count in plans:
            group = len(masks) + 1
            even = fft([plus(a, b) for a, b in zip(near[h], far[h])], -1)
            odd = fft([rotated(minus(a, b), s, 32, -1) for s, (a, b) in enumerate(zip(near[h], far[h]))], -1)
            for row in range(8 * count):
                sources = [(row // 8 * group + k) * 8 + row % 8 for k in range(group)]
                values = [(even, odd)[l % 2][l // 2] for l in sources]
                value = tuple(merged([v[part] for v in values], masks) for part in range(2))
                at = pl.ds((first * 8 + row) * 17 + g * 8, 8)
                if first == 0 and row < 8:
                    following = (below(value[0]), below(value[1]))
                    ur[at, :], ui[at, :] = plus(value, following)
                    vr[at, :], vi[at, :] = minus(value, following)
                else:
                    yr[at, :], yi[at, :] = value

        def corner(s):
            if s < 16:
                return near[0][s], (zr[s, under, :], zi[s, under, :])
            moved = [right([ref[h * 16, under, :] for h in range(tiles)], (0,))[0] for ref in (zr, zi)]
            return far[0][0], tuple(moved)

        def cross(a, b):
            return a[1] * b[0] - a[0] * b[1]

        total = jnp.zeros((8, LANES), jnp.float32)
        here_, under_ = corner(0)
        down = cross(here_, under_)
        for s in range(16):
            next_, next_under = corner(s + 1)
            next_down = cross(next_, next_under)
            loop = (cross(here_, next_) - cross(under_, next_under)) + (next_down - down)
            total = total + loop * loop
            here_, under_, down = next_, next_under, next_down
        sums[pl.ds(pl.multiple_of(step * 16 + g * 8, 8), 8), :] = total

    def split_rows(unit):
        for row in range(8):
            for g in range(2):
                source = pl.ds((unit * 8 + row) * 17 + g * 8, 8)
                at = pl.ds(row * 17 + g * 8, 8)
                value = (yr[source, :], yi[source, :])
                following = (below(value[0]), below(value[1]))
                ur[at, :], ui[at, :] = plus(value, following)
                vr[at, :], vi[at, :] = minus(value, following)

    def join_rows(unit):
        for t in range(16):
            source = pl.ds(t * 9, 8)
            at = pl.ds((unit * 16 + t) * 9, 8)
            wr[at, :] = pr[source, :] + above(qr[source, :])
            wi[at, :] = pi[source, :] + above(qi[source, :])

    def windows(unit):
        join_rows(jnp.maximum(unit - 1, 0))
        scale = gain[pl.ds(pl.multiple_of(unit * 8, 8), 8), :]
        at = [pl.ds(t, 8, stride=17) for t in range(16)]
        back = []
        for parity, (a, b) in enumerate(((ur, ui), (vr, vi))):
            values = [(a[x, :], b[x, :]) for x in at]
            if parity:
                values = [rotated(v, t, 32, -1) for t, v in enumerate(values)]
            filtered = []
            for re, im in fft(values, -1):
                factor = lax.rsqrt(lax.rsqrt((re * re + im * im) * scale))
                filtered.append((re * factor, im * factor))
            back.append(fft(filtered, 1))
        split_rows(unit + 1)
        for t in range(16):
            odd = rotated(back[1][t], t, 32, 1)
            upper = plus(back[0][t], odd)
            lower = minus(back[0][t], odd)
            at = pl.ds(t * 9, 8)
            pr[at, :], pi[at, :] = (v * (ramp(t) / 32) for v in upper)
            qr[at, :], qi[at, :] = (v * (ramp(t + 16) / 32) for v in lower)

    def inverse_columns(plans, units, g):
        rows = pl.ds(pl.multiple_of(g * 8, 8), 8)
        kept = []
        passed = []
        for h, masks, first, count in plans:
            group = len(masks) + 1
            values = [None] * 32
            for row in range(8 * count):
                unit = first + row // 8
                if unit == units - 1:
                    at = pl.ds(g * 72 + row % 8, 8, stride=9)
                    value = (pr[at, :] + above(qr[at, :]), pi[at, :] + above(qi[at, :]))
                else:
                    at = pl.ds(unit * 144 + g * 72 + row % 8, 8, stride=9)
                    value = (wr[at, :], wi[at, :])
                for k in range(group):
                    l = (row // 8 * group + k) * 8 + row % 8
                    values[l] = tuple(pltpu.roll(v, LANES - k * LANES // group, 1) if k else v for v in value)
            even = fft(values[0::2], 1)
            odd = fft(values[1::2], 1)
            own = []
            other = []
            for s in range(16):
                turned = rotated(odd[s], s, 32, 1)
                weight = here[h] * (ramp(s) / 32)
                own.append(tuple(v * weight for v in plus(even[s], turned)))
                weight = both[h] * (ramp(s + 16) / 32)
                other.append(tuple(v * weight for v in minus(even[s], turned)))
            kept.append(own)
            passed.append(other)
        power = [jnp.zeros((8, LANES), jnp.float32) for _ in range(tiles)]
        for s in range(16):
            arrived = [left([passed[h][s][part] for h in range(tiles)]) for part in range(2)]
            for h in range(tiles):
                value = tuple(kept[h][s][part] + arrived[part][h] for part in range(2))
                power[h] = keep(h, s, g, value, power[h])
        for h in range(tiles):
            energy[pl.ds(pl.multiple_of(h * 16 + g * 8, 8), 8), :] = power[h]

    def run(count, body):
        lax.fori_loop(0, count, lambda i, c: (body(i), c)[1], 0)

    for step in range(ITERS):
        needed = range(step - ITERS, blocks + ITERS - 1 - step)
        plans = []
        units = 0
        for h in range(tiles):
            masks = sharing(h, needed)
            plans.append((h, masks, units, 4 // (len(masks) + 1)))
            units += 4 // (len(masks) + 1)
        run(2, functools.partial(forward_columns, step, plans))
        run(units, windows)
        run(2, functools.partial(inverse_columns, plans, units))
    totals = [jnp.sum(sums[step * 16 : step * 16 + 8, :] + sums[step * 16 + 8 : step * 16 + 16, :]) for step in range(ITERS)]

    for step, total in enumerate(totals):
        out_ref[32, step : step + 1, :] = jnp.full((1, LANES), total)
    for part, ref in enumerate((zr, zi)):
        for s in range(16):
            out_ref[part * 16 + s, :, :] = ref[s, 0:16, :]


def filter_tiles(slabs, blocks, tiles, data):
    body = functools.partial(filter_kernel, slabs, blocks, tiles)
    return pl.pallas_call(
        body,
        out_shape=jax.ShapeDtypeStruct((33, 16, LANES), jnp.float32),
        in_specs=[pl.BlockSpec(memory_space=pltpu.VMEM)],
        out_specs=pl.BlockSpec(memory_space=pltpu.VMEM),
        scratch_shapes=[pltpu.VMEM((tiles * 16, 24, LANES), jnp.float32)] * 2
        + [pltpu.VMEM(((tiles * 4 + 1) * 136, LANES), jnp.float32)] * 2
        + [pltpu.VMEM((136, LANES), jnp.float32)] * 4
        + [pltpu.VMEM((tiles * 4 * 144, LANES), jnp.float32)] * 2
        + [pltpu.VMEM((144, LANES), jnp.float32)] * 4
        + [pltpu.VMEM((rows, LANES), jnp.float32) for rows in (tiles * 16, tiles * 32, ITERS * 16)],
        compiler_params=pltpu.CompilerParams(vmem_limit_bytes=16 << 20),
        name="filter_tiles",
    )(data)


def pack_kernel(in_ref, out_ref, turn):
    lane = lax.broadcasted_iota(jnp.int32, (8, LANES), 1)
    zero = jnp.zeros((8, LANES), jnp.float32)
    columns = [[in_ref[g * 8 : g * 8 + 8, c * LANES : (c + 1) * LANES] for g in range(2)] for c in range(16)]
    for c in range(16):
        after = columns[c + 1] if c < 15 else [zero, zero]
        before = columns[c - 1] if c else [zero, zero]
        at = c * IN_ROWS
        out_ref[at : at + 8, :] = columns[c][0]
        out_ref[at + 8 : at + 16, :] = columns[c][1]
        first = jnp.where(lane < 32, after[0], pltpu.roll(before[0], 64, 1))
        second = jnp.where(lane < 96, pltpu.roll(after[1], 64, 1), before[1])
        out_ref[at + 16 : at + 24, :] = jnp.where(lane < 64, first, second)
        turn[c * 8 : c * 8 + 8, :] = jnp.where(lane < 16, pltpu.roll(after[0], 96, 1), pltpu.roll(after[1], 112, 1))
    for q in range(4):
        rows = turn[pl.ds(q * 32, 8, stride=4), :]
        for u in range(1, 4):
            rows = jnp.where(lane // 32 == u, pltpu.roll(turn[pl.ds(q * 32 + u, 8, stride=4), :], 32 * u, 1), rows)
        for k in range(4):
            at = (q * 4 + k) * IN_ROWS + 24
            out_ref[at : at + 2, :] = rows[k * 2 : k * 2 + 2]


def pack(phase):
    return pl.pallas_call(
        pack_kernel,
        out_shape=jax.ShapeDtypeStruct((16 * IN_ROWS, LANES), jnp.float32),
        in_specs=[pl.BlockSpec(memory_space=pltpu.VMEM)],
        out_specs=pl.BlockSpec(memory_space=pltpu.VMEM),
        scratch_shapes=[pltpu.VMEM((128, LANES), jnp.float32)],
        compiler_params=pltpu.CompilerParams(vmem_limit_bytes=8 << 20),
        name="pack",
    )(phase)


def column_kernel(in_ref, out_ref, *scratch):
    zr, zi, yr, yi, wr, wi, shift_r, shift_i, gain, turn = scratch[:10]
    buffers = [scratch[10 + 6 * k : 16 + 6 * k] for k in range(2)]
    final = scratch[22:25]
    tile = lax.axis_index("rows")
    lane = lax.broadcasted_iota(jnp.int32, (8, LANES), 1)
    sub = lax.broadcasted_iota(jnp.int32, (8, LANES), 0)
    in_slab = lane & 7

    def inside(first):
        column = tile * 8 + (first - 2) + sub
        return jnp.where((column >= 0) & (column < 128), 1.0, 0.0)

    def block(body):
        pl.when(tile >= 0)(body)

    def run(count, body):
        lax.fori_loop(0, count, lambda i, c: (body(i), c)[1], 0)

    zero = jnp.zeros((8, LANES), jnp.float32)
    for vr, vi, pr, pi, qr, qi in buffers:
        for ref in (vr, vi):
            for row in (272, 280, 288):
                ref[row : row + 8, :] = zero
        for ref in (qr, qi):
            for t in range(16):
                ref[t * 17 : t * 17 + 1, :] = zero[0:1]

    def stacked(offset):
        return jnp.concatenate([in_ref[a * IN_ROWS + offset : a * IN_ROWS + offset + 8, :] for a in range(16)], axis=0)

    for k, offset in enumerate((0, 8, 16)):
        turned = stacked(offset).T
        for b in range(8):
            turn[k * 136 + b * 17 : k * 136 + b * 17 + 16, :] = turned[b * 16 : b * 16 + 16]
    tail = jnp.concatenate([in_ref[a * IN_ROWS + 24 : a * IN_ROWS + 26, :] for a in range(16)], axis=0)
    for q in range(4):
        for u in range(4):
            value = tail[q * 8 : q * 8 + 8]
            turn[pl.ds(408 + q * 32 + u, 8, stride=4), :] = pltpu.roll(value, LANES - 32 * u, 1) if u else value
    turned = turn[408:536, :].T[0:32]
    beyond = jnp.where(tile * 8 + 10 < 128, 1.0, 0.0)
    for ref, v in zip((zr, zi), cos_sin(turned)):
        for k in range(32):
            ref[k, 12:13, :] = v[k : k + 1] * beyond
    for g in range(2):
        for s in range(16):
            value = cos_sin(turn[pl.ds(g * 136 + s, 8, stride=17), :])
            for ref, v in zip((zr, zi), value):
                ref[g * 16 + s, 2:10, :] = v
    edge = tile * 8 + jnp.where((sub & 3) < 2, 8 + (sub & 3), (sub & 3) - 4)
    edge = jnp.where((edge >= 0) & (edge < 128), 1.0, 0.0)
    for s in range(16):
        value = cos_sin(turn[pl.ds(272 + s, 8, stride=17), :])
        for ref, v in zip((zr, zi), value):
            v = v * edge
            for g in range(2):
                ref[g * 16 + s, 10:12, :] = v[g * 4 : g * 4 + 2]
                ref[g * 16 + s, 0:2, :] = v[g * 4 + 2 : g * 4 + 4]

    def forward_columns(first, width, g):
        energies = []
        for j in range(-(-width // 8)):
            rows = min(8, width - 8 * j)
            at = first + 8 * j
            near = [(zr[g * 16 + s, at : at + 8, :], zi[g * 16 + s, at : at + 8, :]) for s in range(16)]
            far = [(zr[g * 16 + s, at + 1 : at + 9, :], zi[g * 16 + s, at + 1 : at + 9, :]) for s in range(16)]
            power = zero
            for a, b in zip(near, far):
                power = power + ((a[0] * a[0] + a[1] * a[1]) + (b[0] * b[0] + b[1] * b[1]))
            energies.append(power)
            even = fft([plus(a, b) for a, b in zip(near, far)], -1)
            odd = odd_outputs([minus(a, b) for a, b in zip(near, far)])
            for l in range(32):
                re, im = (even, odd)[l % 2][l // 2]
                to = pl.ds(g * 400 + l * width + 8 * j, rows)
                yr[to, :] = re[0:rows]
                yi[to, :] = im[0:rows]
        for j, power in enumerate(energies):
            gain[pl.ds(pl.multiple_of(48 + g * 16 + j * 8, 8), 8), :] = power

    def turn_in(chunk):
        vr, vi = buffers[chunk % 2][:2]
        for source, ref in ((yr, vr), (yi, vi)):
            for g in range(2):
                turned = source[g * 400 + chunk * 128 : g * 400 + chunk * 128 + 128, :].T
                for a in range(16):
                    ref[a * 17 + g * 8 : a * 17 + g * 8 + 8, :] = turned[a * 8 : a * 8 + 8]

    def turn_out(chunk):
        pr, pi, qr, qi = buffers[chunk % 2][2:]
        for p, q, target in ((pr, qr, wr), (pi, qi, wi)):
            for g in range(2):
                parts = []
                for a in range(16):
                    at = pl.ds(g * 136 + a, 8, stride=17)
                    parts.append(p[at, :] + q[at, :])
                target[g * 400 + chunk * 128 : g * 400 + chunk * 128 + 128, :] = jnp.concatenate(parts, axis=0).T

    def window_gains(width, chunks):
        power = [gain[48 + j * 8 : 56 + j * 8, :] + gain[64 + j * 8 : 72 + j * 8, :] for j in range(2)]
        power[1] = jnp.where(sub < width - 8, power[1], 0.0)
        row = lax.broadcasted_iota(jnp.int32, (16, LANES), 0)
        slab = lax.broadcasted_iota(jnp.int32, (16, LANES), 1) // 8
        pick = jnp.where((slab == row) | (slab == row + 1), 1.0, 0.0)
        exact = dict(precision=lax.Precision.HIGHEST, preferred_element_type=jnp.float32)
        mean = lax.dot_general(pick, jnp.concatenate(power, axis=0), (((1,), (1,)), ((), ())), **exact)
        column = lax.broadcasted_iota(jnp.int32, (16, chunks * 128), 1)
        column = column - width * ((column.astype(jnp.float32) + 0.5) * (1.0 / width)).astype(jnp.int32)
        spread = jnp.where(column == lax.broadcasted_iota(jnp.int32, (16, chunks * 128), 0), 1.0, 0.0)
        value = lax.dot_general(1.0 / (mean + EPS), spread, (((1,), (0,)), ((), ())), **exact)
        for c in range(chunks):
            gain[c * 16 : c * 16 + 16, :] = value[:, c * 128 : c * 128 + 128]

    def residues():
        def corner(s):
            at = 2 if s < 16 else 3
            result = []
            for ref in (zr, zi):
                top = ref[s % 16, at : at + 8, :]
                low = ref[16 + s % 16, at : at + 8, :]
                top_left = pltpu.roll(top, LANES - 1, 1)
                low_left = pltpu.roll(low, LANES - 1, 1)
                top_under = jnp.where(in_slab < 7, top_left, pltpu.roll(low, 7, 1))
                low_under = jnp.where(in_slab < 7, low_left, jnp.where(lane < LANES - 1, top_left, 0.0))
                result.append((top, low, top_under, low_under))
            return [((result[0][g], result[1][g]), (result[0][2 + g], result[1][2 + g])) for g in range(2)]

        def cross(a, b):
            return a[1] * b[0] - a[0] * b[1]

        total = zero
        here = corner(0)
        down = [cross(*pair) for pair in here]
        for s in range(16):
            following = corner(s + 1)
            following_down = [cross(*pair) for pair in following]
            for g in range(2):
                across = cross(here[g][0], following[g][0]) - cross(here[g][1], following[g][1])
                loop = across + (following_down[g] - down[g])
                total = total + loop * loop
            here, down = following, following_down
        return total

    def windows(chunk, half):
        vr, vi, pr, pi, qr, qi = buffers[chunk % 2]
        scale = gain[chunk * 16 + half * 8 : chunk * 16 + half * 8 + 8, :]
        sums = []
        differences = []
        for t in range(16):
            at = pl.ds(half * 136 + t, 8, stride=17)
            after = pl.ds(half * 136 + 17 + t, 8, stride=17)
            near = (vr[at, :], vi[at, :])
            far = (vr[after, :], vi[after, :])
            sums.append(plus(near, far))
            differences.append(minus(near, far))
        back = []
        for spectrum in (lambda: fft(sums, -1), lambda: odd_outputs(differences)):
            filtered = []
            for re, im in spectrum():
                factor = lax.rsqrt(lax.rsqrt((re * re + im * im) * scale))
                filtered.append((re * factor, im * factor))
            back.append(filtered)
        back = fft(back[0], 1), join(fft(back[1][0::2], 1), fft(back[1][1::2], 1), 32, 1)
        for t in range(16):
            upper = plus(back[0][t], back[1][t])
            lower = minus(back[0][t], back[1][t])
            at = pl.ds(t * 17 + half * 8, 8)
            pr[at, :], pi[at, :] = (v * (ramp(t) / 32) for v in upper)
            at = pl.ds(t * 17 + half * 8 + 1, 8)
            qr[at, :], qi[at, :] = (v * (ramp(t + 16) / 32) for v in lower)

    def inverse_columns(first, width, last, g):
        groups = range(-(-width // 8))
        kept = []
        for j in groups:
            here = inside(first + 8 * j)
            both = here * inside(first + 8 * j + 1)
            values = []
            for l in range(32):
                at = pl.ds(g * 400 + l * width + 8 * j, 8)
                values.append((wr[at, :], wi[at, :]))
            even = fft(values[0::2], 1)
            odd = join(fft(values[1::4], 1), fft(values[3::4], 1), 32, 1)
            for s in range(16):
                weight = here * (ramp(s) / 32)
                own = [v * weight for v in plus(even[s], odd[s])]
                weight = both * (ramp(s + 16) / 32)
                other = [v * weight for v in minus(even[s], odd[s])]
                if last:
                    for part in range(2):
                        base = (part * 2 + g) * 144 + s * 9
                        final[0][pl.ds(base, 8), :] = own[part]
                        final[1][pl.ds(base + 1, 8), :] = other[part]
                else:
                    kept.append(own)
                    shift_r[s * 24 + 8 * j + 1 : s * 24 + 8 * j + 9, :] = other[0]
                    shift_i[s * 24 + 8 * j + 1 : s * 24 + 8 * j + 9, :] = other[1]
        if last:
            return
        for j in groups:
            rows = min(8, width - 8 * j)
            for s in range(16):
                for part, (ref, shift) in enumerate(((zr, shift_r), (zi, shift_i))):
                    value = kept[j * 16 + s][part] + shift[s * 24 + 8 * j : s * 24 + 8 * j + 8, :]
                    ref[g * 16 + s, first + 8 * j : first + 8 * j + rows, :] = value[0:rows]

    for k in range(4):
        for s in range(16):
            final[1][k * 144 + s * 9 : k * 144 + s * 9 + 1, :] = zero[0:1]

    for step in range(ITERS):
        first = step
        width = 12 - 2 * step
        chunks = -(-width // 4)
        last = step == ITERS - 1
        run(2, functools.partial(forward_columns, first, width))

        @block
        def _():
            window_gains(width, chunks)
            turn_in(0)
            final[2][step * 8 : step * 8 + 8, :] = residues()

        for chunk in range(chunks):

            @block
            def _():
                if chunk + 1 < chunks:
                    turn_in(chunk + 1)
                windows(chunk, 0)
                windows(chunk, 1)
                if chunk:
                    turn_out(chunk - 1)

        block(lambda: turn_out(chunks - 1))
        run(2, functools.partial(inverse_columns, first, width, last))

    spill = []
    for part in range(2):
        for g in range(2):
            base = (part * 2 + g) * 144
            rows = []
            for b in range(8):
                for s in (0, 8):
                    at = pl.ds(base + s * 9 + b, 8, stride=9)
                    rows.append(final[0][at, :] + final[1][at, :])
            turned = jnp.concatenate(rows, axis=0).T
            for a in range(16):
                at = a * OUT_ROWS + part * 16 + g * 8
                out_ref[at : at + 8, :] = turned[a * 8 : a * 8 + 8]
            spill += [final[1][pl.ds(base + s * 9 + 8, 8, stride=9), :] for s in (0, 8)]
    turned = jnp.concatenate(spill + spill, axis=0).T
    report = zero[0:1]
    for step in range(ITERS):
        total = jnp.sum(final[2][step * 8 : step * 8 + 8, :])
        report = jnp.where(lane[0:1] == step * 16 + tile, total, report)
    for a in range(16):
        value = turned[a * 8 : a * 8 + 8]
        out_ref[a * OUT_ROWS + 32 : a * OUT_ROWS + 36, :] = jnp.where(lane[0:4] < 64, value[0:4], value[4:8])
        out_ref[a * OUT_ROWS + 36 : a * OUT_ROWS + 37, :] = report


def filter_columns(data):
    def rows(count):
        return pltpu.VMEM((count, LANES), jnp.float32)

    return pl.pallas_call(
        column_kernel,
        out_shape=jax.ShapeDtypeStruct((16 * OUT_ROWS, LANES), jnp.float32),
        in_specs=[pl.BlockSpec(memory_space=pltpu.VMEM)],
        out_specs=pl.BlockSpec(memory_space=pltpu.VMEM),
        scratch_shapes=[pltpu.VMEM((32, 24, LANES), jnp.float32)] * 2
        + [rows(800)] * 4
        + [rows(384)] * 2
        + [rows(80), rows(544)]
        + ([rows(296)] * 2 + [rows(280)] * 4) * 2
        + [rows(584), rows(584), rows(ITERS * 8)],
        compiler_params=pltpu.CompilerParams(vmem_limit_bytes=16 << 20),
        name="filter_columns",
    )(data)


def finish_kernel(scale, in_ref, field_ref, profile_ref):
    lane = lax.broadcasted_iota(jnp.int32, (8, LANES), 1)
    extras = []
    sums = jnp.zeros((1, LANES), jnp.float32)
    for c in range(16):
        half = in_ref[c * OUT_ROWS + 32 : c * OUT_ROWS + 36, :]
        extras.append(jnp.concatenate([half, pltpu.roll(half, 64, 1)], axis=0))
        sums = sums + in_ref[c * OUT_ROWS + 36 : c * OUT_ROWS + 37, :]
    for step in range(ITERS):
        profile_ref[step : step + 1, :] = sums[:, step * 16 : step * 16 + 16] * scale
    for part in range(2):
        for g in range(2):
            offset = (part * 2 + g) * 16
            for c in range(16):
                at = c * OUT_ROWS + part * 16 + g * 8
                value = in_ref[at : at + 8, :]
                if c:
                    spill = pltpu.roll(extras[c - 1], LANES - offset, 1) if offset else extras[c - 1]
                    value = value + jnp.where(lane < 16, spill, 0.0)
                field_ref[part, g * 8 : g * 8 + 8, c * LANES : (c + 1) * LANES] = value


def finish(scale, data):
    return pl.pallas_call(
        functools.partial(finish_kernel, scale),
        out_shape=(
            jax.ShapeDtypeStruct((2, 16, 16 * LANES), jnp.float32),
            jax.ShapeDtypeStruct((ITERS, 16), jnp.float32),
        ),
        in_specs=[pl.BlockSpec(memory_space=pltpu.VMEM)],
        out_specs=[pl.BlockSpec(memory_space=pltpu.VMEM)] * 2,
        compiler_params=pltpu.CompilerParams(vmem_limit_bytes=8 << 20),
        name="finish",
    )(data)


def ring_of_blocks(phase, devices, blocks, tiles):
    per_tile = LANES // devices
    ring = tiles * per_tile
    width = phase.shape[1]
    padded = jnp.pad(phase, ((0, 0), (HALO * 16, (ring + HALO) * 16)))
    pieces = []
    for d in range(devices):
        start = d * blocks * 16
        ahead = padded[:, start + HALO * 16 : start + (blocks + 2 * HALO) * 16]
        behind = padded[:, start : start + HALO * 16]
        gap = jnp.zeros((16, (ring - blocks - 2 * HALO) * 16), phase.dtype)
        pieces.append(jnp.concatenate([ahead, gap, behind], axis=1))
    return jnp.stack(pieces)


def per_device(phase):
    devices = lax.axis_size("rows")
    height, width = phase.shape
    blocks = width // (16 * devices)
    per_tile = LANES // devices
    if height != 16 or LANES % devices or blocks * 16 * devices != width or blocks != per_tile:
        raise ValueError("unsupported sizes")
    scale = 1.0 / (height * devices * 128.0)
    if devices == 16:
        data = lax.all_to_all(pack(phase).reshape(16, IN_ROWS, 1, LANES), "rows", 0, 0)
        result = filter_columns(data.reshape(16 * IN_ROWS, LANES))
        result = lax.all_to_all(result.reshape(16, OUT_ROWS, 1, LANES), "rows", 0, 0)
        result = result.reshape(16 * OUT_ROWS, LANES)
        return finish(scale, result)
    tiles = -(-(blocks + 2 * HALO) // per_tile)
    data = lax.all_to_all(ring_of_blocks(phase, devices, blocks, tiles), "rows", 0, 0)
    data = data.reshape(devices, 16, tiles, per_tile, 16).transpose(2, 4, 1, 3, 0)
    result = filter_tiles(devices, blocks, tiles, data.reshape(tiles, 16, 16, LANES))
    field = result[:32].reshape(2, 16, 16, per_tile, devices).transpose(4, 0, 2, 3, 1)
    field = field.reshape(devices, 32, per_tile * 16)
    sums = jnp.broadcast_to(result[32, :ITERS, : per_tile * 16][None], (devices, ITERS, per_tile * 16))
    result = lax.all_to_all(jnp.concatenate([field, sums], axis=1), "rows", 0, 0)
    field = result[:, :32].reshape(devices, 2, 16, per_tile * 16).transpose(1, 2, 0, 3).reshape(2, 16, width)
    profile = result[:, 32:, 0].reshape(width // 128, -1, ITERS).sum(1).T
    return field, profile * scale


def solution(mesh):
    return jax.shard_map(
        per_device,
        mesh=mesh,
        in_specs=(P(("groups", "rows"), None),),
        out_specs=(P(None, ("groups", "rows"), None), P("groups", None)),
        check_vma=False,
    )
```

```python
import functools
import math

import jax
import jax.numpy as jnp
from jax import lax
from jax.experimental import pallas as pl
from jax.experimental.pallas import tpu as pltpu
from jax.sharding import PartitionSpec as P

ITERS = 3
EPS = 1e-06
LANES = 128
IN_ROWS = 26
OUT_ROWS = 37
PITCH = 40
HALO = 3

SIN = (9.99999996e-01, -1.66666580e-01, 8.33305053e-03, -1.98090400e-04, 2.60515161e-06)
COS = (9.99999953e-01, -4.99999050e-01, 4.16635780e-02, -1.38536600e-03, 2.31530144e-05)


def rotated(value, k, size, sign):
    re, im = value
    half = math.sqrt(0.5)
    if k == 0:
        return re, im
    if 4 * k == size:
        return (im, -re) if sign < 0 else (-im, re)
    if 8 * k == size:
        return ((re + im) * half, (im - re) * half) if sign < 0 else ((re - im) * half, (im + re) * half)
    if 8 * k == 3 * size:
        return ((im - re) * half, (re + im) * -half) if sign < 0 else ((re + im) * -half, (re - im) * half)
    if 2 * k > size:
        return rotated((-re, -im), k - size // 2, size, sign)
    c = math.cos(2 * math.pi * k / size)
    s = sign * math.sin(2 * math.pi * k / size)
    return re * c - im * s, im * c + re * s


def plus(a, b):
    return a[0] + b[0], a[1] + b[1]


def minus(a, b):
    return a[0] - b[0], a[1] - b[1]


def quarter_turn(a, sign):
    return (-a[1], a[0]) if sign > 0 else (a[1], -a[0])


def join(one, three, size, sign):
    quarter = size // 4
    one = [rotated(one[k], k, size, sign) for k in range(quarter)]
    three = [rotated(three[k], 3 * k, size, sign) for k in range(quarter)]
    turned = [quarter_turn(minus(a, b), sign) for a, b in zip(one, three)]
    return [plus(a, b) for a, b in zip(one, three)] + turned


def fft(values, sign):
    size = len(values)
    if size == 1:
        return values
    if size == 2:
        return [plus(*values), minus(*values)]
    even = fft(values[0::2], sign)
    odd = join(fft(values[1::4], sign), fft(values[3::4], sign), size, sign)
    return [plus(e, o) for e, o in zip(even, odd)] + [minus(e, o) for e, o in zip(even, odd)]


def odd_outputs(differences):
    one = []
    three = []
    for k in range(8):
        turned = quarter_turn(differences[k + 8], -1)
        one.append(rotated(plus(differences[k], turned), k, 32, -1))
        three.append(rotated(minus(differences[k], turned), 3 * k, 32, -1))
    pairs = zip(fft(one, -1), fft(three, -1))
    return [value for pair in pairs for value in pair]


def polynomial(coefficients, w):
    result = jnp.full_like(w, coefficients[-1])
    for c in coefficients[-2::-1]:
        result = result * w + c
    return result


def cos_sin(x):
    u = (jnp.abs(x) - jnp.float32(math.pi / 2)) + jnp.float32(4.371139e-08)
    w = u * u
    cosine = -(u * polynomial(SIN, w))
    sine = polynomial(COS, w)
    return cosine, jnp.where(x < 0, -sine, sine)


def ramp(t):
    return 1.0 - abs(t - 15.5) / 16.0


def filter_kernel(
    slabs, blocks, tiles, in_ref, out_ref, zr, zi, yr, yi, ur, ui, vr, vi, wr, wi, pr, pi, qr, qi, energy, gain, sums
):
    tile = lax.axis_index("rows")
    per_tile = LANES // slabs
    ring = tiles * per_tile
    lane = lax.broadcasted_iota(jnp.int32, (8, LANES), 1)
    sub = lax.broadcasted_iota(jnp.int32, (8, LANES), 0)
    not_last = lane % slabs != slabs - 1
    not_first = lane % slabs != 0
    place = lane // slabs

    def inside(h, step):
        position = (h * per_tile + place + step) % ring
        relative = jnp.where(position < blocks + HALO, position, position - ring)
        column = tile * blocks + relative
        return jnp.where((column >= 0) & (column < slabs * blocks), 1.0, 0.0)

    here = [inside(h, 0) for h in range(tiles)]
    both = [here[h] * inside(h, 1) for h in range(tiles)]

    def right(values, active):
        if per_tile == 1:
            return [values[(h + 1) % tiles] for h in active]
        moved = [pltpu.roll(v, LANES - slabs, 1) for v in values]
        return [jnp.where(lane < LANES - slabs, moved[h], moved[(h + 1) % tiles]) for h in active]

    def left(values):
        if per_tile == 1:
            return [values[h - 1] for h in range(tiles)]
        moved = [pltpu.roll(v, slabs, 1) for v in values]
        return [jnp.where(lane < slabs, moved[h - 1], moved[h]) for h in range(tiles)]

    def below(value):
        return jnp.where(not_last, pltpu.roll(value, LANES - 1, 1), 0.0)

    def above(value):
        return jnp.where(not_first, pltpu.roll(value, 1, 1), 0.0)

    def keep(h, s, g, value, power):
        for part, ref in enumerate((zr, zi)):
            ref[h * 16 + s, pl.ds(g * 8, 8), :] = value[part]
            if h == 0 or s == 0:
                ref[h * 16 + s, pl.ds(16 + g, 1), :] = below(value[part])[0:1]
        return power + (value[0] * value[0] + value[1] * value[1])

    for h in range(tiles):
        for g in range(2):
            phases = [in_ref[h, s, g * 8 : g * 8 + 8, :] for s in range(16)]
            power = jnp.zeros((8, LANES), jnp.float32)
            for s in range(16):
                cosine, sine = cos_sin(phases[s])
                power = keep(h, s, g, (cosine * here[h], sine * here[h]), power)
            energy[h * 16 + g * 8 : h * 16 + g * 8 + 8, :] = power

    def sharing(h, needed):
        places = {w % ring - h * per_tile for w in needed}
        places = {p for p in places if 0 <= p < per_tile}
        group = 1
        for k in (2, 4):
            if per_tile % k == 0:
                taken = {(p + j * (per_tile // k)) % per_tile for p in places for j in range(k)}
                group = k if len(taken) == k * len(places) else group
        masks = []
        for k in range(1, group):
            mask = place < 0
            for p in places:
                mask = mask | (place == (p + k * (per_tile // group)) % per_tile)
            masks.append(mask)
        return masks

    def merged(values, masks):
        result = values[0]
        for k, mask in enumerate(masks):
            result = jnp.where(mask, pltpu.roll(values[k + 1], (k + 1) * LANES // (len(masks) + 1), 1), result)
        return result

    def window_gains(plans):
        both_rows = [energy[h * 16 : h * 16 + 8, :] + energy[h * 16 + 8 : h * 16 + 16, :] for h in range(tiles)]
        blockwise = [jnp.broadcast_to(jnp.sum(e, axis=0, keepdims=True), (8, LANES)) for e in both_rows]
        tall = [e + below(e) for e in blockwise]
        for unit, ((h, masks, first, count), wide) in enumerate(zip(plans, right(tall, [p[0] for p in plans]))):
            value = merged([1.0 / ((tall[h] + wide) + EPS)] * 4, masks)
            for j in range(count):
                gain[(first + j) * 8 : (first + j) * 8 + 8, :] = value

    def forward_columns(step, plans, g):
        rows = pl.ds(pl.multiple_of(g * 8, 8), 8)
        under = pl.ds(g * 8 + 1, 8)
        active = [p[0] for p in plans]
        window_gains(plans)
        near = {h: [] for h in active}
        far = {h: [] for h in active}
        for s in range(16):
            re = [zr[h * 16 + s, rows, :] for h in range(tiles)]
            im = [zi[h * 16 + s, rows, :] for h in range(tiles)]
            for h, a, b in zip(active, right(re, active), right(im, active)):
                near[h].append((re[h], im[h]))
                far[h].append((a, b))
        for h, masks, first, count in plans:
            group = len(masks) + 1
            even = fft([plus(a, b) for a, b in zip(near[h], far[h])], -1)
            odd = fft([rotated(minus(a, b), s, 32, -1) for s, (a, b) in enumerate(zip(near[h], far[h]))], -1)
            for row in range(8 * count):
                sources = [(row // 8 * group + k) * 8 + row % 8 for k in range(group)]
                values = [(even, odd)[l % 2][l // 2] for l in sources]
                value = tuple(merged([v[part] for v in values], masks) for part in range(2))
                at = pl.ds((first * 8 + row) * 17 + g * 8, 8)
                if first == 0 and row < 8:
                    following = (below(value[0]), below(value[1]))
                    ur[at, :], ui[at, :] = plus(value, following)
                    vr[at, :], vi[at, :] = minus(value, following)
                else:
                    yr[at, :], yi[at, :] = value

        def corner(s):
            if s < 16:
                return near[0][s], (zr[s, under, :], zi[s, under, :])
            moved = [right([ref[h * 16, under, :] for h in range(tiles)], (0,))[0] for ref in (zr, zi)]
            return far[0][0], tuple(moved)

        def cross(a, b):
            return a[1] * b[0] - a[0] * b[1]

        total = jnp.zeros((8, LANES), jnp.float32)
        here_, under_ = corner(0)
        down = cross(here_, under_)
        for s in range(16):
            next_, next_under = corner(s + 1)
            next_down = cross(next_, next_under)
            loop = (cross(here_, next_) - cross(under_, next_under)) + (next_down - down)
            total = total + loop * loop
            here_, under_, down = next_, next_under, next_down
        sums[pl.ds(pl.multiple_of(step * 16 + g * 8, 8), 8), :] = total

    def split_rows(unit):
        for row in range(8):
            for g in range(2):
                source = pl.ds((unit * 8 + row) * 17 + g * 8, 8)
                at = pl.ds(row * 17 + g * 8, 8)
                value = (yr[source, :], yi[source, :])
                following = (below(value[0]), below(value[1]))
                ur[at, :], ui[at, :] = plus(value, following)
                vr[at, :], vi[at, :] = minus(value, following)

    def join_rows(unit):
        for t in range(16):
            source = pl.ds(t * 9, 8)
            at = pl.ds((unit * 16 + t) * 9, 8)
            wr[at, :] = pr[source, :] + above(qr[source, :])
            wi[at, :] = pi[source, :] + above(qi[source, :])

    def windows(unit):
        join_rows(jnp.maximum(unit - 1, 0))
        scale = gain[pl.ds(pl.multiple_of(unit * 8, 8), 8), :]
        at = [pl.ds(t, 8, stride=17) for t in range(16)]
        back = []
        for parity, (a, b) in enumerate(((ur, ui), (vr, vi))):
            values = [(a[x, :], b[x, :]) for x in at]
            if parity:
                values = [rotated(v, t, 32, -1) for t, v in enumerate(values)]
            filtered = []
            for re, im in fft(values, -1):
                factor = lax.rsqrt(lax.rsqrt((re * re + im * im) * scale))
                filtered.append((re * factor, im * factor))
            back.append(fft(filtered, 1))
        split_rows(unit + 1)
        for t in range(16):
            odd = rotated(back[1][t], t, 32, 1)
            upper = plus(back[0][t], odd)
            lower = minus(back[0][t], odd)
            at = pl.ds(t * 9, 8)
            pr[at, :], pi[at, :] = (v * (ramp(t) / 32) for v in upper)
            qr[at, :], qi[at, :] = (v * (ramp(t + 16) / 32) for v in lower)

    def inverse_columns(plans, units, g):
        rows = pl.ds(pl.multiple_of(g * 8, 8), 8)
        kept = []
        passed = []
        for h, masks, first, count in plans:
            group = len(masks) + 1
            values = [None] * 32
            for row in range(8 * count):
                unit = first + row // 8
                if unit == units - 1:
                    at = pl.ds(g * 72 + row % 8, 8, stride=9)
                    value = (pr[at, :] + above(qr[at, :]), pi[at, :] + above(qi[at, :]))
                else:
                    at = pl.ds(unit * 144 + g * 72 + row % 8, 8, stride=9)
                    value = (wr[at, :], wi[at, :])
                for k in range(group):
                    l = (row // 8 * group + k) * 8 + row % 8
                    values[l] = tuple(pltpu.roll(v, LANES - k * LANES // group, 1) if k else v for v in value)
            even = fft(values[0::2], 1)
            odd = fft(values[1::2], 1)
            own = []
            other = []
            for s in range(16):
                turned = rotated(odd[s], s, 32, 1)
                weight = here[h] * (ramp(s) / 32)
                own.append(tuple(v * weight for v in plus(even[s], turned)))
                weight = both[h] * (ramp(s + 16) / 32)
                other.append(tuple(v * weight for v in minus(even[s], turned)))
            kept.append(own)
            passed.append(other)
        power = [jnp.zeros((8, LANES), jnp.float32) for _ in range(tiles)]
        for s in range(16):
            arrived = [left([passed[h][s][part] for h in range(tiles)]) for part in range(2)]
            for h in range(tiles):
                value = tuple(kept[h][s][part] + arrived[part][h] for part in range(2))
                power[h] = keep(h, s, g, value, power[h])
        for h in range(tiles):
            energy[pl.ds(pl.multiple_of(h * 16 + g * 8, 8), 8), :] = power[h]

    def run(count, body):
        lax.fori_loop(0, count, lambda i, c: (body(i), c)[1], 0)

    for step in range(ITERS):
        needed = range(step - ITERS, blocks + ITERS - 1 - step)
        plans = []
        units = 0
        for h in range(tiles):
            masks = sharing(h, needed)
            plans.append((h, masks, units, 4 // (len(masks) + 1)))
            units += 4 // (len(masks) + 1)
        run(2, functools.partial(forward_columns, step, plans))
        run(units, windows)
        run(2, functools.partial(inverse_columns, plans, units))
    totals = [jnp.sum(sums[step * 16 : step * 16 + 8, :] + sums[step * 16 + 8 : step * 16 + 16, :]) for step in range(ITERS)]

    for step, total in enumerate(totals):
        out_ref[32, step : step + 1, :] = jnp.full((1, LANES), total)
    for part, ref in enumerate((zr, zi)):
        for s in range(16):
            out_ref[part * 16 + s, :, :] = ref[s, 0:16, :]


def filter_tiles(slabs, blocks, tiles, data):
    body = functools.partial(filter_kernel, slabs, blocks, tiles)
    return pl.pallas_call(
        body,
        out_shape=jax.ShapeDtypeStruct((33, 16, LANES), jnp.float32),
        in_specs=[pl.BlockSpec(memory_space=pltpu.VMEM)],
        out_specs=pl.BlockSpec(memory_space=pltpu.VMEM),
        scratch_shapes=[pltpu.VMEM((tiles * 16, 24, LANES), jnp.float32)] * 2
        + [pltpu.VMEM(((tiles * 4 + 1) * 136, LANES), jnp.float32)] * 2
        + [pltpu.VMEM((136, LANES), jnp.float32)] * 4
        + [pltpu.VMEM((tiles * 4 * 144, LANES), jnp.float32)] * 2
        + [pltpu.VMEM((144, LANES), jnp.float32)] * 4
        + [pltpu.VMEM((rows, LANES), jnp.float32) for rows in (tiles * 16, tiles * 32, ITERS * 16)],
        compiler_params=pltpu.CompilerParams(vmem_limit_bytes=16 << 20),
        name="filter_tiles",
    )(data)


def pack_kernel(in_ref, out_ref, turn):
    lane = lax.broadcasted_iota(jnp.int32, (8, LANES), 1)
    zero = jnp.zeros((8, LANES), jnp.float32)
    columns = [[in_ref[g * 8 : g * 8 + 8, c * LANES : (c + 1) * LANES] for g in range(2)] for c in range(16)]
    for c in range(16):
        after = columns[c + 1] if c < 15 else [zero, zero]
        before = columns[c - 1] if c else [zero, zero]
        at = c * IN_ROWS
        out_ref[at : at + 8, :] = columns[c][0]
        out_ref[at + 8 : at + 16, :] = columns[c][1]
        first = jnp.where(lane < 32, after[0], pltpu.roll(before[0], 64, 1))
        second = jnp.where(lane < 96, pltpu.roll(after[1], 64, 1), before[1])
        out_ref[at + 16 : at + 24, :] = jnp.where(lane < 64, first, second)
        turn[c * 8 : c * 8 + 8, :] = jnp.where(lane < 16, pltpu.roll(after[0], 96, 1), pltpu.roll(after[1], 112, 1))
    for q in range(4):
        rows = turn[pl.ds(q * 32, 8, stride=4), :]
        for u in range(1, 4):
            rows = jnp.where(lane // 32 == u, pltpu.roll(turn[pl.ds(q * 32 + u, 8, stride=4), :], 32 * u, 1), rows)
        for k in range(4):
            at = (q * 4 + k) * IN_ROWS + 24
            out_ref[at : at + 2, :] = rows[k * 2 : k * 2 + 2]


def pack(phase):
    return pl.pallas_call(
        pack_kernel,
        out_shape=jax.ShapeDtypeStruct((16 * IN_ROWS, LANES), jnp.float32),
        in_specs=[pl.BlockSpec(memory_space=pltpu.VMEM)],
        out_specs=pl.BlockSpec(memory_space=pltpu.VMEM),
        scratch_shapes=[pltpu.VMEM((128, LANES), jnp.float32)],
        compiler_params=pltpu.CompilerParams(vmem_limit_bytes=8 << 20),
        name="pack",
    )(phase)


def column_kernel(in_ref, out_ref, *scratch):
    zr, zi, yr, yi, wr, wi, shift_r, shift_i, gain, turn = scratch[:10]
    buffers = [scratch[10 + 6 * k : 16 + 6 * k] for k in range(2)]
    final = scratch[22:25]
    tile = lax.axis_index("rows")
    lane = lax.broadcasted_iota(jnp.int32, (8, LANES), 1)
    sub = lax.broadcasted_iota(jnp.int32, (8, LANES), 0)
    in_slab = lane & 7

    def inside(first):
        column = tile * 8 + (first - 2) + sub // 2
        return jnp.where((column >= 0) & (column < 128), 1.0, 0.0)

    def block(body):
        pl.when(tile >= 0)(body)

    def run(count, body):
        lax.fori_loop(0, count, lambda i, c: (body(i), c)[1], 0)

    zero = jnp.zeros((8, LANES), jnp.float32)
    for vr, vi, pr, pi, qr, qi in buffers:
        for ref in (vr, vi):
            for row in (272, 280, 288):
                ref[row : row + 8, :] = zero
        for ref in (qr, qi):
            for t in range(16):
                ref[t * 17 : t * 17 + 1, :] = zero[0:1]

    def stacked(offset):
        return jnp.concatenate([in_ref[a * IN_ROWS + offset : a * IN_ROWS + offset + 8, :] for a in range(16)], axis=0)

    for k, offset in enumerate((0, 8, 16)):
        turned = stacked(offset).T
        for b in range(8):
            turn[k * 136 + b * 17 : k * 136 + b * 17 + 16, :] = turned[b * 16 : b * 16 + 16]
    tail = jnp.concatenate([in_ref[a * IN_ROWS + 24 : a * IN_ROWS + 26, :] for a in range(16)], axis=0)
    for q in range(4):
        for u in range(4):
            value = tail[q * 8 : q * 8 + 8]
            turn[pl.ds(408 + q * 32 + u, 8, stride=4), :] = pltpu.roll(value, LANES - 32 * u, 1) if u else value
    turned = turn[408:536, :].T[0:32]
    beyond = jnp.where(tile * 8 + 10 < 128, 1.0, 0.0)
    for ref, v in zip((zr, zi), cos_sin(turned)):
        for k in range(32):
            at = (k % 16) * PITCH + 24 + k // 16
            ref[at : at + 1, :] = v[k : k + 1] * beyond
    for g in range(2):
        for s in range(16):
            value = cos_sin(turn[pl.ds(g * 136 + s, 8, stride=17), :])
            for ref, v in zip((zr, zi), value):
                ref[pl.ds(s * PITCH + 4 + g, 8, stride=2), :] = v
    edge = tile * 8 + jnp.where((sub & 3) < 2, 8 + (sub & 3), (sub & 3) - 4)
    edge = jnp.where((edge >= 0) & (edge < 128), 1.0, 0.0)
    for s in range(16):
        value = cos_sin(turn[pl.ds(272 + s, 8, stride=17), :])
        for ref, v in zip((zr, zi), value):
            v = v * edge
            for g in range(2):
                for k, place in enumerate((10, 11, 0, 1)):
                    at = s * PITCH + 2 * place + g
                    ref[at : at + 1, :] = v[g * 4 + k : g * 4 + k + 1]

    def forward_columns(first, width, j):
        near = []
        far = []
        power = zero
        for s in range(16):
            at = pl.ds(s * PITCH + 2 * first + j * 8, 8)
            after = pl.ds(s * PITCH + 2 * first + 2 + j * 8, 8)
            near.append((zr[at, :], zi[at, :]))
            far.append((zr[after, :], zi[after, :]))
            a, b = near[-1], far[-1]
            power = power + ((a[0] * a[0] + a[1] * a[1]) + (b[0] * b[0] + b[1] * b[1]))
        gain[pl.ds(pl.multiple_of(48 + j * 8, 8), 8), :] = power
        even = fft([plus(a, b) for a, b in zip(near, far)], -1)
        odd = odd_outputs([minus(a, b) for a, b in zip(near, far)])
        for l in range(32):
            to = pl.ds(l * 2 * width + j * 8, 8)
            yr[to, :], yi[to, :] = (even, odd)[l % 2][l // 2]

    def turn_in(chunk):
        vr, vi = buffers[chunk % 2][:2]
        for source, ref in ((yr, vr), (yi, vi)):
            for g in range(2):
                parts = [source[pl.ds(chunk * 256 + i * 16 + g, 8, stride=2), :] for i in range(16)]
                turned = jnp.concatenate(parts, axis=0).T
                for a in range(16):
                    ref[a * 17 + g * 8 : a * 17 + g * 8 + 8, :] = turned[a * 8 : a * 8 + 8]

    def turn_out(chunk):
        pr, pi, qr, qi = buffers[chunk % 2][2:]
        for p, q, target in ((pr, qr, wr), (pi, qi, wi)):
            for g in range(2):
                parts = []
                for a in range(16):
                    at = pl.ds(g * 136 + a, 8, stride=17)
                    parts.append(p[at, :] + q[at, :])
                turned = jnp.concatenate(parts, axis=0).T
                for i in range(16):
                    target[pl.ds(chunk * 256 + i * 16 + g, 8, stride=2), :] = turned[i * 8 : i * 8 + 8]

    def window_gains(valid, width):
        count = 2 * width
        power = jnp.concatenate(
            [jnp.where(sub < 2 * valid - 8 * j, gain[48 + j * 8 : 56 + j * 8, :], 0.0) for j in range(count // 8)], axis=0
        )
        row = lax.broadcasted_iota(jnp.int32, (16, LANES), 0)
        slab = lax.broadcasted_iota(jnp.int32, (16, LANES), 1) // 8
        pick = jnp.where((slab == row) | (slab == row + 1), 1.0, 0.0)
        exact = dict(precision=lax.Precision.HIGHEST, preferred_element_type=jnp.float32)
        mean = lax.dot_general(pick, power, (((1,), (1,)), ((), ())), **exact)
        column = lax.broadcasted_iota(jnp.int32, (count, 32 * width), 1)
        column = column - width * ((column.astype(jnp.float32) + 0.5) * (1.0 / width)).astype(jnp.int32)
        spread = jnp.where(column == lax.broadcasted_iota(jnp.int32, (count, 32 * width), 0) // 2, 1.0, 0.0)
        mean = lax.dot_general(mean, spread, (((1,), (0,)), ((), ())), **exact)
        for c in range(width // 4):
            gain[c * 16 : c * 16 + 16, :] = 1.0 / (mean[:, c * 128 : c * 128 + 128] + EPS)

    def residues():
        def corner(s):
            at = s * PITCH + 4 if s < 16 else 6
            result = []
            for ref in (zr, zi):
                top = ref[pl.ds(at, 8, stride=2), :]
                low = ref[pl.ds(at + 1, 8, stride=2), :]
                top_left = pltpu.roll(top, LANES - 1, 1)
                low_left = pltpu.roll(low, LANES - 1, 1)
                top_under = jnp.where(in_slab < 7, top_left, pltpu.roll(low, 7, 1))
                low_under = jnp.where(in_slab < 7, low_left, jnp.where(lane < LANES - 1, top_left, 0.0))
                result.append((top, low, top_under, low_under))
            return [((result[0][g], result[1][g]), (result[0][2 + g], result[1][2 + g])) for g in range(2)]

        def cross(a, b):
            return a[1] * b[0] - a[0] * b[1]

        total = zero
        here = corner(0)
        down = [cross(*pair) for pair in here]
        for s in range(16):
            following = corner(s + 1)
            following_down = [cross(*pair) for pair in following]
            for g in range(2):
                across = cross(here[g][0], following[g][0]) - cross(here[g][1], following[g][1])
                loop = across + (following_down[g] - down[g])
                total = total + loop * loop
            here, down = following, following_down
        return total

    def windows(chunk, half):
        vr, vi, pr, pi, qr, qi = buffers[chunk % 2]
        scale = gain[chunk * 16 + half * 8 : chunk * 16 + half * 8 + 8, :]
        sums = []
        differences = []
        for t in range(16):
            at = pl.ds(half * 136 + t, 8, stride=17)
            after = pl.ds(half * 136 + 17 + t, 8, stride=17)
            near = (vr[at, :], vi[at, :])
            far = (vr[after, :], vi[after, :])
            sums.append(plus(near, far))
            differences.append(minus(near, far))
        back = []
        for spectrum in (lambda: fft(sums, -1), lambda: odd_outputs(differences)):
            filtered = []
            for re, im in spectrum():
                factor = lax.rsqrt(lax.rsqrt((re * re + im * im) * scale))
                filtered.append((re * factor, im * factor))
            back.append(filtered)
        back = fft(back[0], 1), join(fft(back[1][0::2], 1), fft(back[1][1::2], 1), 32, 1)
        for t in range(16):
            upper = plus(back[0][t], back[1][t])
            lower = minus(back[0][t], back[1][t])
            at = pl.ds(t * 17 + half * 8, 8)
            pr[at, :], pi[at, :] = (v * (ramp(t) / 32) for v in upper)
            at = pl.ds(t * 17 + half * 8 + 1, 8)
            qr[at, :], qi[at, :] = (v * (ramp(t + 16) / 32) for v in lower)

    def inverse_columns(first, width, last, j):
        here = inside(first + 4 * j)
        both = here * inside(first + 4 * j + 1)
        values = []
        for l in range(32):
            at = pl.ds(l * 2 * width + 8 * j, 8)
            values.append((wr[at, :], wi[at, :]))
        even = fft(values[0::2], 1)
        odd = join(fft(values[1::4], 1), fft(values[3::4], 1), 32, 1)
        for s in range(16):
            weight = here * (ramp(s) / 32)
            own = [v * weight for v in plus(even[s], odd[s])]
            weight = both * (ramp(s + 16) / 32)
            other = [v * weight for v in minus(even[s], odd[s])]
            for part, (ref, shift) in enumerate(((zr, shift_r), (zi, shift_i))):
                if last:
                    base = part * 304 + s * 19 + 8 * j
                    final[0][pl.ds(base, 8), :] = own[part]
                    final[1][pl.ds(base + 2, 8), :] = other[part]
                else:
                    shift[pl.ds(s * 32 + 8 * j + 2, 8), :] = other[part]
                    value = own[part] + shift[pl.ds(s * 32 + 8 * j, 8), :]
                    ref[pl.ds(s * PITCH + 2 * first + 8 * j, 8), :] = value

    for k in range(32):
        final[1][k * 19 : k * 19 + 2, :] = zero[0:2]

    for step in range(ITERS):
        first = step
        valid = 12 - 2 * step
        width = -(-valid // 4) * 4
        chunks = width // 4
        last = step == ITERS - 1
        run(chunks, functools.partial(forward_columns, first, width))

        @block
        def _():
            window_gains(valid, width)
            turn_in(0)
            final[2][step * 8 : step * 8 + 8, :] = residues()

        for chunk in range(chunks):

            @block
            def _():
                if chunk + 1 < chunks:
                    turn_in(chunk + 1)
                windows(chunk, 0)
                windows(chunk, 1)
                if chunk:
                    turn_out(chunk - 1)

        block(lambda: turn_out(chunks - 1))
        run(chunks, functools.partial(inverse_columns, first, width, last))

    spill = []
    for part in range(2):
        for g in range(2):
            base = part * 304 + g
            rows = []
            for b in range(8):
                for s in (0, 8):
                    at = pl.ds(base + s * 19 + 2 * b, 8, stride=19)
                    rows.append(final[0][at, :] + final[1][at, :])
            turned = jnp.concatenate(rows, axis=0).T
            for a in range(16):
                at = a * OUT_ROWS + part * 16 + g * 8
                out_ref[at : at + 8, :] = turned[a * 8 : a * 8 + 8]
            spill += [final[1][pl.ds(base + s * 19 + 16, 8, stride=19), :] for s in (0, 8)]
    turned = jnp.concatenate(spill + spill, axis=0).T
    report = zero[0:1]
    for step in range(ITERS):
        total = jnp.sum(final[2][step * 8 : step * 8 + 8, :])
        report = jnp.where(lane[0:1] == step * 16 + tile, total, report)
    for a in range(16):
        value = turned[a * 8 : a * 8 + 8]
        out_ref[a * OUT_ROWS + 32 : a * OUT_ROWS + 36, :] = jnp.where(lane[0:4] < 64, value[0:4], value[4:8])
        out_ref[a * OUT_ROWS + 36 : a * OUT_ROWS + 37, :] = report


def filter_columns(data):
    def rows(count):
        return pltpu.VMEM((count, LANES), jnp.float32)

    return pl.pallas_call(
        column_kernel,
        out_shape=jax.ShapeDtypeStruct((16 * OUT_ROWS, LANES), jnp.float32),
        in_specs=[pl.BlockSpec(memory_space=pltpu.VMEM)],
        out_specs=pl.BlockSpec(memory_space=pltpu.VMEM),
        scratch_shapes=[rows(16 * PITCH)] * 2
        + [rows(776)] * 4
        + [rows(520)] * 2
        + [rows(80), rows(544)]
        + ([rows(296)] * 2 + [rows(280)] * 4) * 2
        + [rows(624), rows(624), rows(ITERS * 8)],
        compiler_params=pltpu.CompilerParams(vmem_limit_bytes=16 << 20),
        name="filter_columns",
    )(data)


def finish_kernel(scale, in_ref, field_ref, profile_ref):
    lane = lax.broadcasted_iota(jnp.int32, (8, LANES), 1)
    extras = []
    sums = jnp.zeros((1, LANES), jnp.float32)
    for c in range(16):
        half = in_ref[c * OUT_ROWS + 32 : c * OUT_ROWS + 36, :]
        extras.append(jnp.concatenate([half, pltpu.roll(half, 64, 1)], axis=0))
        sums = sums + in_ref[c * OUT_ROWS + 36 : c * OUT_ROWS + 37, :]
    for step in range(ITERS):
        profile_ref[step : step + 1, :] = sums[:, step * 16 : step * 16 + 16] * scale
    for part in range(2):
        for g in range(2):
            offset = (part * 2 + g) * 16
            for c in range(16):
                at = c * OUT_ROWS + part * 16 + g * 8
                value = in_ref[at : at + 8, :]
                if c:
                    spill = pltpu.roll(extras[c - 1], LANES - offset, 1) if offset else extras[c - 1]
                    value = value + jnp.where(lane < 16, spill, 0.0)
                field_ref[part, g * 8 : g * 8 + 8, c * LANES : (c + 1) * LANES] = value


def finish(scale, data):
    return pl.pallas_call(
        functools.partial(finish_kernel, scale),
        out_shape=(
            jax.ShapeDtypeStruct((2, 16, 16 * LANES), jnp.float32),
            jax.ShapeDtypeStruct((ITERS, 16), jnp.float32),
        ),
        in_specs=[pl.BlockSpec(memory_space=pltpu.VMEM)],
        out_specs=[pl.BlockSpec(memory_space=pltpu.VMEM)] * 2,
        compiler_params=pltpu.CompilerParams(vmem_limit_bytes=8 << 20),
        name="finish",
    )(data)


def ring_of_blocks(phase, devices, blocks, tiles):
    per_tile = LANES // devices
    ring = tiles * per_tile
    width = phase.shape[1]
    padded = jnp.pad(phase, ((0, 0), (HALO * 16, (ring + HALO) * 16)))
    pieces = []
    for d in range(devices):
        start = d * blocks * 16
        ahead = padded[:, start + HALO * 16 : start + (blocks + 2 * HALO) * 16]
        behind = padded[:, start : start + HALO * 16]
        gap = jnp.zeros((16, (ring - blocks - 2 * HALO) * 16), phase.dtype)
        pieces.append(jnp.concatenate([ahead, gap, behind], axis=1))
    return jnp.stack(pieces)


def per_device(phase):
    devices = lax.axis_size("rows")
    height, width = phase.shape
    blocks = width // (16 * devices)
    per_tile = LANES // devices
    if height != 16 or LANES % devices or blocks * 16 * devices != width or blocks != per_tile:
        raise ValueError("unsupported sizes")
    scale = 1.0 / (height * devices * 128.0)
    if devices == 16:
        data = lax.all_to_all(pack(phase).reshape(16, IN_ROWS, 1, LANES), "rows", 0, 0)
        result = filter_columns(data.reshape(16 * IN_ROWS, LANES))
        result = lax.all_to_all(result.reshape(16, OUT_ROWS, 1, LANES), "rows", 0, 0)
        result = result.reshape(16 * OUT_ROWS, LANES)
        return finish(scale, result)
    tiles = -(-(blocks + 2 * HALO) // per_tile)
    data = lax.all_to_all(ring_of_blocks(phase, devices, blocks, tiles), "rows", 0, 0)
    data = data.reshape(devices, 16, tiles, per_tile, 16).transpose(2, 4, 1, 3, 0)
    result = filter_tiles(devices, blocks, tiles, data.reshape(tiles, 16, 16, LANES))
    field = result[:32].reshape(2, 16, 16, per_tile, devices).transpose(4, 0, 2, 3, 1)
    field = field.reshape(devices, 32, per_tile * 16)
    sums = jnp.broadcast_to(result[32, :ITERS, : per_tile * 16][None], (devices, ITERS, per_tile * 16))
    result = lax.all_to_all(jnp.concatenate([field, sums], axis=1), "rows", 0, 0)
    field = result[:, :32].reshape(devices, 2, 16, per_tile * 16).transpose(1, 2, 0, 3).reshape(2, 16, width)
    profile = result[:, 32:, 0].reshape(width // 128, -1, ITERS).sum(1).T
    return field, profile * scale


def solution(mesh):
    return jax.shard_map(
        per_device,
        mesh=mesh,
        in_specs=(P(("groups", "rows"), None),),
        out_specs=(P(None, ("groups", "rows"), None), P("groups", None)),
        check_vma=False,
    )
```

```python
import functools
import math

import jax
import jax.numpy as jnp
from jax import lax
from jax.experimental import pallas as pl
from jax.experimental.pallas import tpu as pltpu
from jax.sharding import PartitionSpec as P

ITERS = 3
EPS = 1e-06
LANES = 128
IN_ROWS = 26
OUT_ROWS = 37
PITCH = 41
HALO = 3

SIN = (9.99999996e-01, -1.66666580e-01, 8.33305053e-03, -1.98090400e-04, 2.60515161e-06)
COS = (9.99999953e-01, -4.99999050e-01, 4.16635780e-02, -1.38536600e-03, 2.31530144e-05)


def rotated(value, k, size, sign):
    re, im = value
    half = math.sqrt(0.5)
    if k == 0:
        return re, im
    if 4 * k == size:
        return (im, -re) if sign < 0 else (-im, re)
    if 8 * k == size:
        return ((re + im) * half, (im - re) * half) if sign < 0 else ((re - im) * half, (im + re) * half)
    if 8 * k == 3 * size:
        return ((im - re) * half, (re + im) * -half) if sign < 0 else ((re + im) * -half, (re - im) * half)
    if 2 * k > size:
        return rotated((-re, -im), k - size // 2, size, sign)
    c = math.cos(2 * math.pi * k / size)
    s = sign * math.sin(2 * math.pi * k / size)
    return re * c - im * s, im * c + re * s


def plus(a, b):
    return a[0] + b[0], a[1] + b[1]


def minus(a, b):
    return a[0] - b[0], a[1] - b[1]


def quarter_turn(a, sign):
    return (-a[1], a[0]) if sign > 0 else (a[1], -a[0])


def join(one, three, size, sign):
    quarter = size // 4
    one = [rotated(one[k], k, size, sign) for k in range(quarter)]
    three = [rotated(three[k], 3 * k, size, sign) for k in range(quarter)]
    turned = [quarter_turn(minus(a, b), sign) for a, b in zip(one, three)]
    return [plus(a, b) for a, b in zip(one, three)] + turned


def fft(values, sign):
    size = len(values)
    if size == 1:
        return values
    if size == 2:
        return [plus(*values), minus(*values)]
    even = fft(values[0::2], sign)
    odd = join(fft(values[1::4], sign), fft(values[3::4], sign), size, sign)
    return [plus(e, o) for e, o in zip(even, odd)] + [minus(e, o) for e, o in zip(even, odd)]


def odd_outputs(differences):
    one = []
    three = []
    for k in range(8):
        turned = quarter_turn(differences[k + 8], -1)
        one.append(rotated(plus(differences[k], turned), k, 32, -1))
        three.append(rotated(minus(differences[k], turned), 3 * k, 32, -1))
    pairs = zip(fft(one, -1), fft(three, -1))
    return [value for pair in pairs for value in pair]


def polynomial(coefficients, w):
    result = jnp.full_like(w, coefficients[-1])
    for c in coefficients[-2::-1]:
        result = result * w + c
    return result


def cos_sin(x):
    u = (jnp.abs(x) - jnp.float32(math.pi / 2)) + jnp.float32(4.371139e-08)
    w = u * u
    cosine = -(u * polynomial(SIN, w))
    sine = polynomial(COS, w)
    return cosine, jnp.where(x < 0, -sine, sine)


def ramp(t):
    return 1.0 - abs(t - 15.5) / 16.0


def filter_kernel(
    slabs, blocks, tiles, in_ref, out_ref, zr, zi, yr, yi, ur, ui, vr, vi, wr, wi, pr, pi, qr, qi, energy, gain, sums
):
    tile = lax.axis_index("rows")
    per_tile = LANES // slabs
    ring = tiles * per_tile
    lane = lax.broadcasted_iota(jnp.int32, (8, LANES), 1)
    sub = lax.broadcasted_iota(jnp.int32, (8, LANES), 0)
    not_last = lane % slabs != slabs - 1
    not_first = lane % slabs != 0
    place = lane // slabs

    def inside(h, step):
        position = (h * per_tile + place + step) % ring
        relative = jnp.where(position < blocks + HALO, position, position - ring)
        column = tile * blocks + relative
        return jnp.where((column >= 0) & (column < slabs * blocks), 1.0, 0.0)

    here = [inside(h, 0) for h in range(tiles)]
    both = [here[h] * inside(h, 1) for h in range(tiles)]

    def right(values, active):
        if per_tile == 1:
            return [values[(h + 1) % tiles] for h in active]
        moved = [pltpu.roll(v, LANES - slabs, 1) for v in values]
        return [jnp.where(lane < LANES - slabs, moved[h], moved[(h + 1) % tiles]) for h in active]

    def left(values):
        if per_tile == 1:
            return [values[h - 1] for h in range(tiles)]
        moved = [pltpu.roll(v, slabs, 1) for v in values]
        return [jnp.where(lane < slabs, moved[h - 1], moved[h]) for h in range(tiles)]

    def below(value):
        return jnp.where(not_last, pltpu.roll(value, LANES - 1, 1), 0.0)

    def above(value):
        return jnp.where(not_first, pltpu.roll(value, 1, 1), 0.0)

    def keep(h, s, g, value, power):
        for part, ref in enumerate((zr, zi)):
            ref[h * 16 + s, pl.ds(g * 8, 8), :] = value[part]
            if h == 0 or s == 0:
                ref[h * 16 + s, pl.ds(16 + g, 1), :] = below(value[part])[0:1]
        return power + (value[0] * value[0] + value[1] * value[1])

    for h in range(tiles):
        for g in range(2):
            phases = [in_ref[h, s, g * 8 : g * 8 + 8, :] for s in range(16)]
            power = jnp.zeros((8, LANES), jnp.float32)
            for s in range(16):
                cosine, sine = cos_sin(phases[s])
                power = keep(h, s, g, (cosine * here[h], sine * here[h]), power)
            energy[h * 16 + g * 8 : h * 16 + g * 8 + 8, :] = power

    def sharing(h, needed):
        places = {w % ring - h * per_tile for w in needed}
        places = {p for p in places if 0 <= p < per_tile}
        group = 1
        for k in (2, 4):
            if per_tile % k == 0:
                taken = {(p + j * (per_tile // k)) % per_tile for p in places for j in range(k)}
                group = k if len(taken) == k * len(places) else group
        masks = []
        for k in range(1, group):
            mask = place < 0
            for p in places:
                mask = mask | (place == (p + k * (per_tile // group)) % per_tile)
            masks.append(mask)
        return masks

    def merged(values, masks):
        result = values[0]
        for k, mask in enumerate(masks):
            result = jnp.where(mask, pltpu.roll(values[k + 1], (k + 1) * LANES // (len(masks) + 1), 1), result)
        return result

    def window_gains(plans):
        both_rows = [energy[h * 16 : h * 16 + 8, :] + energy[h * 16 + 8 : h * 16 + 16, :] for h in range(tiles)]
        blockwise = [jnp.broadcast_to(jnp.sum(e, axis=0, keepdims=True), (8, LANES)) for e in both_rows]
        tall = [e + below(e) for e in blockwise]
        for unit, ((h, masks, first, count), wide) in enumerate(zip(plans, right(tall, [p[0] for p in plans]))):
            value = merged([1.0 / ((tall[h] + wide) + EPS)] * 4, masks)
            for j in range(count):
                gain[(first + j) * 8 : (first + j) * 8 + 8, :] = value

    def forward_columns(step, plans, g):
        rows = pl.ds(pl.multiple_of(g * 8, 8), 8)
        under = pl.ds(g * 8 + 1, 8)
        active = [p[0] for p in plans]
        window_gains(plans)
        near = {h: [] for h in active}
        far = {h: [] for h in active}
        for s in range(16):
            re = [zr[h * 16 + s, rows, :] for h in range(tiles)]
            im = [zi[h * 16 + s, rows, :] for h in range(tiles)]
            for h, a, b in zip(active, right(re, active), right(im, active)):
                near[h].append((re[h], im[h]))
                far[h].append((a, b))
        for h, masks, first, count in plans:
            group = len(masks) + 1
            even = fft([plus(a, b) for a, b in zip(near[h], far[h])], -1)
            odd = fft([rotated(minus(a, b), s, 32, -1) for s, (a, b) in enumerate(zip(near[h], far[h]))], -1)
            for row in range(8 * count):
                sources = [(row // 8 * group + k) * 8 + row % 8 for k in range(group)]
                values = [(even, odd)[l % 2][l // 2] for l in sources]
                value = tuple(merged([v[part] for v in values], masks) for part in range(2))
                at = pl.ds((first * 8 + row) * 17 + g * 8, 8)
                if first == 0 and row < 8:
                    following = (below(value[0]), below(value[1]))
                    ur[at, :], ui[at, :] = plus(value, following)
                    vr[at, :], vi[at, :] = minus(value, following)
                else:
                    yr[at, :], yi[at, :] = value

        def corner(s):
            if s < 16:
                return near[0][s], (zr[s, under, :], zi[s, under, :])
            moved = [right([ref[h * 16, under, :] for h in range(tiles)], (0,))[0] for ref in (zr, zi)]
            return far[0][0], tuple(moved)

        def cross(a, b):
            return a[1] * b[0] - a[0] * b[1]

        total = jnp.zeros((8, LANES), jnp.float32)
        here_, under_ = corner(0)
        down = cross(here_, under_)
        for s in range(16):
            next_, next_under = corner(s + 1)
            next_down = cross(next_, next_under)
            loop = (cross(here_, next_) - cross(under_, next_under)) + (next_down - down)
            total = total + loop * loop
            here_, under_, down = next_, next_under, next_down
        sums[pl.ds(pl.multiple_of(step * 16 + g * 8, 8), 8), :] = total

    def split_rows(unit):
        for row in range(8):
            for g in range(2):
                source = pl.ds((unit * 8 + row) * 17 + g * 8, 8)
                at = pl.ds(row * 17 + g * 8, 8)
                value = (yr[source, :], yi[source, :])
                following = (below(value[0]), below(value[1]))
                ur[at, :], ui[at, :] = plus(value, following)
                vr[at, :], vi[at, :] = minus(value, following)

    def join_rows(unit):
        for t in range(16):
            source = pl.ds(t * 9, 8)
            at = pl.ds((unit * 16 + t) * 9, 8)
            wr[at, :] = pr[source, :] + above(qr[source, :])
            wi[at, :] = pi[source, :] + above(qi[source, :])

    def windows(unit):
        join_rows(jnp.maximum(unit - 1, 0))
        scale = gain[pl.ds(pl.multiple_of(unit * 8, 8), 8), :]
        at = [pl.ds(t, 8, stride=17) for t in range(16)]
        back = []
        for parity, (a, b) in enumerate(((ur, ui), (vr, vi))):
            values = [(a[x, :], b[x, :]) for x in at]
            if parity:
                values = [rotated(v, t, 32, -1) for t, v in enumerate(values)]
            filtered = []
            for re, im in fft(values, -1):
                factor = lax.rsqrt(lax.rsqrt((re * re + im * im) * scale))
                filtered.append((re * factor, im * factor))
            back.append(fft(filtered, 1))
        split_rows(unit + 1)
        for t in range(16):
            odd = rotated(back[1][t], t, 32, 1)
            upper = plus(back[0][t], odd)
            lower = minus(back[0][t], odd)
            at = pl.ds(t * 9, 8)
            pr[at, :], pi[at, :] = (v * (ramp(t) / 32) for v in upper)
            qr[at, :], qi[at, :] = (v * (ramp(t + 16) / 32) for v in lower)

    def inverse_columns(plans, units, g):
        rows = pl.ds(pl.multiple_of(g * 8, 8), 8)
        kept = []
        passed = []
        for h, masks, first, count in plans:
            group = len(masks) + 1
            values = [None] * 32
            for row in range(8 * count):
                unit = first + row // 8
                if unit == units - 1:
                    at = pl.ds(g * 72 + row % 8, 8, stride=9)
                    value = (pr[at, :] + above(qr[at, :]), pi[at, :] + above(qi[at, :]))
                else:
                    at = pl.ds(unit * 144 + g * 72 + row % 8, 8, stride=9)
                    value = (wr[at, :], wi[at, :])
                for k in range(group):
                    l = (row // 8 * group + k) * 8 + row % 8
                    values[l] = tuple(pltpu.roll(v, LANES - k * LANES // group, 1) if k else v for v in value)
            even = fft(values[0::2], 1)
            odd = fft(values[1::2], 1)
            own = []
            other = []
            for s in range(16):
                turned = rotated(odd[s], s, 32, 1)
                weight = here[h] * (ramp(s) / 32)
                own.append(tuple(v * weight for v in plus(even[s], turned)))
                weight = both[h] * (ramp(s + 16) / 32)
                other.append(tuple(v * weight for v in minus(even[s], turned)))
            kept.append(own)
            passed.append(other)
        power = [jnp.zeros((8, LANES), jnp.float32) for _ in range(tiles)]
        for s in range(16):
            arrived = [left([passed[h][s][part] for h in range(tiles)]) for part in range(2)]
            for h in range(tiles):
                value = tuple(kept[h][s][part] + arrived[part][h] for part in range(2))
                power[h] = keep(h, s, g, value, power[h])
        for h in range(tiles):
            energy[pl.ds(pl.multiple_of(h * 16 + g * 8, 8), 8), :] = power[h]

    def run(count, body):
        lax.fori_loop(0, count, lambda i, c: (body(i), c)[1], 0)

    for step in range(ITERS):
        needed = range(step - ITERS, blocks + ITERS - 1 - step)
        plans = []
        units = 0
        for h in range(tiles):
            masks = sharing(h, needed)
            plans.append((h, masks, units, 4 // (len(masks) + 1)))
            units += 4 // (len(masks) + 1)
        run(2, functools.partial(forward_columns, step, plans))
        run(units, windows)
        run(2, functools.partial(inverse_columns, plans, units))
    totals = [jnp.sum(sums[step * 16 : step * 16 + 8, :] + sums[step * 16 + 8 : step * 16 + 16, :]) for step in range(ITERS)]

    for step, total in enumerate(totals):
        out_ref[32, step : step + 1, :] = jnp.full((1, LANES), total)
    for part, ref in enumerate((zr, zi)):
        for s in range(16):
            out_ref[part * 16 + s, :, :] = ref[s, 0:16, :]


def filter_tiles(slabs, blocks, tiles, data):
    body = functools.partial(filter_kernel, slabs, blocks, tiles)
    return pl.pallas_call(
        body,
        out_shape=jax.ShapeDtypeStruct((33, 16, LANES), jnp.float32),
        in_specs=[pl.BlockSpec(memory_space=pltpu.VMEM)],
        out_specs=pl.BlockSpec(memory_space=pltpu.VMEM),
        scratch_shapes=[pltpu.VMEM((tiles * 16, 24, LANES), jnp.float32)] * 2
        + [pltpu.VMEM(((tiles * 4 + 1) * 136, LANES), jnp.float32)] * 2
        + [pltpu.VMEM((136, LANES), jnp.float32)] * 4
        + [pltpu.VMEM((tiles * 4 * 144, LANES), jnp.float32)] * 2
        + [pltpu.VMEM((144, LANES), jnp.float32)] * 4
        + [pltpu.VMEM((rows, LANES), jnp.float32) for rows in (tiles * 16, tiles * 32, ITERS * 16)],
        compiler_params=pltpu.CompilerParams(vmem_limit_bytes=16 << 20),
        name="filter_tiles",
    )(data)


def pack_kernel(in_ref, out_ref, turn):
    lane = lax.broadcasted_iota(jnp.int32, (8, LANES), 1)
    zero = jnp.zeros((8, LANES), jnp.float32)
    columns = [[in_ref[g * 8 : g * 8 + 8, c * LANES : (c + 1) * LANES] for g in range(2)] for c in range(16)]
    for c in range(16):
        after = columns[c + 1] if c < 15 else [zero, zero]
        before = columns[c - 1] if c else [zero, zero]
        at = c * IN_ROWS
        out_ref[at : at + 8, :] = columns[c][0]
        out_ref[at + 8 : at + 16, :] = columns[c][1]
        first = jnp.where(lane < 32, after[0], pltpu.roll(before[0], 64, 1))
        second = jnp.where(lane < 96, pltpu.roll(after[1], 64, 1), before[1])
        out_ref[at + 16 : at + 24, :] = jnp.where(lane < 64, first, second)
        turn[c * 8 : c * 8 + 8, :] = jnp.where(lane < 16, pltpu.roll(after[0], 96, 1), pltpu.roll(after[1], 112, 1))
    for q in range(4):
        rows = turn[pl.ds(q * 32, 8, stride=4), :]
        for u in range(1, 4):
            rows = jnp.where(lane // 32 == u, pltpu.roll(turn[pl.ds(q * 32 + u, 8, stride=4), :], 32 * u, 1), rows)
        for k in range(4):
            at = (q * 4 + k) * IN_ROWS + 24
            out_ref[at : at + 2, :] = rows[k * 2 : k * 2 + 2]


def pack(phase):
    return pl.pallas_call(
        pack_kernel,
        out_shape=jax.ShapeDtypeStruct((16 * IN_ROWS, LANES), jnp.float32),
        in_specs=[pl.BlockSpec(memory_space=pltpu.VMEM)],
        out_specs=pl.BlockSpec(memory_space=pltpu.VMEM),
        scratch_shapes=[pltpu.VMEM((128, LANES), jnp.float32)],
        compiler_params=pltpu.CompilerParams(vmem_limit_bytes=8 << 20),
        name="pack",
    )(phase)


def column_kernel(in_ref, out_ref, *scratch):
    zr, zi, yr, yi, wr, wi, shift_r, shift_i, gain, turn = scratch[:10]
    buffers = [scratch[10 + 6 * k : 16 + 6 * k] for k in range(2)]
    final = scratch[22:25]
    tile = lax.axis_index("rows")
    lane = lax.broadcasted_iota(jnp.int32, (8, LANES), 1)
    sub = lax.broadcasted_iota(jnp.int32, (8, LANES), 0)
    in_slab = lane & 7

    def inside(first):
        column = tile * 8 + (first - 2) + sub // 2
        return jnp.where((column >= 0) & (column < 128), 1.0, 0.0)

    def block(body):
        pl.when(tile >= 0)(body)

    def run(count, body):
        lax.fori_loop(0, count, lambda i, c: (body(i), c)[1], 0)

    zero = jnp.zeros((8, LANES), jnp.float32)
    for vr, vi, pr, pi, qr, qi in buffers:
        for ref in (vr, vi):
            for row in (272, 280, 288):
                ref[row : row + 8, :] = zero
        for ref in (qr, qi):
            for t in range(16):
                ref[t * 17 : t * 17 + 1, :] = zero[0:1]

    def stacked(offset):
        return jnp.concatenate([in_ref[a * IN_ROWS + offset : a * IN_ROWS + offset + 8, :] for a in range(16)], axis=0)

    for k, offset in enumerate((0, 8, 16)):
        turned = stacked(offset).T
        for b in range(8):
            at = k * 136 + (b % 4 * 2 + b // 4 if k == 2 else b) * 17
            turn[at : at + 16, :] = turned[b * 16 : b * 16 + 16]
    tail = jnp.concatenate([in_ref[a * IN_ROWS + 24 : a * IN_ROWS + 26, :] for a in range(16)], axis=0)
    for q in range(4):
        for u in range(4):
            value = tail[q * 8 : q * 8 + 8]
            turn[pl.ds(408 + q * 32 + u, 8, stride=4), :] = pltpu.roll(value, LANES - 32 * u, 1) if u else value
    turned = turn[408:536, :].T[0:32]
    beyond = jnp.where(tile * 8 + 10 < 128, 1.0, 0.0)
    for ref, v in zip((zr, zi), cos_sin(turned)):
        for k in range(4):
            at = (k % 2) * 8 * PITCH + 24 + k // 2
            ref[pl.ds(at, 8, stride=PITCH), :] = v[k * 8 : k * 8 + 8] * beyond
    for g in range(2):
        for s in range(16):
            value = cos_sin(turn[pl.ds(g * 136 + s, 8, stride=17), :])
            for ref, v in zip((zr, zi), value):
                ref[pl.ds(s * PITCH + 4 + g, 8, stride=2), :] = v
    edge = tile * 8 + jnp.where(sub < 4, 8 + sub // 2, sub // 2 - 4)
    edge = jnp.where((edge >= 0) & (edge < 128), 1.0, 0.0)
    for s in range(16):
        value = cos_sin(turn[pl.ds(272 + s, 8, stride=17), :])
        for ref, v in zip((zr, zi), value):
            v = v * edge
            ref[s * PITCH + 20 : s * PITCH + 24, :] = v[0:4]
            ref[s * PITCH : s * PITCH + 4, :] = v[4:8]

    def forward_columns(first, width, j):
        near = []
        far = []
        power = zero
        for s in range(16):
            at = pl.ds(s * PITCH + 2 * first + j * 8, 8)
            after = pl.ds(s * PITCH + 2 * first + 2 + j * 8, 8)
            near.append((zr[at, :], zi[at, :]))
            far.append((zr[after, :], zi[after, :]))
            a, b = near[-1], far[-1]
            power = power + ((a[0] * a[0] + a[1] * a[1]) + (b[0] * b[0] + b[1] * b[1]))
        gain[pl.ds(pl.multiple_of(48 + j * 8, 8), 8), :] = power
        even = fft([plus(a, b) for a, b in zip(near, far)], -1)
        odd = odd_outputs([minus(a, b) for a, b in zip(near, far)])
        for l in range(32):
            to = pl.ds(l * 2 * width + j * 8, 8)
            yr[to, :], yi[to, :] = (even, odd)[l % 2][l // 2]

    def turn_in(chunk):
        vr, vi = buffers[chunk % 2][:2]
        for source, ref in ((yr, vr), (yi, vi)):
            for g in range(2):
                parts = [source[pl.ds(chunk * 256 + i * 16 + g, 8, stride=2), :] for i in range(16)]
                turned = jnp.concatenate(parts, axis=0).T
                for a in range(16):
                    ref[a * 17 + g * 8 : a * 17 + g * 8 + 8, :] = turned[a * 8 : a * 8 + 8]

    def turn_out(chunk):
        pr, pi, qr, qi = buffers[chunk % 2][2:]
        for p, q, target in ((pr, qr, wr), (pi, qi, wi)):
            for g in range(2):
                parts = []
                for a in range(16):
                    at = pl.ds(g * 136 + a, 8, stride=17)
                    parts.append(p[at, :] + q[at, :])
                turned = jnp.concatenate(parts, axis=0).T
                for i in range(16):
                    target[pl.ds(chunk * 256 + i * 16 + g, 8, stride=2), :] = turned[i * 8 : i * 8 + 8]

    def window_gains(valid, width):
        count = 2 * width
        power = jnp.concatenate(
            [jnp.where(sub < 2 * valid - 8 * j, gain[48 + j * 8 : 56 + j * 8, :], 0.0) for j in range(count // 8)], axis=0
        )
        row = lax.broadcasted_iota(jnp.int32, (16, LANES), 0)
        slab = lax.broadcasted_iota(jnp.int32, (16, LANES), 1) // 8
        pick = jnp.where((slab == row) | (slab == row + 1), 1.0, 0.0)
        exact = dict(precision=lax.Precision.HIGHEST, preferred_element_type=jnp.float32)
        mean = lax.dot_general(pick, power, (((1,), (1,)), ((), ())), **exact)
        column = lax.broadcasted_iota(jnp.int32, (count, 32 * width), 1)
        column = column - width * ((column.astype(jnp.float32) + 0.5) * (1.0 / width)).astype(jnp.int32)
        spread = jnp.where(column == lax.broadcasted_iota(jnp.int32, (count, 32 * width), 0) // 2, 1.0, 0.0)
        mean = lax.dot_general(mean, spread, (((1,), (0,)), ((), ())), **exact)
        for c in range(width // 4):
            gain[c * 16 : c * 16 + 16, :] = 1.0 / (mean[:, c * 128 : c * 128 + 128] + EPS)

    def residues():
        def corner(s):
            at = s * PITCH + 4 if s < 16 else 6
            result = []
            for ref in (zr, zi):
                top = ref[pl.ds(at, 8, stride=2), :]
                low = ref[pl.ds(at + 1, 8, stride=2), :]
                top_left = pltpu.roll(top, LANES - 1, 1)
                low_left = pltpu.roll(low, LANES - 1, 1)
                top_under = jnp.where(in_slab < 7, top_left, pltpu.roll(low, 7, 1))
                low_under = jnp.where(in_slab < 7, low_left, jnp.where(lane < LANES - 1, top_left, 0.0))
                result.append((top, low, top_under, low_under))
            return [((result[0][g], result[1][g]), (result[0][2 + g], result[1][2 + g])) for g in range(2)]

        def cross(a, b):
            return a[1] * b[0] - a[0] * b[1]

        total = zero
        here = corner(0)
        down = [cross(*pair) for pair in here]
        for s in range(16):
            following = corner(s + 1)
            following_down = [cross(*pair) for pair in following]
            for g in range(2):
                across = cross(here[g][0], following[g][0]) - cross(here[g][1], following[g][1])
                loop = across + (following_down[g] - down[g])
                total = total + loop * loop
            here, down = following, following_down
        return total

    def windows(chunk, half):
        vr, vi, pr, pi, qr, qi = buffers[chunk % 2]
        scale = gain[chunk * 16 + half * 8 : chunk * 16 + half * 8 + 8, :]
        sums = []
        differences = []
        for t in range(16):
            at = pl.ds(half * 136 + t, 8, stride=17)
            after = pl.ds(half * 136 + 17 + t, 8, stride=17)
            near = (vr[at, :], vi[at, :])
            far = (vr[after, :], vi[after, :])
            sums.append(plus(near, far))
            differences.append(minus(near, far))
        back = []
        for spectrum in (lambda: fft(sums, -1), lambda: odd_outputs(differences)):
            filtered = []
            for re, im in spectrum():
                factor = lax.rsqrt(lax.rsqrt((re * re + im * im) * scale))
                filtered.append((re * factor, im * factor))
            back.append(filtered)
        back = fft(back[0], 1), join(fft(back[1][0::2], 1), fft(back[1][1::2], 1), 32, 1)
        for t in range(16):
            upper = plus(back[0][t], back[1][t])
            lower = minus(back[0][t], back[1][t])
            at = pl.ds(t * 17 + half * 8, 8)
            pr[at, :], pi[at, :] = (v * (ramp(t) / 32) for v in upper)
            at = pl.ds(t * 17 + half * 8 + 1, 8)
            qr[at, :], qi[at, :] = (v * (ramp(t + 16) / 32) for v in lower)

    def inverse_columns(first, width, last, j):
        here = inside(first + 4 * j)
        both = here * inside(first + 4 * j + 1)
        values = []
        for l in range(32):
            at = pl.ds(l * 2 * width + 8 * j, 8)
            values.append((wr[at, :], wi[at, :]))
        even = fft(values[0::2], 1)
        odd = join(fft(values[1::4], 1), fft(values[3::4], 1), 32, 1)
        for s in range(16):
            weight = here * (ramp(s) / 32)
            own = [v * weight for v in plus(even[s], odd[s])]
            weight = both * (ramp(s + 16) / 32)
            other = [v * weight for v in minus(even[s], odd[s])]
            for part, (ref, shift) in enumerate(((zr, shift_r), (zi, shift_i))):
                if last:
                    base = part * 304 + s * 19 + 8 * j
                    final[0][pl.ds(base, 8), :] = own[part]
                    final[1][pl.ds(base + 2, 8), :] = other[part]
                else:
                    shift[pl.ds(s * 32 + 8 * j + 2, 8), :] = other[part]
                    value = own[part] + shift[pl.ds(s * 32 + 8 * j, 8), :]
                    ref[pl.ds(s * PITCH + 2 * first + 8 * j, 8), :] = value

    for k in range(32):
        final[1][k * 19 : k * 19 + 2, :] = zero[0:2]

    def iteration(step, width, last):
        chunks = width // 4
        run(chunks, functools.partial(forward_columns, step, width))

        @block
        def _():
            window_gains(12 - 2 * step, width)
            turn_in(0)
            final[2][pl.ds(step * 8, 8), :] = residues()

        for chunk in range(chunks):

            @block
            def _():
                if chunk + 1 < chunks:
                    turn_in(chunk + 1)
                windows(chunk, 0)
                windows(chunk, 1)
                if chunk:
                    turn_out(chunk - 1)

        block(lambda: turn_out(chunks - 1))
        run(chunks, functools.partial(inverse_columns, step, width, last))

    run(ITERS - 1, lambda step: iteration(step, 12, False))
    iteration(ITERS - 1, 8, True)

    spill = []
    for part in range(2):
        for g in range(2):
            base = part * 304 + g
            rows = []
            for b in range(8):
                for s in (0, 8):
                    at = pl.ds(base + s * 19 + 2 * b, 8, stride=19)
                    rows.append(final[0][at, :] + final[1][at, :])
            turned = jnp.concatenate(rows, axis=0).T
            for a in range(16):
                at = a * OUT_ROWS + part * 16 + g * 8
                out_ref[at : at + 8, :] = turned[a * 8 : a * 8 + 8]
            spill += [final[1][pl.ds(base + s * 19 + 16, 8, stride=19), :] for s in (0, 8)]
    turned = jnp.concatenate(spill + spill, axis=0).T
    report = zero[0:1]
    for step in range(ITERS):
        total = jnp.sum(final[2][step * 8 : step * 8 + 8, :])
        report = jnp.where(lane[0:1] == step * 16 + tile, total, report)
    for a in range(16):
        value = turned[a * 8 : a * 8 + 8]
        out_ref[a * OUT_ROWS + 32 : a * OUT_ROWS + 36, :] = jnp.where(lane[0:4] < 64, value[0:4], value[4:8])
        out_ref[a * OUT_ROWS + 36 : a * OUT_ROWS + 37, :] = report


def filter_columns(data):
    def rows(count):
        return pltpu.VMEM((count, LANES), jnp.float32)

    return pl.pallas_call(
        column_kernel,
        out_shape=jax.ShapeDtypeStruct((16 * OUT_ROWS, LANES), jnp.float32),
        in_specs=[pl.BlockSpec(memory_space=pltpu.VMEM)],
        out_specs=pl.BlockSpec(memory_space=pltpu.VMEM),
        scratch_shapes=[rows(16 * PITCH)] * 2
        + [rows(776)] * 4
        + [rows(520)] * 2
        + [rows(80), rows(544)]
        + ([rows(296)] * 2 + [rows(280)] * 4) * 2
        + [rows(624), rows(624), rows(ITERS * 8)],
        compiler_params=pltpu.CompilerParams(vmem_limit_bytes=16 << 20),
        name="filter_columns",
    )(data)


def finish_kernel(scale, in_ref, field_ref, profile_ref, rows, sent):
    lane = lax.broadcasted_iota(jnp.int32, (8, LANES), 1)
    extras = []
    sums = jnp.zeros((1, LANES), jnp.float32)
    for c in range(16):
        half = in_ref[c * OUT_ROWS + 32 : c * OUT_ROWS + 36, :]
        extras.append(jnp.concatenate([half, pltpu.roll(half, 64, 1)], axis=0))
        sums = sums + in_ref[c * OUT_ROWS + 36 : c * OUT_ROWS + 37, :]
    for step in range(ITERS):
        profile_ref[step : step + 1, :] = sums[:, step * 16 : step * 16 + 16] * scale
    copies = []
    for k in range(4):
        part, g = k // 2, k % 2
        for c in range(16):
            value = in_ref[c * OUT_ROWS + k * 8 : c * OUT_ROWS + k * 8 + 8, :]
            if c:
                spill = pltpu.roll(extras[c - 1], LANES - k * 16, 1) if k else extras[c - 1]
                value = value + jnp.where(lane < 16, spill, 0.0)
            rows[k, :, c * LANES : (c + 1) * LANES] = value
        copies.append(pltpu.make_async_copy(rows.at[k], field_ref.at[part, pl.ds(g * 8, 8)], sent.at[k]))
        copies[-1].start()
    for copy in copies:
        copy.wait()


def finish(scale, data):
    return pl.pallas_call(
        functools.partial(finish_kernel, scale),
        out_shape=(
            jax.ShapeDtypeStruct((2, 16, 16 * LANES), jnp.float32),
            jax.ShapeDtypeStruct((ITERS, 16), jnp.float32),
        ),
        in_specs=[pl.BlockSpec(memory_space=pltpu.VMEM)],
        out_specs=[pl.BlockSpec(memory_space=pl.ANY), pl.BlockSpec(memory_space=pltpu.VMEM)],
        scratch_shapes=[pltpu.VMEM((4, 8, 16 * LANES), jnp.float32), pltpu.SemaphoreType.DMA((4,))],
        compiler_params=pltpu.CompilerParams(vmem_limit_bytes=8 << 20),
        name="finish",
    )(data)


def ring_of_blocks(phase, devices, blocks, tiles):
    per_tile = LANES // devices
    ring = tiles * per_tile
    width = phase.shape[1]
    padded = jnp.pad(phase, ((0, 0), (HALO * 16, (ring + HALO) * 16)))
    pieces = []
    for d in range(devices):
        start = d * blocks * 16
        ahead = padded[:, start + HALO * 16 : start + (blocks + 2 * HALO) * 16]
        behind = padded[:, start : start + HALO * 16]
        gap = jnp.zeros((16, (ring - blocks - 2 * HALO) * 16), phase.dtype)
        pieces.append(jnp.concatenate([ahead, gap, behind], axis=1))
    return jnp.stack(pieces)


def per_device(phase):
    devices = lax.axis_size("rows")
    height, width = phase.shape
    blocks = width // (16 * devices)
    per_tile = LANES // devices
    if height != 16 or LANES % devices or blocks * 16 * devices != width or blocks != per_tile:
        raise ValueError("unsupported sizes")
    scale = 1.0 / (height * devices * 128.0)
    if devices == 16:
        data = lax.all_to_all(pack(phase).reshape(16, IN_ROWS, 1, LANES), "rows", 0, 0)
        result = filter_columns(data.reshape(16 * IN_ROWS, LANES))
        result = lax.all_to_all(result.reshape(16, OUT_ROWS, 1, LANES), "rows", 0, 0)
        result = result.reshape(16 * OUT_ROWS, LANES)
        return finish(scale, result)
    tiles = -(-(blocks + 2 * HALO) // per_tile)
    data = lax.all_to_all(ring_of_blocks(phase, devices, blocks, tiles), "rows", 0, 0)
    data = data.reshape(devices, 16, tiles, per_tile, 16).transpose(2, 4, 1, 3, 0)
    result = filter_tiles(devices, blocks, tiles, data.reshape(tiles, 16, 16, LANES))
    field = result[:32].reshape(2, 16, 16, per_tile, devices).transpose(4, 0, 2, 3, 1)
    field = field.reshape(devices, 32, per_tile * 16)
    sums = jnp.broadcast_to(result[32, :ITERS, : per_tile * 16][None], (devices, ITERS, per_tile * 16))
    result = lax.all_to_all(jnp.concatenate([field, sums], axis=1), "rows", 0, 0)
    field = result[:, :32].reshape(devices, 2, 16, per_tile * 16).transpose(1, 2, 0, 3).reshape(2, 16, width)
    profile = result[:, 32:, 0].reshape(width // 128, -1, ITERS).sum(1).T
    return field, profile * scale


def solution(mesh):
    return jax.shard_map(
        per_device,
        mesh=mesh,
        in_specs=(P(("groups", "rows"), None),),
        out_specs=(P(None, ("groups", "rows"), None), P("groups", None)),
        check_vma=False,
    )
```

```python
import functools
import math

import jax
import jax.numpy as jnp
from jax import lax
from jax.experimental import pallas as pl
from jax.experimental.pallas import tpu as pltpu
from jax.sharding import PartitionSpec as P

ITERS = 3
EPS = 1e-06
LANES = 128
IN_ROWS = 26
OUT_ROWS = 37
PITCH = 41
HALO = 3

SIN = (9.99999996e-01, -1.66666580e-01, 8.33305053e-03, -1.98090400e-04, 2.60515161e-06)
COS = (9.99999953e-01, -4.99999050e-01, 4.16635780e-02, -1.38536600e-03, 2.31530144e-05)


def rotated(value, k, size, sign):
    re, im = value
    half = math.sqrt(0.5)
    if k == 0:
        return re, im
    if 4 * k == size:
        return (im, -re) if sign < 0 else (-im, re)
    if 8 * k == size:
        return ((re + im) * half, (im - re) * half) if sign < 0 else ((re - im) * half, (im + re) * half)
    if 8 * k == 3 * size:
        return ((im - re) * half, (re + im) * -half) if sign < 0 else ((re + im) * -half, (re - im) * half)
    if 2 * k > size:
        return rotated((-re, -im), k - size // 2, size, sign)
    c = math.cos(2 * math.pi * k / size)
    s = sign * math.sin(2 * math.pi * k / size)
    return re * c - im * s, im * c + re * s


def plus(a, b):
    return a[0] + b[0], a[1] + b[1]


def minus(a, b):
    return a[0] - b[0], a[1] - b[1]


def quarter_turn(a, sign):
    return (-a[1], a[0]) if sign > 0 else (a[1], -a[0])


def join(one, three, size, sign):
    quarter = size // 4
    one = [rotated(one[k], k, size, sign) for k in range(quarter)]
    three = [rotated(three[k], 3 * k, size, sign) for k in range(quarter)]
    turned = [quarter_turn(minus(a, b), sign) for a, b in zip(one, three)]
    return [plus(a, b) for a, b in zip(one, three)] + turned


def fft(values, sign):
    size = len(values)
    if size == 1:
        return values
    if size == 2:
        return [plus(*values), minus(*values)]
    even = fft(values[0::2], sign)
    odd = join(fft(values[1::4], sign), fft(values[3::4], sign), size, sign)
    return [plus(e, o) for e, o in zip(even, odd)] + [minus(e, o) for e, o in zip(even, odd)]


def odd_outputs(differences):
    one = []
    three = []
    for k in range(8):
        turned = quarter_turn(differences[k + 8], -1)
        one.append(rotated(plus(differences[k], turned), k, 32, -1))
        three.append(rotated(minus(differences[k], turned), 3 * k, 32, -1))
    pairs = zip(fft(one, -1), fft(three, -1))
    return [value for pair in pairs for value in pair]


def polynomial(coefficients, w):
    result = jnp.full_like(w, coefficients[-1])
    for c in coefficients[-2::-1]:
        result = result * w + c
    return result


def cos_sin(x):
    u = (jnp.abs(x) - jnp.float32(math.pi / 2)) + jnp.float32(4.371139e-08)
    w = u * u
    cosine = -(u * polynomial(SIN, w))
    sine = polynomial(COS, w)
    return cosine, jnp.where(x < 0, -sine, sine)


def ramp(t):
    return 1.0 - abs(t - 15.5) / 16.0


def filter_kernel(
    slabs, blocks, tiles, in_ref, out_ref, zr, zi, yr, yi, ur, ui, vr, vi, wr, wi, pr, pi, qr, qi, energy, gain, sums
):
    tile = lax.axis_index("rows")
    per_tile = LANES // slabs
    ring = tiles * per_tile
    lane = lax.broadcasted_iota(jnp.int32, (8, LANES), 1)
    sub = lax.broadcasted_iota(jnp.int32, (8, LANES), 0)
    not_last = lane % slabs != slabs - 1
    not_first = lane % slabs != 0
    place = lane // slabs

    def inside(h, step):
        position = (h * per_tile + place + step) % ring
        relative = jnp.where(position < blocks + HALO, position, position - ring)
        column = tile * blocks + relative
        return jnp.where((column >= 0) & (column < slabs * blocks), 1.0, 0.0)

    here = [inside(h, 0) for h in range(tiles)]
    both = [here[h] * inside(h, 1) for h in range(tiles)]

    def right(values, active):
        if per_tile == 1:
            return [values[(h + 1) % tiles] for h in active]
        moved = [pltpu.roll(v, LANES - slabs, 1) for v in values]
        return [jnp.where(lane < LANES - slabs, moved[h], moved[(h + 1) % tiles]) for h in active]

    def left(values):
        if per_tile == 1:
            return [values[h - 1] for h in range(tiles)]
        moved = [pltpu.roll(v, slabs, 1) for v in values]
        return [jnp.where(lane < slabs, moved[h - 1], moved[h]) for h in range(tiles)]

    def below(value):
        return jnp.where(not_last, pltpu.roll(value, LANES - 1, 1), 0.0)

    def above(value):
        return jnp.where(not_first, pltpu.roll(value, 1, 1), 0.0)

    def keep(h, s, g, value, power):
        for part, ref in enumerate((zr, zi)):
            ref[h * 16 + s, pl.ds(g * 8, 8), :] = value[part]
            if h == 0 or s == 0:
                ref[h * 16 + s, pl.ds(16 + g, 1), :] = below(value[part])[0:1]
        return power + (value[0] * value[0] + value[1] * value[1])

    for h in range(tiles):
        for g in range(2):
            phases = [in_ref[h, s, g * 8 : g * 8 + 8, :] for s in range(16)]
            power = jnp.zeros((8, LANES), jnp.float32)
            for s in range(16):
                cosine, sine = cos_sin(phases[s])
                power = keep(h, s, g, (cosine * here[h], sine * here[h]), power)
            energy[h * 16 + g * 8 : h * 16 + g * 8 + 8, :] = power

    def sharing(h, needed):
        places = {w % ring - h * per_tile for w in needed}
        places = {p for p in places if 0 <= p < per_tile}
        group = 1
        for k in (2, 4):
            if per_tile % k == 0:
                taken = {(p + j * (per_tile // k)) % per_tile for p in places for j in range(k)}
                group = k if len(taken) == k * len(places) else group
        masks = []
        for k in range(1, group):
            mask = place < 0
            for p in places:
                mask = mask | (place == (p + k * (per_tile // group)) % per_tile)
            masks.append(mask)
        return masks

    def merged(values, masks):
        result = values[0]
        for k, mask in enumerate(masks):
            result = jnp.where(mask, pltpu.roll(values[k + 1], (k + 1) * LANES // (len(masks) + 1), 1), result)
        return result

    def window_gains(plans):
        both_rows = [energy[h * 16 : h * 16 + 8, :] + energy[h * 16 + 8 : h * 16 + 16, :] for h in range(tiles)]
        blockwise = [jnp.broadcast_to(jnp.sum(e, axis=0, keepdims=True), (8, LANES)) for e in both_rows]
        tall = [e + below(e) for e in blockwise]
        for unit, ((h, masks, first, count), wide) in enumerate(zip(plans, right(tall, [p[0] for p in plans]))):
            value = merged([1.0 / ((tall[h] + wide) + EPS)] * 4, masks)
            for j in range(count):
                gain[(first + j) * 8 : (first + j) * 8 + 8, :] = value

    def forward_columns(step, plans, g):
        rows = pl.ds(pl.multiple_of(g * 8, 8), 8)
        under = pl.ds(g * 8 + 1, 8)
        active = [p[0] for p in plans]
        window_gains(plans)
        near = {h: [] for h in active}
        far = {h: [] for h in active}
        for s in range(16):
            re = [zr[h * 16 + s, rows, :] for h in range(tiles)]
            im = [zi[h * 16 + s, rows, :] for h in range(tiles)]
            for h, a, b in zip(active, right(re, active), right(im, active)):
                near[h].append((re[h], im[h]))
                far[h].append((a, b))
        for h, masks, first, count in plans:
            group = len(masks) + 1
            even = fft([plus(a, b) for a, b in zip(near[h], far[h])], -1)
            odd = fft([rotated(minus(a, b), s, 32, -1) for s, (a, b) in enumerate(zip(near[h], far[h]))], -1)
            for row in range(8 * count):
                sources = [(row // 8 * group + k) * 8 + row % 8 for k in range(group)]
                values = [(even, odd)[l % 2][l // 2] for l in sources]
                value = tuple(merged([v[part] for v in values], masks) for part in range(2))
                at = pl.ds((first * 8 + row) * 17 + g * 8, 8)
                if first == 0 and row < 8:
                    following = (below(value[0]), below(value[1]))
                    ur[at, :], ui[at, :] = plus(value, following)
                    vr[at, :], vi[at, :] = minus(value, following)
                else:
                    yr[at, :], yi[at, :] = value

        def corner(s):
            if s < 16:
                return near[0][s], (zr[s, under, :], zi[s, under, :])
            moved = [right([ref[h * 16, under, :] for h in range(tiles)], (0,))[0] for ref in (zr, zi)]
            return far[0][0], tuple(moved)

        def cross(a, b):
            return a[1] * b[0] - a[0] * b[1]

        total = jnp.zeros((8, LANES), jnp.float32)
        here_, under_ = corner(0)
        down = cross(here_, under_)
        for s in range(16):
            next_, next_under = corner(s + 1)
            next_down = cross(next_, next_under)
            loop = (cross(here_, next_) - cross(under_, next_under)) + (next_down - down)
            total = total + loop * loop
            here_, under_, down = next_, next_under, next_down
        sums[pl.ds(pl.multiple_of(step * 16 + g * 8, 8), 8), :] = total

    def split_rows(unit):
        for row in range(8):
            for g in range(2):
                source = pl.ds((unit * 8 + row) * 17 + g * 8, 8)
                at = pl.ds(row * 17 + g * 8, 8)
                value = (yr[source, :], yi[source, :])
                following = (below(value[0]), below(value[1]))
                ur[at, :], ui[at, :] = plus(value, following)
                vr[at, :], vi[at, :] = minus(value, following)

    def join_rows(unit):
        for t in range(16):
            source = pl.ds(t * 9, 8)
            at = pl.ds((unit * 16 + t) * 9, 8)
            wr[at, :] = pr[source, :] + above(qr[source, :])
            wi[at, :] = pi[source, :] + above(qi[source, :])

    def windows(unit):
        join_rows(jnp.maximum(unit - 1, 0))
        scale = gain[pl.ds(pl.multiple_of(unit * 8, 8), 8), :]
        at = [pl.ds(t, 8, stride=17) for t in range(16)]
        back = []
        for parity, (a, b) in enumerate(((ur, ui), (vr, vi))):
            values = [(a[x, :], b[x, :]) for x in at]
            if parity:
                values = [rotated(v, t, 32, -1) for t, v in enumerate(values)]
            filtered = []
            for re, im in fft(values, -1):
                factor = lax.rsqrt(lax.rsqrt((re * re + im * im) * scale))
                filtered.append((re * factor, im * factor))
            back.append(fft(filtered, 1))
        split_rows(unit + 1)
        for t in range(16):
            odd = rotated(back[1][t], t, 32, 1)
            upper = plus(back[0][t], odd)
            lower = minus(back[0][t], odd)
            at = pl.ds(t * 9, 8)
            pr[at, :], pi[at, :] = (v * (ramp(t) / 32) for v in upper)
            qr[at, :], qi[at, :] = (v * (ramp(t + 16) / 32) for v in lower)

    def inverse_columns(plans, units, g):
        rows = pl.ds(pl.multiple_of(g * 8, 8), 8)
        kept = []
        passed = []
        for h, masks, first, count in plans:
            group = len(masks) + 1
            values = [None] * 32
            for row in range(8 * count):
                unit = first + row // 8
                if unit == units - 1:
                    at = pl.ds(g * 72 + row % 8, 8, stride=9)
                    value = (pr[at, :] + above(qr[at, :]), pi[at, :] + above(qi[at, :]))
                else:
                    at = pl.ds(unit * 144 + g * 72 + row % 8, 8, stride=9)
                    value = (wr[at, :], wi[at, :])
                for k in range(group):
                    l = (row // 8 * group + k) * 8 + row % 8
                    values[l] = tuple(pltpu.roll(v, LANES - k * LANES // group, 1) if k else v for v in value)
            even = fft(values[0::2], 1)
            odd = fft(values[1::2], 1)
            own = []
            other = []
            for s in range(16):
                turned = rotated(odd[s], s, 32, 1)
                weight = here[h] * (ramp(s) / 32)
                own.append(tuple(v * weight for v in plus(even[s], turned)))
                weight = both[h] * (ramp(s + 16) / 32)
                other.append(tuple(v * weight for v in minus(even[s], turned)))
            kept.append(own)
            passed.append(other)
        power = [jnp.zeros((8, LANES), jnp.float32) for _ in range(tiles)]
        for s in range(16):
            arrived = [left([passed[h][s][part] for h in range(tiles)]) for part in range(2)]
            for h in range(tiles):
                value = tuple(kept[h][s][part] + arrived[part][h] for part in range(2))
                power[h] = keep(h, s, g, value, power[h])
        for h in range(tiles):
            energy[pl.ds(pl.multiple_of(h * 16 + g * 8, 8), 8), :] = power[h]

    def run(count, body):
        lax.fori_loop(0, count, lambda i, c: (body(i), c)[1], 0)

    for step in range(ITERS):
        needed = range(step - ITERS, blocks + ITERS - 1 - step)
        plans = []
        units = 0
        for h in range(tiles):
            masks = sharing(h, needed)
            plans.append((h, masks, units, 4 // (len(masks) + 1)))
            units += 4 // (len(masks) + 1)
        run(2, functools.partial(forward_columns, step, plans))
        run(units, windows)
        run(2, functools.partial(inverse_columns, plans, units))
    totals = [jnp.sum(sums[step * 16 : step * 16 + 8, :] + sums[step * 16 + 8 : step * 16 + 16, :]) for step in range(ITERS)]

    for step, total in enumerate(totals):
        out_ref[32, step : step + 1, :] = jnp.full((1, LANES), total)
    for part, ref in enumerate((zr, zi)):
        for s in range(16):
            out_ref[part * 16 + s, :, :] = ref[s, 0:16, :]


def filter_tiles(slabs, blocks, tiles, data):
    body = functools.partial(filter_kernel, slabs, blocks, tiles)
    return pl.pallas_call(
        body,
        out_shape=jax.ShapeDtypeStruct((33, 16, LANES), jnp.float32),
        in_specs=[pl.BlockSpec(memory_space=pltpu.VMEM)],
        out_specs=pl.BlockSpec(memory_space=pltpu.VMEM),
        scratch_shapes=[pltpu.VMEM((tiles * 16, 24, LANES), jnp.float32)] * 2
        + [pltpu.VMEM(((tiles * 4 + 1) * 136, LANES), jnp.float32)] * 2
        + [pltpu.VMEM((136, LANES), jnp.float32)] * 4
        + [pltpu.VMEM((tiles * 4 * 144, LANES), jnp.float32)] * 2
        + [pltpu.VMEM((144, LANES), jnp.float32)] * 4
        + [pltpu.VMEM((rows, LANES), jnp.float32) for rows in (tiles * 16, tiles * 32, ITERS * 16)],
        compiler_params=pltpu.CompilerParams(vmem_limit_bytes=16 << 20),
        name="filter_tiles",
    )(data)


def pack_kernel(in_ref, out_ref, turn):
    lane = lax.broadcasted_iota(jnp.int32, (8, LANES), 1)
    zero = jnp.zeros((8, LANES), jnp.float32)
    columns = [[in_ref[g * 8 : g * 8 + 8, c * LANES : (c + 1) * LANES] for g in range(2)] for c in range(16)]
    for c in range(16):
        after = columns[c + 1] if c < 15 else [zero, zero]
        before = columns[c - 1] if c else [zero, zero]
        at = c * IN_ROWS
        out_ref[at : at + 8, :] = columns[c][0]
        out_ref[at + 8 : at + 16, :] = columns[c][1]
        first = jnp.where(lane < 32, after[0], pltpu.roll(before[0], 64, 1))
        second = jnp.where(lane < 96, pltpu.roll(after[1], 64, 1), before[1])
        out_ref[at + 16 : at + 24, :] = jnp.where(lane < 64, first, second)
        turn[c * 8 : c * 8 + 8, :] = jnp.where(lane < 16, pltpu.roll(after[0], 96, 1), pltpu.roll(after[1], 112, 1))
    for q in range(4):
        rows = turn[pl.ds(q * 32, 8, stride=4), :]
        for u in range(1, 4):
            rows = jnp.where(lane // 32 == u, pltpu.roll(turn[pl.ds(q * 32 + u, 8, stride=4), :], 32 * u, 1), rows)
        for k in range(4):
            at = (q * 4 + k) * IN_ROWS + 24
            out_ref[at : at + 2, :] = rows[k * 2 : k * 2 + 2]


def pack(phase):
    return pl.pallas_call(
        pack_kernel,
        out_shape=jax.ShapeDtypeStruct((16 * IN_ROWS, LANES), jnp.float32),
        in_specs=[pl.BlockSpec(memory_space=pltpu.VMEM)],
        out_specs=pl.BlockSpec(memory_space=pltpu.VMEM),
        scratch_shapes=[pltpu.VMEM((128, LANES), jnp.float32)],
        compiler_params=pltpu.CompilerParams(vmem_limit_bytes=8 << 20),
        name="pack",
    )(phase)


def column_kernel(in_ref, out_ref, *scratch):
    zr, zi, yr, yi, wr, wi, shift_r, shift_i, gain, turn = scratch[:10]
    buffers = [scratch[10 + 6 * k : 16 + 6 * k] for k in range(2)]
    final = scratch[22:25]
    tile = lax.axis_index("rows")
    lane = lax.broadcasted_iota(jnp.int32, (8, LANES), 1)
    sub = lax.broadcasted_iota(jnp.int32, (8, LANES), 0)
    in_slab = lane & 7

    def inside(first):
        column = tile * 8 + (first - 2) + sub // 2
        return jnp.where((column >= 0) & (column < 128), 1.0, 0.0)

    def block(body):
        pl.when(tile >= 0)(body)

    def run(count, body):
        lax.fori_loop(0, count, lambda i, c: (body(i), c)[1], 0)

    zero = jnp.zeros((8, LANES), jnp.float32)
    for vr, vi, pr, pi, qr, qi in buffers:
        for ref in (vr, vi):
            for row in (272, 280, 288):
                ref[row : row + 8, :] = zero
        for ref in (qr, qi):
            for t in range(16):
                ref[t * 17 : t * 17 + 1, :] = zero[0:1]

    def stacked(offset):
        return jnp.concatenate([in_ref[a * IN_ROWS + offset : a * IN_ROWS + offset + 8, :] for a in range(16)], axis=0)

    for k, offset in enumerate((0, 8, 16)):
        turned = stacked(offset).T
        for b in range(8):
            at = k * 136 + (b % 4 * 2 + b // 4 if k == 2 else b) * 17
            turn[at : at + 16, :] = turned[b * 16 : b * 16 + 16]
    tail = jnp.concatenate([in_ref[a * IN_ROWS + 24 : a * IN_ROWS + 26, :] for a in range(16)], axis=0)
    for q in range(4):
        for u in range(4):
            value = tail[q * 8 : q * 8 + 8]
            turn[pl.ds(408 + q * 32 + u, 8, stride=4), :] = pltpu.roll(value, LANES - 32 * u, 1) if u else value
    turned = turn[408:536, :].T[0:32]
    beyond = jnp.where(tile * 8 + 10 < 128, 1.0, 0.0)
    for ref, v in zip((zr, zi), cos_sin(turned)):
        for k in range(4):
            at = (k % 2) * 8 * PITCH + 24 + k // 2
            ref[pl.ds(at, 8, stride=PITCH), :] = v[k * 8 : k * 8 + 8] * beyond
    for g in range(2):
        for s in range(16):
            value = cos_sin(turn[pl.ds(g * 136 + s, 8, stride=17), :])
            for ref, v in zip((zr, zi), value):
                ref[pl.ds(s * PITCH + 4 + g, 8, stride=2), :] = v
    edge = tile * 8 + jnp.where(sub < 4, 8 + sub // 2, sub // 2 - 4)
    edge = jnp.where((edge >= 0) & (edge < 128), 1.0, 0.0)
    for s in range(16):
        value = cos_sin(turn[pl.ds(272 + s, 8, stride=17), :])
        for ref, v in zip((zr, zi), value):
            v = v * edge
            ref[s * PITCH + 20 : s * PITCH + 24, :] = v[0:4]
            ref[s * PITCH : s * PITCH + 4, :] = v[4:8]

    def forward_columns(first, width, j):
        near = []
        far = []
        power = zero
        for s in range(16):
            at = pl.ds(s * PITCH + 2 * first + j * 8, 8)
            after = pl.ds(s * PITCH + 2 * first + 2 + j * 8, 8)
            near.append((zr[at, :], zi[at, :]))
            far.append((zr[after, :], zi[after, :]))
            a, b = near[-1], far[-1]
            power = power + ((a[0] * a[0] + a[1] * a[1]) + (b[0] * b[0] + b[1] * b[1]))
        gain[pl.ds(pl.multiple_of(48 + j * 8, 8), 8), :] = power
        even = fft([plus(a, b) for a, b in zip(near, far)], -1)
        odd = odd_outputs([minus(a, b) for a, b in zip(near, far)])
        for l in range(32):
            to = pl.ds(l * 2 * width + j * 8, 8)
            yr[to, :], yi[to, :] = (even, odd)[l % 2][l // 2]

    def turn_in(chunk):
        vr, vi = buffers[chunk % 2][:2]
        for source, ref in ((yr, vr), (yi, vi)):
            for g in range(2):
                parts = [source[pl.ds(chunk * 256 + i * 16 + g, 8, stride=2), :] for i in range(16)]
                turned = jnp.concatenate(parts, axis=0).T
                for a in range(16):
                    ref[a * 17 + g * 8 : a * 17 + g * 8 + 8, :] = turned[a * 8 : a * 8 + 8]

    def turn_out(chunk):
        pr, pi, qr, qi = buffers[chunk % 2][2:]
        for p, q, target in ((pr, qr, wr), (pi, qi, wi)):
            for g in range(2):
                parts = []
                for a in range(16):
                    at = pl.ds(g * 136 + a, 8, stride=17)
                    parts.append(p[at, :] + q[at, :])
                turned = jnp.concatenate(parts, axis=0).T
                for i in range(16):
                    target[pl.ds(chunk * 256 + i * 16 + g, 8, stride=2), :] = turned[i * 8 : i * 8 + 8]

    def window_gains(valid, width):
        count = 2 * width
        power = jnp.concatenate(
            [jnp.where(sub < 2 * valid - 8 * j, gain[48 + j * 8 : 56 + j * 8, :], 0.0) for j in range(count // 8)], axis=0
        )
        row = lax.broadcasted_iota(jnp.int32, (16, LANES), 0)
        slab = lax.broadcasted_iota(jnp.int32, (16, LANES), 1) // 8
        pick = jnp.where((slab == row) | (slab == row + 1), 1.0, 0.0)
        exact = dict(precision=lax.Precision.HIGHEST, preferred_element_type=jnp.float32)
        mean = lax.dot_general(pick, power, (((1,), (1,)), ((), ())), **exact)
        column = lax.broadcasted_iota(jnp.int32, (count, 32 * width), 1)
        column = column - width * ((column.astype(jnp.float32) + 0.5) * (1.0 / width)).astype(jnp.int32)
        spread = jnp.where(column == lax.broadcasted_iota(jnp.int32, (count, 32 * width), 0) // 2, 1.0, 0.0)
        mean = lax.dot_general(mean, spread, (((1,), (0,)), ((), ())), **exact)
        for c in range(width // 4):
            gain[c * 16 : c * 16 + 16, :] = 1.0 / (mean[:, c * 128 : c * 128 + 128] + EPS)

    def residues():
        def corner(s):
            at = s * PITCH + 4 if s < 16 else 6
            result = []
            for ref in (zr, zi):
                top = ref[pl.ds(at, 8, stride=2), :]
                low = ref[pl.ds(at + 1, 8, stride=2), :]
                top_left = pltpu.roll(top, LANES - 1, 1)
                low_left = pltpu.roll(low, LANES - 1, 1)
                top_under = jnp.where(in_slab < 7, top_left, pltpu.roll(low, 7, 1))
                low_under = jnp.where(in_slab < 7, low_left, jnp.where(lane < LANES - 1, top_left, 0.0))
                result.append((top, low, top_under, low_under))
            return [((result[0][g], result[1][g]), (result[0][2 + g], result[1][2 + g])) for g in range(2)]

        def cross(a, b):
            return a[1] * b[0] - a[0] * b[1]

        total = zero
        here = corner(0)
        down = [cross(*pair) for pair in here]
        for s in range(16):
            following = corner(s + 1)
            following_down = [cross(*pair) for pair in following]
            for g in range(2):
                across = cross(here[g][0], following[g][0]) - cross(here[g][1], following[g][1])
                loop = across + (following_down[g] - down[g])
                total = total + loop * loop
            here, down = following, following_down
        return total

    def windows(chunk, half):
        vr, vi, pr, pi, qr, qi = buffers[chunk % 2]
        scale = gain[chunk * 16 + half * 8 : chunk * 16 + half * 8 + 8, :]
        sums = []
        differences = []
        for t in range(16):
            at = pl.ds(half * 136 + t, 8, stride=17)
            after = pl.ds(half * 136 + 17 + t, 8, stride=17)
            near = (vr[at, :], vi[at, :])
            far = (vr[after, :], vi[after, :])
            sums.append(plus(near, far))
            differences.append(minus(near, far))
        back = []
        for spectrum in (lambda: fft(sums, -1), lambda: odd_outputs(differences)):
            filtered = []
            for re, im in spectrum():
                factor = lax.rsqrt(lax.rsqrt((re * re + im * im) * scale))
                filtered.append((re * factor, im * factor))
            back.append(filtered)
        back = fft(back[0], 1), join(fft(back[1][0::2], 1), fft(back[1][1::2], 1), 32, 1)
        for t in range(16):
            upper = plus(back[0][t], back[1][t])
            lower = minus(back[0][t], back[1][t])
            at = pl.ds(t * 17 + half * 8, 8)
            pr[at, :], pi[at, :] = (v * (ramp(t) / 32) for v in upper)
            at = pl.ds(t * 17 + half * 8 + 1, 8)
            qr[at, :], qi[at, :] = (v * (ramp(t + 16) / 32) for v in lower)

    def inverse_columns(first, width, last, j):
        here = inside(first + 4 * j)
        both = here * inside(first + 4 * j + 1)
        values = []
        for l in range(32):
            at = pl.ds(l * 2 * width + 8 * j, 8)
            values.append((wr[at, :], wi[at, :]))
        even = fft(values[0::2], 1)
        odd = join(fft(values[1::4], 1), fft(values[3::4], 1), 32, 1)
        for s in range(16):
            weight = here * (ramp(s) / 32)
            own = [v * weight for v in plus(even[s], odd[s])]
            weight = both * (ramp(s + 16) / 32)
            other = [v * weight for v in minus(even[s], odd[s])]
            for part, (ref, shift) in enumerate(((zr, shift_r), (zi, shift_i))):
                if last:
                    base = part * 304 + s * 19 + 8 * j
                    final[0][pl.ds(base, 8), :] = own[part]
                    final[1][pl.ds(base + 2, 8), :] = other[part]
                else:
                    shift[pl.ds(s * 32 + 8 * j + 2, 8), :] = other[part]
                    value = own[part] + shift[pl.ds(s * 32 + 8 * j, 8), :]
                    ref[pl.ds(s * PITCH + 2 * first + 8 * j, 8), :] = value

    for k in range(32):
        final[1][k * 19 : k * 19 + 2, :] = zero[0:2]

    def iteration(step, width, last):
        chunks = width // 4
        run(chunks, functools.partial(forward_columns, step, width))

        @block
        def _():
            window_gains(12 - 2 * step, width)
            turn_in(0)
            final[2][pl.ds(step * 8, 8), :] = residues()

        for chunk in range(chunks):

            @block
            def _():
                if chunk + 1 < chunks:
                    turn_in(chunk + 1)
                windows(chunk, 0)
                windows(chunk, 1)
                if chunk:
                    turn_out(chunk - 1)

        block(lambda: turn_out(chunks - 1))
        run(chunks, functools.partial(inverse_columns, step, width, last))

    run(ITERS - 1, lambda step: iteration(step, 12, False))
    iteration(ITERS - 1, 8, True)

    spill = []
    for part in range(2):
        for g in range(2):
            base = part * 304 + g
            rows = []
            for b in range(8):
                for s in (0, 8):
                    at = pl.ds(base + s * 19 + 2 * b, 8, stride=19)
                    rows.append(final[0][at, :] + final[1][at, :])
            turned = jnp.concatenate(rows, axis=0).T
            for a in range(16):
                at = a * OUT_ROWS + part * 16 + g * 8
                out_ref[at : at + 8, :] = turned[a * 8 : a * 8 + 8]
            spill += [final[1][pl.ds(base + s * 19 + 16, 8, stride=19), :] for s in (0, 8)]
    turned = jnp.concatenate(spill + spill, axis=0).T
    report = zero[0:1]
    for step in range(ITERS):
        total = jnp.sum(final[2][step * 8 : step * 8 + 8, :])
        report = jnp.where(lane[0:1] == step * 16 + tile, total, report)
    for a in range(16):
        value = turned[a * 8 : a * 8 + 8]
        out_ref[a * OUT_ROWS + 32 : a * OUT_ROWS + 36, :] = jnp.where(lane[0:4] < 64, value[0:4], value[4:8])
        out_ref[a * OUT_ROWS + 36 : a * OUT_ROWS + 37, :] = report


def filter_columns(data):
    def rows(count):
        return pltpu.VMEM((count, LANES), jnp.float32)

    return pl.pallas_call(
        column_kernel,
        out_shape=jax.ShapeDtypeStruct((16 * OUT_ROWS, LANES), jnp.float32),
        in_specs=[pl.BlockSpec(memory_space=pltpu.VMEM)],
        out_specs=pl.BlockSpec(memory_space=pltpu.VMEM),
        scratch_shapes=[rows(16 * PITCH)] * 2
        + [rows(776)] * 4
        + [rows(520)] * 2
        + [rows(80), rows(544)]
        + ([rows(296)] * 2 + [rows(280)] * 4) * 2
        + [rows(624), rows(624), rows(ITERS * 8)],
        compiler_params=pltpu.CompilerParams(vmem_limit_bytes=16 << 20),
        name="filter_columns",
    )(data)


def finish_kernel(scale, in_ref, field_ref, profile_ref):
    lane = lax.broadcasted_iota(jnp.int32, (8, LANES), 1)
    extras = []
    sums = jnp.zeros((1, LANES), jnp.float32)
    for c in range(16):
        half = in_ref[c * OUT_ROWS + 32 : c * OUT_ROWS + 36, :]
        extras.append(jnp.concatenate([half, pltpu.roll(half, 64, 1)], axis=0))
        sums = sums + in_ref[c * OUT_ROWS + 36 : c * OUT_ROWS + 37, :]
    for step in range(ITERS):
        profile_ref[step : step + 1, :] = sums[:, step * 16 : step * 16 + 16] * scale
    for part in range(2):
        for g in range(2):
            offset = (part * 2 + g) * 16
            for c in range(16):
                at = c * OUT_ROWS + part * 16 + g * 8
                value = in_ref[at : at + 8, :]
                if c:
                    spill = pltpu.roll(extras[c - 1], LANES - offset, 1) if offset else extras[c - 1]
                    value = value + jnp.where(lane < 16, spill, 0.0)
                field_ref[part, g * 8 : g * 8 + 8, c * LANES : (c + 1) * LANES] = value


def finish(scale, data):
    return pl.pallas_call(
        functools.partial(finish_kernel, scale),
        out_shape=(
            jax.ShapeDtypeStruct((2, 16, 16 * LANES), jnp.float32),
            jax.ShapeDtypeStruct((ITERS, 16), jnp.float32),
        ),
        in_specs=[pl.BlockSpec(memory_space=pltpu.VMEM)],
        out_specs=[pl.BlockSpec(memory_space=pltpu.VMEM)] * 2,
        compiler_params=pltpu.CompilerParams(vmem_limit_bytes=8 << 20),
        name="finish",
    )(data)


def ring_of_blocks(phase, devices, blocks, tiles):
    per_tile = LANES // devices
    ring = tiles * per_tile
    width = phase.shape[1]
    padded = jnp.pad(phase, ((0, 0), (HALO * 16, (ring + HALO) * 16)))
    pieces = []
    for d in range(devices):
        start = d * blocks * 16
        ahead = padded[:, start + HALO * 16 : start + (blocks + 2 * HALO) * 16]
        behind = padded[:, start : start + HALO * 16]
        gap = jnp.zeros((16, (ring - blocks - 2 * HALO) * 16), phase.dtype)
        pieces.append(jnp.concatenate([ahead, gap, behind], axis=1))
    return jnp.stack(pieces)


def per_device(phase):
    devices = lax.axis_size("rows")
    height, width = phase.shape
    blocks = width // (16 * devices)
    per_tile = LANES // devices
    if height != 16 or LANES % devices or blocks * 16 * devices != width or blocks != per_tile:
        raise ValueError("unsupported sizes")
    scale = 1.0 / (height * devices * 128.0)
    if devices == 16:
        data = lax.all_to_all(pack(phase).reshape(16, IN_ROWS, 1, LANES), "rows", 0, 0)
        result = filter_columns(data.reshape(16 * IN_ROWS, LANES))
        result = lax.all_to_all(result.reshape(16, OUT_ROWS, 1, LANES), "rows", 0, 0)
        result = result.reshape(16 * OUT_ROWS, LANES)
        return finish(scale, result)
    tiles = -(-(blocks + 2 * HALO) // per_tile)
    data = lax.all_to_all(ring_of_blocks(phase, devices, blocks, tiles), "rows", 0, 0)
    data = data.reshape(devices, 16, tiles, per_tile, 16).transpose(2, 4, 1, 3, 0)
    result = filter_tiles(devices, blocks, tiles, data.reshape(tiles, 16, 16, LANES))
    field = result[:32].reshape(2, 16, 16, per_tile, devices).transpose(4, 0, 2, 3, 1)
    field = field.reshape(devices, 32, per_tile * 16)
    sums = jnp.broadcast_to(result[32, :ITERS, : per_tile * 16][None], (devices, ITERS, per_tile * 16))
    result = lax.all_to_all(jnp.concatenate([field, sums], axis=1), "rows", 0, 0)
    field = result[:, :32].reshape(devices, 2, 16, per_tile * 16).transpose(1, 2, 0, 3).reshape(2, 16, width)
    profile = result[:, 32:, 0].reshape(width // 128, -1, ITERS).sum(1).T
    return field, profile * scale


def solution(mesh):
    return jax.shard_map(
        per_device,
        mesh=mesh,
        in_specs=(P(("groups", "rows"), None),),
        out_specs=(P(None, ("groups", "rows"), None), P("groups", None)),
        check_vma=False,
    )
```

```python
import functools
import math

import jax
import jax.numpy as jnp
import numpy as np
from jax import lax
from jax.experimental import pallas as pl
from jax.experimental.pallas import tpu as pltpu
from jax.sharding import PartitionSpec as P

ITERS = 3
EPS = 1e-06
LANES = 128
IN_ROWS = 26
OUT_ROWS = 37
PITCH = 41
HALO = 3

SIN = (9.99999996e-01, -1.66666580e-01, 8.33305053e-03, -1.98090400e-04, 2.60515161e-06)
COS = (9.99999953e-01, -4.99999050e-01, 4.16635780e-02, -1.38536600e-03, 2.31530144e-05)


def rotated(value, k, size, sign):
    re, im = value
    half = math.sqrt(0.5)
    if k == 0:
        return re, im
    if 4 * k == size:
        return (im, -re) if sign < 0 else (-im, re)
    if 8 * k == size:
        return ((re + im) * half, (im - re) * half) if sign < 0 else ((re - im) * half, (im + re) * half)
    if 8 * k == 3 * size:
        return ((im - re) * half, (re + im) * -half) if sign < 0 else ((re + im) * -half, (re - im) * half)
    if 2 * k > size:
        return rotated((-re, -im), k - size // 2, size, sign)
    c = math.cos(2 * math.pi * k / size)
    s = sign * math.sin(2 * math.pi * k / size)
    return re * c - im * s, im * c + re * s


def plus(a, b):
    return a[0] + b[0], a[1] + b[1]


def minus(a, b):
    return a[0] - b[0], a[1] - b[1]


def quarter_turn(a, sign):
    return (-a[1], a[0]) if sign > 0 else (a[1], -a[0])


def join(one, three, size, sign):
    quarter = size // 4
    one = [rotated(one[k], k, size, sign) for k in range(quarter)]
    three = [rotated(three[k], 3 * k, size, sign) for k in range(quarter)]
    turned = [quarter_turn(minus(a, b), sign) for a, b in zip(one, three)]
    return [plus(a, b) for a, b in zip(one, three)] + turned


def fft(values, sign):
    size = len(values)
    if size == 1:
        return values
    if size == 2:
        return [plus(*values), minus(*values)]
    even = fft(values[0::2], sign)
    odd = join(fft(values[1::4], sign), fft(values[3::4], sign), size, sign)
    return [plus(e, o) for e, o in zip(even, odd)] + [minus(e, o) for e, o in zip(even, odd)]


def odd_outputs(differences):
    one = []
    three = []
    for k in range(8):
        turned = quarter_turn(differences[k + 8], -1)
        one.append(rotated(plus(differences[k], turned), k, 32, -1))
        three.append(rotated(minus(differences[k], turned), 3 * k, 32, -1))
    pairs = zip(fft(one, -1), fft(three, -1))
    return [value for pair in pairs for value in pair]


def polynomial(coefficients, w):
    result = jnp.full_like(w, coefficients[-1])
    for c in coefficients[-2::-1]:
        result = result * w + c
    return result


def cos_sin(x):
    u = (jnp.abs(x) - jnp.float32(math.pi / 2)) + jnp.float32(4.371139e-08)
    w = u * u
    cosine = -(u * polynomial(SIN, w))
    sine = polynomial(COS, w)
    return cosine, jnp.where(x < 0, -sine, sine)


def ramp(t):
    return 1.0 - abs(t - 15.5) / 16.0


def filter_kernel(
    slabs, blocks, tiles, in_ref, out_ref, zr, zi, yr, yi, ur, ui, vr, vi, wr, wi, pr, pi, qr, qi, energy, gain, sums
):
    tile = lax.axis_index("rows")
    per_tile = LANES // slabs
    ring = tiles * per_tile
    lane = lax.broadcasted_iota(jnp.int32, (8, LANES), 1)
    sub = lax.broadcasted_iota(jnp.int32, (8, LANES), 0)
    not_last = lane % slabs != slabs - 1
    not_first = lane % slabs != 0
    place = lane // slabs

    def inside(h, step):
        position = (h * per_tile + place + step) % ring
        relative = jnp.where(position < blocks + HALO, position, position - ring)
        column = tile * blocks + relative
        return jnp.where((column >= 0) & (column < slabs * blocks), 1.0, 0.0)

    here = [inside(h, 0) for h in range(tiles)]
    both = [here[h] * inside(h, 1) for h in range(tiles)]

    def right(values, active):
        if per_tile == 1:
            return [values[(h + 1) % tiles] for h in active]
        moved = [pltpu.roll(v, LANES - slabs, 1) for v in values]
        return [jnp.where(lane < LANES - slabs, moved[h], moved[(h + 1) % tiles]) for h in active]

    def left(values):
        if per_tile == 1:
            return [values[h - 1] for h in range(tiles)]
        moved = [pltpu.roll(v, slabs, 1) for v in values]
        return [jnp.where(lane < slabs, moved[h - 1], moved[h]) for h in range(tiles)]

    def below(value):
        return jnp.where(not_last, pltpu.roll(value, LANES - 1, 1), 0.0)

    def above(value):
        return jnp.where(not_first, pltpu.roll(value, 1, 1), 0.0)

    def keep(h, s, g, value, power):
        for part, ref in enumerate((zr, zi)):
            ref[h * 16 + s, pl.ds(g * 8, 8), :] = value[part]
            if h == 0 or s == 0:
                ref[h * 16 + s, pl.ds(16 + g, 1), :] = below(value[part])[0:1]
        return power + (value[0] * value[0] + value[1] * value[1])

    for h in range(tiles):
        for g in range(2):
            phases = [in_ref[h, s, g * 8 : g * 8 + 8, :] for s in range(16)]
            power = jnp.zeros((8, LANES), jnp.float32)
            for s in range(16):
                cosine, sine = cos_sin(phases[s])
                power = keep(h, s, g, (cosine * here[h], sine * here[h]), power)
            energy[h * 16 + g * 8 : h * 16 + g * 8 + 8, :] = power

    def sharing(h, needed):
        places = {w % ring - h * per_tile for w in needed}
        places = {p for p in places if 0 <= p < per_tile}
        group = 1
        for k in (2, 4):
            if per_tile % k == 0:
                taken = {(p + j * (per_tile // k)) % per_tile for p in places for j in range(k)}
                group = k if len(taken) == k * len(places) else group
        masks = []
        for k in range(1, group):
            mask = place < 0
            for p in places:
                mask = mask | (place == (p + k * (per_tile // group)) % per_tile)
            masks.append(mask)
        return masks

    def merged(values, masks):
        result = values[0]
        for k, mask in enumerate(masks):
            result = jnp.where(mask, pltpu.roll(values[k + 1], (k + 1) * LANES // (len(masks) + 1), 1), result)
        return result

    def window_gains(plans):
        both_rows = [energy[h * 16 : h * 16 + 8, :] + energy[h * 16 + 8 : h * 16 + 16, :] for h in range(tiles)]
        blockwise = [jnp.broadcast_to(jnp.sum(e, axis=0, keepdims=True), (8, LANES)) for e in both_rows]
        tall = [e + below(e) for e in blockwise]
        for unit, ((h, masks, first, count), wide) in enumerate(zip(plans, right(tall, [p[0] for p in plans]))):
            value = merged([1.0 / ((tall[h] + wide) + EPS)] * 4, masks)
            for j in range(count):
                gain[(first + j) * 8 : (first + j) * 8 + 8, :] = value

    def forward_columns(step, plans, g):
        rows = pl.ds(pl.multiple_of(g * 8, 8), 8)
        under = pl.ds(g * 8 + 1, 8)
        active = [p[0] for p in plans]
        window_gains(plans)
        near = {h: [] for h in active}
        far = {h: [] for h in active}
        for s in range(16):
            re = [zr[h * 16 + s, rows, :] for h in range(tiles)]
            im = [zi[h * 16 + s, rows, :] for h in range(tiles)]
            for h, a, b in zip(active, right(re, active), right(im, active)):
                near[h].append((re[h], im[h]))
                far[h].append((a, b))
        for h, masks, first, count in plans:
            group = len(masks) + 1
            even = fft([plus(a, b) for a, b in zip(near[h], far[h])], -1)
            odd = fft([rotated(minus(a, b), s, 32, -1) for s, (a, b) in enumerate(zip(near[h], far[h]))], -1)
            for row in range(8 * count):
                sources = [(row // 8 * group + k) * 8 + row % 8 for k in range(group)]
                values = [(even, odd)[l % 2][l // 2] for l in sources]
                value = tuple(merged([v[part] for v in values], masks) for part in range(2))
                at = pl.ds((first * 8 + row) * 17 + g * 8, 8)
                if first == 0 and row < 8:
                    following = (below(value[0]), below(value[1]))
                    ur[at, :], ui[at, :] = plus(value, following)
                    vr[at, :], vi[at, :] = minus(value, following)
                else:
                    yr[at, :], yi[at, :] = value

        def corner(s):
            if s < 16:
                return near[0][s], (zr[s, under, :], zi[s, under, :])
            moved = [right([ref[h * 16, under, :] for h in range(tiles)], (0,))[0] for ref in (zr, zi)]
            return far[0][0], tuple(moved)

        def cross(a, b):
            return a[1] * b[0] - a[0] * b[1]

        total = jnp.zeros((8, LANES), jnp.float32)
        here_, under_ = corner(0)
        down = cross(here_, under_)
        for s in range(16):
            next_, next_under = corner(s + 1)
            next_down = cross(next_, next_under)
            loop = (cross(here_, next_) - cross(under_, next_under)) + (next_down - down)
            total = total + loop * loop
            here_, under_, down = next_, next_under, next_down
        sums[pl.ds(pl.multiple_of(step * 16 + g * 8, 8), 8), :] = total

    def split_rows(unit):
        for row in range(8):
            for g in range(2):
                source = pl.ds((unit * 8 + row) * 17 + g * 8, 8)
                at = pl.ds(row * 17 + g * 8, 8)
                value = (yr[source, :], yi[source, :])
                following = (below(value[0]), below(value[1]))
                ur[at, :], ui[at, :] = plus(value, following)
                vr[at, :], vi[at, :] = minus(value, following)

    def join_rows(unit):
        for t in range(16):
            source = pl.ds(t * 9, 8)
            at = pl.ds((unit * 16 + t) * 9, 8)
            wr[at, :] = pr[source, :] + above(qr[source, :])
            wi[at, :] = pi[source, :] + above(qi[source, :])

    def windows(unit):
        join_rows(jnp.maximum(unit - 1, 0))
        scale = gain[pl.ds(pl.multiple_of(unit * 8, 8), 8), :]
        at = [pl.ds(t, 8, stride=17) for t in range(16)]
        back = []
        for parity, (a, b) in enumerate(((ur, ui), (vr, vi))):
            values = [(a[x, :], b[x, :]) for x in at]
            if parity:
                values = [rotated(v, t, 32, -1) for t, v in enumerate(values)]
            filtered = []
            for re, im in fft(values, -1):
                factor = lax.rsqrt(lax.rsqrt((re * re + im * im) * scale))
                filtered.append((re * factor, im * factor))
            back.append(fft(filtered, 1))
        split_rows(unit + 1)
        for t in range(16):
            odd = rotated(back[1][t], t, 32, 1)
            upper = plus(back[0][t], odd)
            lower = minus(back[0][t], odd)
            at = pl.ds(t * 9, 8)
            pr[at, :], pi[at, :] = (v * (ramp(t) / 32) for v in upper)
            qr[at, :], qi[at, :] = (v * (ramp(t + 16) / 32) for v in lower)

    def inverse_columns(plans, units, g):
        rows = pl.ds(pl.multiple_of(g * 8, 8), 8)
        kept = []
        passed = []
        for h, masks, first, count in plans:
            group = len(masks) + 1
            values = [None] * 32
            for row in range(8 * count):
                unit = first + row // 8
                if unit == units - 1:
                    at = pl.ds(g * 72 + row % 8, 8, stride=9)
                    value = (pr[at, :] + above(qr[at, :]), pi[at, :] + above(qi[at, :]))
                else:
                    at = pl.ds(unit * 144 + g * 72 + row % 8, 8, stride=9)
                    value = (wr[at, :], wi[at, :])
                for k in range(group):
                    l = (row // 8 * group + k) * 8 + row % 8
                    values[l] = tuple(pltpu.roll(v, LANES - k * LANES // group, 1) if k else v for v in value)
            even = fft(values[0::2], 1)
            odd = fft(values[1::2], 1)
            own = []
            other = []
            for s in range(16):
                turned = rotated(odd[s], s, 32, 1)
                weight = here[h] * (ramp(s) / 32)
                own.append(tuple(v * weight for v in plus(even[s], turned)))
                weight = both[h] * (ramp(s + 16) / 32)
                other.append(tuple(v * weight for v in minus(even[s], turned)))
            kept.append(own)
            passed.append(other)
        power = [jnp.zeros((8, LANES), jnp.float32) for _ in range(tiles)]
        for s in range(16):
            arrived = [left([passed[h][s][part] for h in range(tiles)]) for part in range(2)]
            for h in range(tiles):
                value = tuple(kept[h][s][part] + arrived[part][h] for part in range(2))
                power[h] = keep(h, s, g, value, power[h])
        for h in range(tiles):
            energy[pl.ds(pl.multiple_of(h * 16 + g * 8, 8), 8), :] = power[h]

    def run(count, body):
        lax.fori_loop(0, count, lambda i, c: (body(i), c)[1], 0)

    for step in range(ITERS):
        needed = range(step - ITERS, blocks + ITERS - 1 - step)
        plans = []
        units = 0
        for h in range(tiles):
            masks = sharing(h, needed)
            plans.append((h, masks, units, 4 // (len(masks) + 1)))
            units += 4 // (len(masks) + 1)
        run(2, functools.partial(forward_columns, step, plans))
        run(units, windows)
        run(2, functools.partial(inverse_columns, plans, units))
    totals = [jnp.sum(sums[step * 16 : step * 16 + 8, :] + sums[step * 16 + 8 : step * 16 + 16, :]) for step in range(ITERS)]

    for step, total in enumerate(totals):
        out_ref[32, step : step + 1, :] = jnp.full((1, LANES), total)
    for part, ref in enumerate((zr, zi)):
        for s in range(16):
            out_ref[part * 16 + s, :, :] = ref[s, 0:16, :]


def filter_tiles(slabs, blocks, tiles, data):
    body = functools.partial(filter_kernel, slabs, blocks, tiles)
    return pl.pallas_call(
        body,
        out_shape=jax.ShapeDtypeStruct((33, 16, LANES), jnp.float32),
        in_specs=[pl.BlockSpec(memory_space=pltpu.VMEM)],
        out_specs=pl.BlockSpec(memory_space=pltpu.VMEM),
        scratch_shapes=[pltpu.VMEM((tiles * 16, 24, LANES), jnp.float32)] * 2
        + [pltpu.VMEM(((tiles * 4 + 1) * 136, LANES), jnp.float32)] * 2
        + [pltpu.VMEM((136, LANES), jnp.float32)] * 4
        + [pltpu.VMEM((tiles * 4 * 144, LANES), jnp.float32)] * 2
        + [pltpu.VMEM((144, LANES), jnp.float32)] * 4
        + [pltpu.VMEM((rows, LANES), jnp.float32) for rows in (tiles * 16, tiles * 32, ITERS * 16)],
        compiler_params=pltpu.CompilerParams(vmem_limit_bytes=16 << 20),
        name="filter_tiles",
    )(data)


def pack_kernel(in_ref, out_ref, turn):
    lane = lax.broadcasted_iota(jnp.int32, (8, LANES), 1)
    zero = jnp.zeros((8, LANES), jnp.float32)
    columns = [[in_ref[g * 8 : g * 8 + 8, c * LANES : (c + 1) * LANES] for g in range(2)] for c in range(16)]
    for c in range(16):
        after = columns[c + 1] if c < 15 else [zero, zero]
        before = columns[c - 1] if c else [zero, zero]
        at = c * IN_ROWS
        out_ref[at : at + 8, :] = columns[c][0]
        out_ref[at + 8 : at + 16, :] = columns[c][1]
        first = jnp.where(lane < 32, after[0], pltpu.roll(before[0], 64, 1))
        second = jnp.where(lane < 96, pltpu.roll(after[1], 64, 1), before[1])
        out_ref[at + 16 : at + 24, :] = jnp.where(lane < 64, first, second)
        turn[c * 8 : c * 8 + 8, :] = jnp.where(lane < 16, pltpu.roll(after[0], 96, 1), pltpu.roll(after[1], 112, 1))
    for q in range(4):
        rows = turn[pl.ds(q * 32, 8, stride=4), :]
        for u in range(1, 4):
            rows = jnp.where(lane // 32 == u, pltpu.roll(turn[pl.ds(q * 32 + u, 8, stride=4), :], 32 * u, 1), rows)
        for k in range(4):
            at = (q * 4 + k) * IN_ROWS + 24
            out_ref[at : at + 2, :] = rows[k * 2 : k * 2 + 2]


def pack(phase):
    return pl.pallas_call(
        pack_kernel,
        out_shape=jax.ShapeDtypeStruct((16 * IN_ROWS, LANES), jnp.float32),
        in_specs=[pl.BlockSpec(memory_space=pltpu.VMEM)],
        out_specs=pl.BlockSpec(memory_space=pltpu.VMEM),
        scratch_shapes=[pltpu.VMEM((128, LANES), jnp.float32)],
        compiler_params=pltpu.CompilerParams(vmem_limit_bytes=8 << 20),
        name="pack",
    )(phase)


def row_matrices():
    k = np.arange(32)
    angle = 2 * np.pi * (k[:, None] * k[None, :] % 32) / 32
    cos, sin = np.cos(angle), np.sin(angle)
    weight = np.array([ramp(t) / 32 for t in range(32)])[:, None]
    result = []
    for matrix in (np.block([[cos, sin], [-sin, cos]]), np.block([[cos * weight, -sin * weight], [sin * weight, cos * weight]])):
        whole = jnp.asarray(matrix, jnp.float32)
        high = whole.astype(jnp.bfloat16)
        low = (whole - high.astype(jnp.float32)).astype(jnp.bfloat16)
        result.append(jnp.concatenate([high, low, high], axis=1))
    return result


def column_kernel(in_ref, forward_ref, inverse_ref, out_ref, *scratch):
    zr, zi, yr, yi, wr, wi, shift_r, shift_i, gain, turn = scratch[:10]
    buffers = [scratch[10 + 8 * k : 18 + 8 * k] for k in range(2)]
    final = scratch[26:29]
    tile = lax.axis_index("rows")
    lane = lax.broadcasted_iota(jnp.int32, (8, LANES), 1)
    sub = lax.broadcasted_iota(jnp.int32, (8, LANES), 0)
    in_slab = lane & 7

    def inside(first):
        column = tile * 8 + (first - 2) + sub // 2
        return jnp.where((column >= 0) & (column < 128), 1.0, 0.0)

    def block(body):
        pl.when(tile >= 0)(body)

    def run(count, body):
        lax.fori_loop(0, count, lambda i, c: (body(i), c)[1], 0)

    zero = jnp.zeros((8, LANES), jnp.float32)
    for part in buffers:
        for ref in part[:4]:
            ref[256:272, :] = jnp.zeros((16, LANES), jnp.bfloat16)
        for ref in part[6:8]:
            ref[0:8, :] = zero
            ref[8:16, :] = zero

    def stacked(offset):
        return jnp.concatenate([in_ref[a * IN_ROWS + offset : a * IN_ROWS + offset + 8, :] for a in range(16)], axis=0)

    for k, offset in enumerate((0, 8, 16)):
        turned = stacked(offset).T
        for b in range(8):
            at = k * 136 + (b % 4 * 2 + b // 4 if k == 2 else b) * 17
            turn[at : at + 16, :] = turned[b * 16 : b * 16 + 16]
    tail = jnp.concatenate([in_ref[a * IN_ROWS + 24 : a * IN_ROWS + 26, :] for a in range(16)], axis=0)
    for q in range(4):
        for u in range(4):
            value = tail[q * 8 : q * 8 + 8]
            turn[pl.ds(408 + q * 32 + u, 8, stride=4), :] = pltpu.roll(value, LANES - 32 * u, 1) if u else value
    turned = turn[408:536, :].T[0:32]
    beyond = jnp.where(tile * 8 + 10 < 128, 1.0, 0.0)
    for ref, v in zip((zr, zi), cos_sin(turned)):
        for k in range(4):
            at = (k % 2) * 8 * PITCH + 24 + k // 2
            ref[pl.ds(at, 8, stride=PITCH), :] = v[k * 8 : k * 8 + 8] * beyond
    for g in range(2):
        for s in range(16):
            value = cos_sin(turn[pl.ds(g * 136 + s, 8, stride=17), :])
            for ref, v in zip((zr, zi), value):
                ref[pl.ds(s * PITCH + 4 + g, 8, stride=2), :] = v
    edge = tile * 8 + jnp.where(sub < 4, 8 + sub // 2, sub // 2 - 4)
    edge = jnp.where((edge >= 0) & (edge < 128), 1.0, 0.0)
    for s in range(16):
        value = cos_sin(turn[pl.ds(272 + s, 8, stride=17), :])
        for ref, v in zip((zr, zi), value):
            v = v * edge
            ref[s * PITCH + 20 : s * PITCH + 24, :] = v[0:4]
            ref[s * PITCH : s * PITCH + 4, :] = v[4:8]

    def forward_columns(first, width, j):
        near = []
        far = []
        power = zero
        for s in range(16):
            at = pl.ds(s * PITCH + 2 * first + j * 8, 8)
            after = pl.ds(s * PITCH + 2 * first + 2 + j * 8, 8)
            near.append((zr[at, :], zi[at, :]))
            far.append((zr[after, :], zi[after, :]))
            a, b = near[-1], far[-1]
            power = power + ((a[0] * a[0] + a[1] * a[1]) + (b[0] * b[0] + b[1] * b[1]))
        gain[pl.ds(pl.multiple_of(48 + j * 8, 8), 8), :] = power
        even = fft([plus(a, b) for a, b in zip(near, far)], -1)
        odd = odd_outputs([minus(a, b) for a, b in zip(near, far)])
        for l in range(32):
            to = pl.ds(l * 2 * width + j * 8, 8)
            yr[to, :], yi[to, :] = (even, odd)[l % 2][l // 2]

    def split(value):
        high = value.astype(jnp.bfloat16)
        return high, (value - high.astype(jnp.float32)).astype(jnp.bfloat16)

    def turn_in(chunk):
        for part, source in enumerate((yr, yi)):
            halves = []
            for g in range(2):
                parts = [source[pl.ds(chunk * 256 + i * 16 + g, 8, stride=2), :] for i in range(16)]
                halves.append(jnp.concatenate(parts, axis=0).T)
            high, low = buffers[chunk % 2][part], buffers[chunk % 2][2 + part]
            for a in range(16):
                value = jnp.concatenate([v[a * 8 : a * 8 + 8] for v in halves], axis=0)
                high[a * 16 : a * 16 + 16, :], low[a * 16 : a * 16 + 16, :] = split(value)

    def turn_out(chunk):
        pr, pi, qr, qi = buffers[chunk % 2][4:]
        for p, q, target in ((pr, qr, wr), (pi, qi, wi)):
            for g in range(2):
                parts = [p[a * 16 + g * 8 : a * 16 + g * 8 + 8, :] + q[a * 16 + g * 8 : a * 16 + g * 8 + 8, :] for a in range(16)]
                turned = jnp.concatenate(parts, axis=0).T
                for i in range(16):
                    target[pl.ds(chunk * 256 + i * 16 + g, 8, stride=2), :] = turned[i * 8 : i * 8 + 8]

    def window_gains(valid, width):
        count = 2 * width
        power = jnp.concatenate(
            [jnp.where(sub < 2 * valid - 8 * j, gain[48 + j * 8 : 56 + j * 8, :], 0.0) for j in range(count // 8)], axis=0
        )
        row = lax.broadcasted_iota(jnp.int32, (16, LANES), 0)
        slab = lax.broadcasted_iota(jnp.int32, (16, LANES), 1) // 8
        pick = jnp.where((slab == row) | (slab == row + 1), 1.0, 0.0)
        exact = dict(precision=lax.Precision.HIGHEST, preferred_element_type=jnp.float32)
        mean = lax.dot_general(pick, power, (((1,), (1,)), ((), ())), **exact)
        column = lax.broadcasted_iota(jnp.int32, (count, 32 * width), 1)
        column = column - width * ((column.astype(jnp.float32) + 0.5) * (1.0 / width)).astype(jnp.int32)
        spread = jnp.where(column == lax.broadcasted_iota(jnp.int32, (count, 32 * width), 0) // 2, 1.0, 0.0)
        mean = lax.dot_general(mean, spread, (((1,), (0,)), ((), ())), **exact)
        for c in range(width // 4):
            gain[c * 16 : c * 16 + 16, :] = 1.0 / (mean[:, c * 128 : c * 128 + 128] + EPS)

    def residues():
        def corner(s):
            at = s * PITCH + 4 if s < 16 else 6
            result = []
            for ref in (zr, zi):
                top = ref[pl.ds(at, 8, stride=2), :]
                low = ref[pl.ds(at + 1, 8, stride=2), :]
                top_left = pltpu.roll(top, LANES - 1, 1)
                low_left = pltpu.roll(low, LANES - 1, 1)
                top_under = jnp.where(in_slab < 7, top_left, pltpu.roll(low, 7, 1))
                low_under = jnp.where(in_slab < 7, low_left, jnp.where(lane < LANES - 1, top_left, 0.0))
                result.append((top, low, top_under, low_under))
            return [((result[0][g], result[1][g]), (result[0][2 + g], result[1][2 + g])) for g in range(2)]

        def cross(a, b):
            return a[1] * b[0] - a[0] * b[1]

        total = zero
        here = corner(0)
        down = [cross(*pair) for pair in here]
        for s in range(16):
            following = corner(s + 1)
            following_down = [cross(*pair) for pair in following]
            for g in range(2):
                across = cross(here[g][0], following[g][0]) - cross(here[g][1], following[g][1])
                loop = across + (following_down[g] - down[g])
                total = total + loop * loop
            here, down = following, following_down
        return total

    def windows(chunk, pair):
        hr, hi, lr, li, pr, pi, qr, qi = buffers[chunk % 2]
        data = []
        scale = []
        for a in (2 * pair, 2 * pair + 1):
            rows = slice(a * 16, a * 16 + 32)
            data.append(jnp.concatenate([hr[rows, :], hi[rows, :], hr[rows, :], hi[rows, :], lr[rows, :], li[rows, :]], axis=0))
            scale.append(jnp.broadcast_to(gain[chunk * 16 + a : chunk * 16 + a + 1, :], (32, LANES)))
        spectrum = jnp.dot(forward_ref[...], jnp.concatenate(data, axis=1), preferred_element_type=jnp.float32)
        re, im = spectrum[0:32], spectrum[32:64]
        factor = lax.rsqrt(lax.rsqrt((re * re + im * im) * jnp.concatenate(scale, axis=1)))
        high, low = split(jnp.concatenate([re * factor, im * factor], axis=0))
        back = jnp.dot(inverse_ref[...], jnp.concatenate([high, high, low], axis=0), preferred_element_type=jnp.float32)
        for k in range(2):
            at = (2 * pair + k) * 16
            part = back[:, k * LANES : (k + 1) * LANES]
            pr[at : at + 16, :], qr[at + 16 : at + 32, :] = part[0:16], part[16:32]
            pi[at : at + 16, :], qi[at + 16 : at + 32, :] = part[32:48], part[48:64]

    def inverse_columns(first, width, last, j):
        here = inside(first + 4 * j)
        both = here * inside(first + 4 * j + 1)
        values = []
        for l in range(32):
            at = pl.ds(l * 2 * width + 8 * j, 8)
            values.append((wr[at, :], wi[at, :]))
        even = fft(values[0::2], 1)
        odd = join(fft(values[1::4], 1), fft(values[3::4], 1), 32, 1)
        for s in range(16):
            weight = here * (ramp(s) / 32)
            own = [v * weight for v in plus(even[s], odd[s])]
            weight = both * (ramp(s + 16) / 32)
            other = [v * weight for v in minus(even[s], odd[s])]
            for part, (ref, shift) in enumerate(((zr, shift_r), (zi, shift_i))):
                if last:
                    base = part * 304 + s * 19 + 8 * j
                    final[0][pl.ds(base, 8), :] = own[part]
                    final[1][pl.ds(base + 2, 8), :] = other[part]
                else:
                    shift[pl.ds(s * 32 + 8 * j + 2, 8), :] = other[part]
                    value = own[part] + shift[pl.ds(s * 32 + 8 * j, 8), :]
                    ref[pl.ds(s * PITCH + 2 * first + 8 * j, 8), :] = value

    for k in range(32):
        final[1][k * 19 : k * 19 + 2, :] = zero[0:2]

    def iteration(step, width, last):
        chunks = width // 4
        run(chunks, functools.partial(forward_columns, step, width))

        @block
        def _():
            window_gains(12 - 2 * step, width)
            turn_in(0)
            final[2][pl.ds(step * 8, 8), :] = residues()

        for chunk in range(chunks):

            @block
            def _():
                if chunk + 1 < chunks:
                    turn_in(chunk + 1)
                for pair in range(8):
                    windows(chunk, pair)
                if chunk:
                    turn_out(chunk - 1)

        block(lambda: turn_out(chunks - 1))
        run(chunks, functools.partial(inverse_columns, step, width, last))

    run(ITERS - 1, lambda step: iteration(step, 12, False))
    iteration(ITERS - 1, 8, True)

    spill = []
    for part in range(2):
        for g in range(2):
            base = part * 304 + g
            rows = []
            for b in range(8):
                for s in (0, 8):
                    at = pl.ds(base + s * 19 + 2 * b, 8, stride=19)
                    rows.append(final[0][at, :] + final[1][at, :])
            turned = jnp.concatenate(rows, axis=0).T
            for a in range(16):
                at = a * OUT_ROWS + part * 16 + g * 8
                out_ref[at : at + 8, :] = turned[a * 8 : a * 8 + 8]
            spill += [final[1][pl.ds(base + s * 19 + 16, 8, stride=19), :] for s in (0, 8)]
    turned = jnp.concatenate(spill + spill, axis=0).T
    report = zero[0:1]
    for step in range(ITERS):
        total = jnp.sum(final[2][step * 8 : step * 8 + 8, :])
        report = jnp.where(lane[0:1] == step * 16 + tile, total, report)
    for a in range(16):
        value = turned[a * 8 : a * 8 + 8]
        out_ref[a * OUT_ROWS + 32 : a * OUT_ROWS + 36, :] = jnp.where(lane[0:4] < 64, value[0:4], value[4:8])
        out_ref[a * OUT_ROWS + 36 : a * OUT_ROWS + 37, :] = report


def filter_columns(data):
    def rows(count):
        return pltpu.VMEM((count, LANES), jnp.float32)

    return pl.pallas_call(
        column_kernel,
        out_shape=jax.ShapeDtypeStruct((16 * OUT_ROWS, LANES), jnp.float32),
        in_specs=[pl.BlockSpec(memory_space=pltpu.VMEM)] * 3,
        out_specs=pl.BlockSpec(memory_space=pltpu.VMEM),
        scratch_shapes=[rows(16 * PITCH)] * 2
        + [rows(776)] * 4
        + [rows(520)] * 2
        + [rows(80), rows(544)]
        + ([pltpu.VMEM((272, LANES), jnp.bfloat16)] * 4 + [rows(272)] * 4) * 2
        + [rows(624), rows(624), rows(ITERS * 8)],
        compiler_params=pltpu.CompilerParams(vmem_limit_bytes=16 << 20),
        name="filter_columns",
    )(data, *row_matrices())


def finish_kernel(scale, in_ref, field_ref, profile_ref):
    lane = lax.broadcasted_iota(jnp.int32, (8, LANES), 1)
    extras = []
    sums = jnp.zeros((1, LANES), jnp.float32)
    for c in range(16):
        half = in_ref[c * OUT_ROWS + 32 : c * OUT_ROWS + 36, :]
        extras.append(jnp.concatenate([half, pltpu.roll(half, 64, 1)], axis=0))
        sums = sums + in_ref[c * OUT_ROWS + 36 : c * OUT_ROWS + 37, :]
    for step in range(ITERS):
        profile_ref[step : step + 1, :] = sums[:, step * 16 : step * 16 + 16] * scale
    for part in range(2):
        for g in range(2):
            offset = (part * 2 + g) * 16
            for c in range(16):
                at = c * OUT_ROWS + part * 16 + g * 8
                value = in_ref[at : at + 8, :]
                if c:
                    spill = pltpu.roll(extras[c - 1], LANES - offset, 1) if offset else extras[c - 1]
                    value = value + jnp.where(lane < 16, spill, 0.0)
                field_ref[part, g * 8 : g * 8 + 8, c * LANES : (c + 1) * LANES] = value


def finish(scale, data):
    return pl.pallas_call(
        functools.partial(finish_kernel, scale),
        out_shape=(
            jax.ShapeDtypeStruct((2, 16, 16 * LANES), jnp.float32),
            jax.ShapeDtypeStruct((ITERS, 16), jnp.float32),
        ),
        in_specs=[pl.BlockSpec(memory_space=pltpu.VMEM)],
        out_specs=[pl.BlockSpec(memory_space=pltpu.VMEM)] * 2,
        compiler_params=pltpu.CompilerParams(vmem_limit_bytes=8 << 20),
        name="finish",
    )(data)


def ring_of_blocks(phase, devices, blocks, tiles):
    per_tile = LANES // devices
    ring = tiles * per_tile
    width = phase.shape[1]
    padded = jnp.pad(phase, ((0, 0), (HALO * 16, (ring + HALO) * 16)))
    pieces = []
    for d in range(devices):
        start = d * blocks * 16
        ahead = padded[:, start + HALO * 16 : start + (blocks + 2 * HALO) * 16]
        behind = padded[:, start : start + HALO * 16]
        gap = jnp.zeros((16, (ring - blocks - 2 * HALO) * 16), phase.dtype)
        pieces.append(jnp.concatenate([ahead, gap, behind], axis=1))
    return jnp.stack(pieces)


def per_device(phase):
    devices = lax.axis_size("rows")
    height, width = phase.shape
    blocks = width // (16 * devices)
    per_tile = LANES // devices
    if height != 16 or LANES % devices or blocks * 16 * devices != width or blocks != per_tile:
        raise ValueError("unsupported sizes")
    scale = 1.0 / (height * devices * 128.0)
    if devices == 16:
        data = lax.all_to_all(pack(phase).reshape(16, IN_ROWS, 1, LANES), "rows", 0, 0)
        result = filter_columns(data.reshape(16 * IN_ROWS, LANES))
        result = lax.all_to_all(result.reshape(16, OUT_ROWS, 1, LANES), "rows", 0, 0)
        result = result.reshape(16 * OUT_ROWS, LANES)
        return finish(scale, result)
    tiles = -(-(blocks + 2 * HALO) // per_tile)
    data = lax.all_to_all(ring_of_blocks(phase, devices, blocks, tiles), "rows", 0, 0)
    data = data.reshape(devices, 16, tiles, per_tile, 16).transpose(2, 4, 1, 3, 0)
    result = filter_tiles(devices, blocks, tiles, data.reshape(tiles, 16, 16, LANES))
    field = result[:32].reshape(2, 16, 16, per_tile, devices).transpose(4, 0, 2, 3, 1)
    field = field.reshape(devices, 32, per_tile * 16)
    sums = jnp.broadcast_to(result[32, :ITERS, : per_tile * 16][None], (devices, ITERS, per_tile * 16))
    result = lax.all_to_all(jnp.concatenate([field, sums], axis=1), "rows", 0, 0)
    field = result[:, :32].reshape(devices, 2, 16, per_tile * 16).transpose(1, 2, 0, 3).reshape(2, 16, width)
    profile = result[:, 32:, 0].reshape(width // 128, -1, ITERS).sum(1).T
    return field, profile * scale


def solution(mesh):
    return jax.shard_map(
        per_device,
        mesh=mesh,
        in_specs=(P(("groups", "rows"), None),),
        out_specs=(P(None, ("groups", "rows"), None), P("groups", None)),
        check_vma=False,
    )
```

```python
import functools
import math

import jax
import jax.numpy as jnp
import numpy as np
from jax import lax
from jax.experimental import pallas as pl
from jax.experimental.pallas import tpu as pltpu
from jax.sharding import PartitionSpec as P

ITERS = 3
EPS = 1e-06
LANES = 128
IN_ROWS = 26
OUT_ROWS = 37
PITCH = 41
HALO = 3

SIN = (9.99999996e-01, -1.66666580e-01, 8.33305053e-03, -1.98090400e-04, 2.60515161e-06)
COS = (9.99999953e-01, -4.99999050e-01, 4.16635780e-02, -1.38536600e-03, 2.31530144e-05)


def rotated(value, k, size, sign):
    re, im = value
    half = math.sqrt(0.5)
    if k == 0:
        return re, im
    if 4 * k == size:
        return (im, -re) if sign < 0 else (-im, re)
    if 8 * k == size:
        return ((re + im) * half, (im - re) * half) if sign < 0 else ((re - im) * half, (im + re) * half)
    if 8 * k == 3 * size:
        return ((im - re) * half, (re + im) * -half) if sign < 0 else ((re + im) * -half, (re - im) * half)
    if 2 * k > size:
        return rotated((-re, -im), k - size // 2, size, sign)
    c = math.cos(2 * math.pi * k / size)
    s = sign * math.sin(2 * math.pi * k / size)
    return re * c - im * s, im * c + re * s


def plus(a, b):
    return a[0] + b[0], a[1] + b[1]


def minus(a, b):
    return a[0] - b[0], a[1] - b[1]


def quarter_turn(a, sign):
    return (-a[1], a[0]) if sign > 0 else (a[1], -a[0])


def join(one, three, size, sign):
    quarter = size // 4
    one = [rotated(one[k], k, size, sign) for k in range(quarter)]
    three = [rotated(three[k], 3 * k, size, sign) for k in range(quarter)]
    turned = [quarter_turn(minus(a, b), sign) for a, b in zip(one, three)]
    return [plus(a, b) for a, b in zip(one, three)] + turned


def fft(values, sign):
    size = len(values)
    if size == 1:
        return values
    if size == 2:
        return [plus(*values), minus(*values)]
    even = fft(values[0::2], sign)
    odd = join(fft(values[1::4], sign), fft(values[3::4], sign), size, sign)
    return [plus(e, o) for e, o in zip(even, odd)] + [minus(e, o) for e, o in zip(even, odd)]


def odd_outputs(differences):
    one = []
    three = []
    for k in range(8):
        turned = quarter_turn(differences[k + 8], -1)
        one.append(rotated(plus(differences[k], turned), k, 32, -1))
        three.append(rotated(minus(differences[k], turned), 3 * k, 32, -1))
    pairs = zip(fft(one, -1), fft(three, -1))
    return [value for pair in pairs for value in pair]


def polynomial(coefficients, w):
    result = jnp.full_like(w, coefficients[-1])
    for c in coefficients[-2::-1]:
        result = result * w + c
    return result


def cos_sin(x):
    u = (jnp.abs(x) - jnp.float32(math.pi / 2)) + jnp.float32(4.371139e-08)
    w = u * u
    cosine = -(u * polynomial(SIN, w))
    sine = polynomial(COS, w)
    return cosine, jnp.where(x < 0, -sine, sine)


def ramp(t):
    return 1.0 - abs(t - 15.5) / 16.0


def filter_kernel(
    slabs, blocks, tiles, in_ref, out_ref, zr, zi, yr, yi, ur, ui, vr, vi, wr, wi, pr, pi, qr, qi, energy, gain, sums
):
    tile = lax.axis_index("rows")
    per_tile = LANES // slabs
    ring = tiles * per_tile
    lane = lax.broadcasted_iota(jnp.int32, (8, LANES), 1)
    sub = lax.broadcasted_iota(jnp.int32, (8, LANES), 0)
    not_last = lane % slabs != slabs - 1
    not_first = lane % slabs != 0
    place = lane // slabs

    def inside(h, step):
        position = (h * per_tile + place + step) % ring
        relative = jnp.where(position < blocks + HALO, position, position - ring)
        column = tile * blocks + relative
        return jnp.where((column >= 0) & (column < slabs * blocks), 1.0, 0.0)

    here = [inside(h, 0) for h in range(tiles)]
    both = [here[h] * inside(h, 1) for h in range(tiles)]

    def right(values, active):
        if per_tile == 1:
            return [values[(h + 1) % tiles] for h in active]
        moved = [pltpu.roll(v, LANES - slabs, 1) for v in values]
        return [jnp.where(lane < LANES - slabs, moved[h], moved[(h + 1) % tiles]) for h in active]

    def left(values):
        if per_tile == 1:
            return [values[h - 1] for h in range(tiles)]
        moved = [pltpu.roll(v, slabs, 1) for v in values]
        return [jnp.where(lane < slabs, moved[h - 1], moved[h]) for h in range(tiles)]

    def below(value):
        return jnp.where(not_last, pltpu.roll(value, LANES - 1, 1), 0.0)

    def above(value):
        return jnp.where(not_first, pltpu.roll(value, 1, 1), 0.0)

    def keep(h, s, g, value, power):
        for part, ref in enumerate((zr, zi)):
            ref[h * 16 + s, pl.ds(g * 8, 8), :] = value[part]
            if h == 0 or s == 0:
                ref[h * 16 + s, pl.ds(16 + g, 1), :] = below(value[part])[0:1]
        return power + (value[0] * value[0] + value[1] * value[1])

    for h in range(tiles):
        for g in range(2):
            phases = [in_ref[h, s, g * 8 : g * 8 + 8, :] for s in range(16)]
            power = jnp.zeros((8, LANES), jnp.float32)
            for s in range(16):
                cosine, sine = cos_sin(phases[s])
                power = keep(h, s, g, (cosine * here[h], sine * here[h]), power)
            energy[h * 16 + g * 8 : h * 16 + g * 8 + 8, :] = power

    def sharing(h, needed):
        places = {w % ring - h * per_tile for w in needed}
        places = {p for p in places if 0 <= p < per_tile}
        group = 1
        for k in (2, 4):
            if per_tile % k == 0:
                taken = {(p + j * (per_tile // k)) % per_tile for p in places for j in range(k)}
                group = k if len(taken) == k * len(places) else group
        masks = []
        for k in range(1, group):
            mask = place < 0
            for p in places:
                mask = mask | (place == (p + k * (per_tile // group)) % per_tile)
            masks.append(mask)
        return masks

    def merged(values, masks):
        result = values[0]
        for k, mask in enumerate(masks):
            result = jnp.where(mask, pltpu.roll(values[k + 1], (k + 1) * LANES // (len(masks) + 1), 1), result)
        return result

    def window_gains(plans):
        both_rows = [energy[h * 16 : h * 16 + 8, :] + energy[h * 16 + 8 : h * 16 + 16, :] for h in range(tiles)]
        blockwise = [jnp.broadcast_to(jnp.sum(e, axis=0, keepdims=True), (8, LANES)) for e in both_rows]
        tall = [e + below(e) for e in blockwise]
        for unit, ((h, masks, first, count), wide) in enumerate(zip(plans, right(tall, [p[0] for p in plans]))):
            value = merged([1.0 / ((tall[h] + wide) + EPS)] * 4, masks)
            for j in range(count):
                gain[(first + j) * 8 : (first + j) * 8 + 8, :] = value

    def forward_columns(step, plans, g):
        rows = pl.ds(pl.multiple_of(g * 8, 8), 8)
        under = pl.ds(g * 8 + 1, 8)
        active = [p[0] for p in plans]
        window_gains(plans)
        near = {h: [] for h in active}
        far = {h: [] for h in active}
        for s in range(16):
            re = [zr[h * 16 + s, rows, :] for h in range(tiles)]
            im = [zi[h * 16 + s, rows, :] for h in range(tiles)]
            for h, a, b in zip(active, right(re, active), right(im, active)):
                near[h].append((re[h], im[h]))
                far[h].append((a, b))
        for h, masks, first, count in plans:
            group = len(masks) + 1
            even = fft([plus(a, b) for a, b in zip(near[h], far[h])], -1)
            odd = fft([rotated(minus(a, b), s, 32, -1) for s, (a, b) in enumerate(zip(near[h], far[h]))], -1)
            for row in range(8 * count):
                sources = [(row // 8 * group + k) * 8 + row % 8 for k in range(group)]
                values = [(even, odd)[l % 2][l // 2] for l in sources]
                value = tuple(merged([v[part] for v in values], masks) for part in range(2))
                at = pl.ds((first * 8 + row) * 17 + g * 8, 8)
                if first == 0 and row < 8:
                    following = (below(value[0]), below(value[1]))
                    ur[at, :], ui[at, :] = plus(value, following)
                    vr[at, :], vi[at, :] = minus(value, following)
                else:
                    yr[at, :], yi[at, :] = value

        def corner(s):
            if s < 16:
                return near[0][s], (zr[s, under, :], zi[s, under, :])
            moved = [right([ref[h * 16, under, :] for h in range(tiles)], (0,))[0] for ref in (zr, zi)]
            return far[0][0], tuple(moved)

        def cross(a, b):
            return a[1] * b[0] - a[0] * b[1]

        total = jnp.zeros((8, LANES), jnp.float32)
        here_, under_ = corner(0)
        down = cross(here_, under_)
        for s in range(16):
            next_, next_under = corner(s + 1)
            next_down = cross(next_, next_under)
            loop = (cross(here_, next_) - cross(under_, next_under)) + (next_down - down)
            total = total + loop * loop
            here_, under_, down = next_, next_under, next_down
        sums[pl.ds(pl.multiple_of(step * 16 + g * 8, 8), 8), :] = total

    def split_rows(unit):
        for row in range(8):
            for g in range(2):
                source = pl.ds((unit * 8 + row) * 17 + g * 8, 8)
                at = pl.ds(row * 17 + g * 8, 8)
                value = (yr[source, :], yi[source, :])
                following = (below(value[0]), below(value[1]))
                ur[at, :], ui[at, :] = plus(value, following)
                vr[at, :], vi[at, :] = minus(value, following)

    def join_rows(unit):
        for t in range(16):
            source = pl.ds(t * 9, 8)
            at = pl.ds((unit * 16 + t) * 9, 8)
            wr[at, :] = pr[source, :] + above(qr[source, :])
            wi[at, :] = pi[source, :] + above(qi[source, :])

    def windows(unit):
        join_rows(jnp.maximum(unit - 1, 0))
        scale = gain[pl.ds(pl.multiple_of(unit * 8, 8), 8), :]
        at = [pl.ds(t, 8, stride=17) for t in range(16)]
        back = []
        for parity, (a, b) in enumerate(((ur, ui), (vr, vi))):
            values = [(a[x, :], b[x, :]) for x in at]
            if parity:
                values = [rotated(v, t, 32, -1) for t, v in enumerate(values)]
            filtered = []
            for re, im in fft(values, -1):
                factor = lax.rsqrt(lax.rsqrt((re * re + im * im) * scale))
                filtered.append((re * factor, im * factor))
            back.append(fft(filtered, 1))
        split_rows(unit + 1)
        for t in range(16):
            odd = rotated(back[1][t], t, 32, 1)
            upper = plus(back[0][t], odd)
            lower = minus(back[0][t], odd)
            at = pl.ds(t * 9, 8)
            pr[at, :], pi[at, :] = (v * (ramp(t) / 32) for v in upper)
            qr[at, :], qi[at, :] = (v * (ramp(t + 16) / 32) for v in lower)

    def inverse_columns(plans, units, g):
        rows = pl.ds(pl.multiple_of(g * 8, 8), 8)
        kept = []
        passed = []
        for h, masks, first, count in plans:
            group = len(masks) + 1
            values = [None] * 32
            for row in range(8 * count):
                unit = first + row // 8
                if unit == units - 1:
                    at = pl.ds(g * 72 + row % 8, 8, stride=9)
                    value = (pr[at, :] + above(qr[at, :]), pi[at, :] + above(qi[at, :]))
                else:
                    at = pl.ds(unit * 144 + g * 72 + row % 8, 8, stride=9)
                    value = (wr[at, :], wi[at, :])
                for k in range(group):
                    l = (row // 8 * group + k) * 8 + row % 8
                    values[l] = tuple(pltpu.roll(v, LANES - k * LANES // group, 1) if k else v for v in value)
            even = fft(values[0::2], 1)
            odd = fft(values[1::2], 1)
            own = []
            other = []
            for s in range(16):
                turned = rotated(odd[s], s, 32, 1)
                weight = here[h] * (ramp(s) / 32)
                own.append(tuple(v * weight for v in plus(even[s], turned)))
                weight = both[h] * (ramp(s + 16) / 32)
                other.append(tuple(v * weight for v in minus(even[s], turned)))
            kept.append(own)
            passed.append(other)
        power = [jnp.zeros((8, LANES), jnp.float32) for _ in range(tiles)]
        for s in range(16):
            arrived = [left([passed[h][s][part] for h in range(tiles)]) for part in range(2)]
            for h in range(tiles):
                value = tuple(kept[h][s][part] + arrived[part][h] for part in range(2))
                power[h] = keep(h, s, g, value, power[h])
        for h in range(tiles):
            energy[pl.ds(pl.multiple_of(h * 16 + g * 8, 8), 8), :] = power[h]

    def run(count, body):
        lax.fori_loop(0, count, lambda i, c: (body(i), c)[1], 0)

    for step in range(ITERS):
        needed = range(step - ITERS, blocks + ITERS - 1 - step)
        plans = []
        units = 0
        for h in range(tiles):
            masks = sharing(h, needed)
            plans.append((h, masks, units, 4 // (len(masks) + 1)))
            units += 4 // (len(masks) + 1)
        run(2, functools.partial(forward_columns, step, plans))
        run(units, windows)
        run(2, functools.partial(inverse_columns, plans, units))
    totals = [jnp.sum(sums[step * 16 : step * 16 + 8, :] + sums[step * 16 + 8 : step * 16 + 16, :]) for step in range(ITERS)]

    for step, total in enumerate(totals):
        out_ref[32, step : step + 1, :] = jnp.full((1, LANES), total)
    for part, ref in enumerate((zr, zi)):
        for s in range(16):
            out_ref[part * 16 + s, :, :] = ref[s, 0:16, :]


def filter_tiles(slabs, blocks, tiles, data):
    body = functools.partial(filter_kernel, slabs, blocks, tiles)
    return pl.pallas_call(
        body,
        out_shape=jax.ShapeDtypeStruct((33, 16, LANES), jnp.float32),
        in_specs=[pl.BlockSpec(memory_space=pltpu.VMEM)],
        out_specs=pl.BlockSpec(memory_space=pltpu.VMEM),
        scratch_shapes=[pltpu.VMEM((tiles * 16, 24, LANES), jnp.float32)] * 2
        + [pltpu.VMEM(((tiles * 4 + 1) * 136, LANES), jnp.float32)] * 2
        + [pltpu.VMEM((136, LANES), jnp.float32)] * 4
        + [pltpu.VMEM((tiles * 4 * 144, LANES), jnp.float32)] * 2
        + [pltpu.VMEM((144, LANES), jnp.float32)] * 4
        + [pltpu.VMEM((rows, LANES), jnp.float32) for rows in (tiles * 16, tiles * 32, ITERS * 16)],
        compiler_params=pltpu.CompilerParams(vmem_limit_bytes=16 << 20),
        name="filter_tiles",
    )(data)


def pack_kernel(in_ref, out_ref, turn):
    lane = lax.broadcasted_iota(jnp.int32, (8, LANES), 1)
    zero = jnp.zeros((8, LANES), jnp.float32)
    columns = [[in_ref[g * 8 : g * 8 + 8, c * LANES : (c + 1) * LANES] for g in range(2)] for c in range(16)]
    for c in range(16):
        after = columns[c + 1] if c < 15 else [zero, zero]
        before = columns[c - 1] if c else [zero, zero]
        at = c * IN_ROWS
        out_ref[at : at + 8, :] = columns[c][0]
        out_ref[at + 8 : at + 16, :] = columns[c][1]
        first = jnp.where(lane < 32, after[0], pltpu.roll(before[0], 64, 1))
        second = jnp.where(lane < 96, pltpu.roll(after[1], 64, 1), before[1])
        out_ref[at + 16 : at + 24, :] = jnp.where(lane < 64, first, second)
        turn[c * 8 : c * 8 + 8, :] = jnp.where(lane < 16, pltpu.roll(after[0], 96, 1), pltpu.roll(after[1], 112, 1))
    for q in range(4):
        rows = turn[pl.ds(q * 32, 8, stride=4), :]
        for u in range(1, 4):
            rows = jnp.where(lane // 32 == u, pltpu.roll(turn[pl.ds(q * 32 + u, 8, stride=4), :], 32 * u, 1), rows)
        for k in range(4):
            at = (q * 4 + k) * IN_ROWS + 24
            out_ref[at : at + 2, :] = rows[k * 2 : k * 2 + 2]


def pack(phase):
    return pl.pallas_call(
        pack_kernel,
        out_shape=jax.ShapeDtypeStruct((16 * IN_ROWS, LANES), jnp.float32),
        in_specs=[pl.BlockSpec(memory_space=pltpu.VMEM)],
        out_specs=pl.BlockSpec(memory_space=pltpu.VMEM),
        scratch_shapes=[pltpu.VMEM((128, LANES), jnp.float32)],
        compiler_params=pltpu.CompilerParams(vmem_limit_bytes=8 << 20),
        name="pack",
    )(phase)


def row_matrices():
    k = np.arange(32)
    angle = 2 * np.pi * (k[:, None] * k[None, :] % 32) / 32
    cos, sin = np.cos(angle), np.sin(angle)
    weight = np.array([ramp(t) / 32 for t in range(32)])[:, None]
    result = []
    for matrix in (np.block([[cos, sin], [-sin, cos]]), np.block([[cos * weight, -sin * weight], [sin * weight, cos * weight]])):
        whole = jnp.asarray(matrix, jnp.float32)
        high = whole.astype(jnp.bfloat16)
        low = (whole - high.astype(jnp.float32)).astype(jnp.bfloat16)
        result.append(jnp.concatenate([high, low, high], axis=1))
    return result


def column_kernel(in_ref, forward_ref, inverse_ref, out_ref, *scratch):
    zr, zi, yr, yi, wr, wi, shift_r, shift_i, gain, turn = scratch[:10]
    buffers = [scratch[10 + 8 * k : 18 + 8 * k] for k in range(2)]
    final = scratch[26:29]
    tile = lax.axis_index("rows")
    lane = lax.broadcasted_iota(jnp.int32, (8, LANES), 1)
    sub = lax.broadcasted_iota(jnp.int32, (8, LANES), 0)
    in_slab = lane & 7

    def inside(first):
        column = tile * 8 + (first - 2) + sub // 2
        return jnp.where((column >= 0) & (column < 128), 1.0, 0.0)

    def block(body):
        pl.when(tile >= 0)(body)

    def run(count, body):
        lax.fori_loop(0, count, lambda i, c: (body(i), c)[1], 0)

    zero = jnp.zeros((8, LANES), jnp.float32)
    for part in buffers:
        for ref in part[:4]:
            ref[256:272, :] = jnp.zeros((16, LANES), jnp.bfloat16)
        for ref in part[6:8]:
            ref[0:8, :] = zero
            ref[8:16, :] = zero

    def stacked(offset):
        return jnp.concatenate([in_ref[a * IN_ROWS + offset : a * IN_ROWS + offset + 8, :] for a in range(16)], axis=0)

    for k, offset in enumerate((0, 8, 16)):
        turned = stacked(offset).T
        for b in range(8):
            at = k * 136 + (b % 4 * 2 + b // 4 if k == 2 else b) * 17
            turn[at : at + 16, :] = turned[b * 16 : b * 16 + 16]
    tail = jnp.concatenate([in_ref[a * IN_ROWS + 24 : a * IN_ROWS + 26, :] for a in range(16)], axis=0)
    for q in range(4):
        for u in range(4):
            value = tail[q * 8 : q * 8 + 8]
            turn[pl.ds(408 + q * 32 + u, 8, stride=4), :] = pltpu.roll(value, LANES - 32 * u, 1) if u else value
    turned = turn[408:536, :].T[0:32]
    beyond = jnp.where(tile * 8 + 10 < 128, 1.0, 0.0)
    for ref, v in zip((zr, zi), cos_sin(turned)):
        for k in range(4):
            at = (k % 2) * 8 * PITCH + 24 + k // 2
            ref[pl.ds(at, 8, stride=PITCH), :] = v[k * 8 : k * 8 + 8] * beyond
    for g in range(2):
        for s in range(16):
            value = cos_sin(turn[pl.ds(g * 136 + s, 8, stride=17), :])
            for ref, v in zip((zr, zi), value):
                ref[pl.ds(s * PITCH + 4 + g, 8, stride=2), :] = v
    edge = tile * 8 + jnp.where(sub < 4, 8 + sub // 2, sub // 2 - 4)
    edge = jnp.where((edge >= 0) & (edge < 128), 1.0, 0.0)
    for s in range(16):
        value = cos_sin(turn[pl.ds(272 + s, 8, stride=17), :])
        for ref, v in zip((zr, zi), value):
            v = v * edge
            ref[s * PITCH + 20 : s * PITCH + 24, :] = v[0:4]
            ref[s * PITCH : s * PITCH + 4, :] = v[4:8]

    def forward_columns(first, width, j):
        near = []
        far = []
        power = zero
        for s in range(16):
            at = pl.ds(s * PITCH + 2 * first + j * 8, 8)
            after = pl.ds(s * PITCH + 2 * first + 2 + j * 8, 8)
            near.append((zr[at, :], zi[at, :]))
            far.append((zr[after, :], zi[after, :]))
            a, b = near[-1], far[-1]
            power = power + ((a[0] * a[0] + a[1] * a[1]) + (b[0] * b[0] + b[1] * b[1]))
        gain[pl.ds(pl.multiple_of(48 + j * 8, 8), 8), :] = power
        even = fft([plus(a, b) for a, b in zip(near, far)], -1)
        odd = odd_outputs([minus(a, b) for a, b in zip(near, far)])
        for l in range(32):
            to = pl.ds(j * 256 + l * 8, 8)
            yr[to, :], yi[to, :] = (even, odd)[l % 2][l // 2]

    def split(value):
        high = value.astype(jnp.bfloat16)
        return high, (value - high.astype(jnp.float32)).astype(jnp.bfloat16)

    def turn_in(chunk):
        for part, source in enumerate((yr, yi)):
            halves = []
            for g in range(2):
                parts = [source[pl.ds(chunk * 256 + i * 16 + g, 8, stride=2), :] for i in range(16)]
                halves.append(jnp.concatenate(parts, axis=0).T)
            high, low = buffers[chunk % 2][part], buffers[chunk % 2][2 + part]
            for a in range(16):
                value = jnp.concatenate([v[a * 8 : a * 8 + 8] for v in halves], axis=0)
                high[a * 16 : a * 16 + 16, :], low[a * 16 : a * 16 + 16, :] = split(value)

    def turn_out(chunk):
        pr, pi, qr, qi = buffers[chunk % 2][4:]
        for p, q, target in ((pr, qr, wr), (pi, qi, wi)):
            for g in range(2):
                parts = [p[a * 16 + g * 8 : a * 16 + g * 8 + 8, :] + q[a * 16 + g * 8 : a * 16 + g * 8 + 8, :] for a in range(16)]
                turned = jnp.concatenate(parts, axis=0).T
                for i in range(16):
                    target[pl.ds(chunk * 256 + i * 16 + g, 8, stride=2), :] = turned[i * 8 : i * 8 + 8]

    def window_gains(valid, width):
        count = 2 * width
        power = jnp.concatenate(
            [jnp.where(sub < 2 * valid - 8 * j, gain[48 + j * 8 : 56 + j * 8, :], 0.0) for j in range(count // 8)], axis=0
        )
        row = lax.broadcasted_iota(jnp.int32, (16, LANES), 0)
        slab = lax.broadcasted_iota(jnp.int32, (16, LANES), 1) // 8
        pick = jnp.where((slab == row) | (slab == row + 1), 1.0, 0.0)
        exact = dict(precision=lax.Precision.HIGHEST, preferred_element_type=jnp.float32)
        mean = lax.dot_general(pick, power, (((1,), (1,)), ((), ())), **exact)
        column = lax.broadcasted_iota(jnp.int32, (count, 32 * width), 1)
        column = column // 128 * 4 + column % 4
        spread = jnp.where(column == lax.broadcasted_iota(jnp.int32, (count, 32 * width), 0) // 2, 1.0, 0.0)
        mean = lax.dot_general(mean, spread, (((1,), (0,)), ((), ())), **exact)
        for c in range(width // 4):
            gain[c * 16 : c * 16 + 16, :] = 1.0 / (mean[:, c * 128 : c * 128 + 128] + EPS)

    def residues():
        def corner(s):
            at = s * PITCH + 4 if s < 16 else 6
            result = []
            for ref in (zr, zi):
                top = ref[pl.ds(at, 8, stride=2), :]
                low = ref[pl.ds(at + 1, 8, stride=2), :]
                top_left = pltpu.roll(top, LANES - 1, 1)
                low_left = pltpu.roll(low, LANES - 1, 1)
                top_under = jnp.where(in_slab < 7, top_left, pltpu.roll(low, 7, 1))
                low_under = jnp.where(in_slab < 7, low_left, jnp.where(lane < LANES - 1, top_left, 0.0))
                result.append((top, low, top_under, low_under))
            return [((result[0][g], result[1][g]), (result[0][2 + g], result[1][2 + g])) for g in range(2)]

        def cross(a, b):
            return a[1] * b[0] - a[0] * b[1]

        total = zero
        here = corner(0)
        down = [cross(*pair) for pair in here]
        for s in range(16):
            following = corner(s + 1)
            following_down = [cross(*pair) for pair in following]
            for g in range(2):
                across = cross(here[g][0], following[g][0]) - cross(here[g][1], following[g][1])
                loop = across + (following_down[g] - down[g])
                total = total + loop * loop
            here, down = following, following_down
        return total

    def windows(chunk, pair):
        hr, hi, lr, li, pr, pi, qr, qi = buffers[chunk % 2]
        data = []
        scale = []
        for a in (2 * pair, 2 * pair + 1):
            rows = slice(a * 16, a * 16 + 32)
            data.append(jnp.concatenate([hr[rows, :], hi[rows, :], hr[rows, :], hi[rows, :], lr[rows, :], li[rows, :]], axis=0))
            scale.append(jnp.broadcast_to(gain[chunk * 16 + a : chunk * 16 + a + 1, :], (32, LANES)))
        spectrum = jnp.dot(forward_ref[...], jnp.concatenate(data, axis=1), preferred_element_type=jnp.float32)
        re, im = spectrum[0:32], spectrum[32:64]
        factor = lax.rsqrt(lax.rsqrt((re * re + im * im) * jnp.concatenate(scale, axis=1)))
        high, low = split(jnp.concatenate([re * factor, im * factor], axis=0))
        back = jnp.dot(inverse_ref[...], jnp.concatenate([high, high, low], axis=0), preferred_element_type=jnp.float32)
        for k in range(2):
            at = (2 * pair + k) * 16
            part = back[:, k * LANES : (k + 1) * LANES]
            pr[at : at + 16, :], qr[at + 16 : at + 32, :] = part[0:16], part[16:32]
            pi[at : at + 16, :], qi[at + 16 : at + 32, :] = part[32:48], part[48:64]

    def inverse_columns(first, width, last, j):
        here = inside(first + 4 * j)
        both = here * inside(first + 4 * j + 1)
        values = []
        for l in range(32):
            at = pl.ds(j * 256 + l * 8, 8)
            values.append((wr[at, :], wi[at, :]))
        even = fft(values[0::2], 1)
        odd = join(fft(values[1::4], 1), fft(values[3::4], 1), 32, 1)
        for s in range(16):
            weight = here * (ramp(s) / 32)
            own = [v * weight for v in plus(even[s], odd[s])]
            weight = both * (ramp(s + 16) / 32)
            other = [v * weight for v in minus(even[s], odd[s])]
            for part, (ref, shift) in enumerate(((zr, shift_r), (zi, shift_i))):
                if last:
                    base = part * 304 + s * 19 + 8 * j
                    final[0][pl.ds(base, 8), :] = own[part]
                    final[1][pl.ds(base + 2, 8), :] = other[part]
                else:
                    shift[pl.ds(s * 32 + 8 * j + 2, 8), :] = other[part]
                    value = own[part] + shift[pl.ds(s * 32 + 8 * j, 8), :]
                    ref[pl.ds(s * PITCH + 2 * first + 8 * j, 8), :] = value

    for k in range(32):
        final[1][k * 19 : k * 19 + 2, :] = zero[0:2]

    def iteration(step, width, last):
        chunks = width // 4
        @block
        def _():
            for j in range(chunks):
                forward_columns(step, width, j)
            window_gains(12 - 2 * step, width)
            turn_in(0)
            final[2][pl.ds(step * 8, 8), :] = residues()

        for chunk in range(chunks):

            @block
            def _():
                if chunk + 1 < chunks:
                    turn_in(chunk + 1)
                for pair in range(8):
                    windows(chunk, pair)
                if chunk:
                    turn_out(chunk - 1)

        @block
        def _():
            turn_out(chunks - 1)
            for j in range(chunks):
                inverse_columns(step, width, last, j)

    run(ITERS - 1, lambda step: iteration(step, 12, False))
    iteration(ITERS - 1, 8, True)

    spill = []
    for part in range(2):
        for g in range(2):
            base = part * 304 + g
            rows = []
            for b in range(8):
                for s in (0, 8):
                    at = pl.ds(base + s * 19 + 2 * b, 8, stride=19)
                    rows.append(final[0][at, :] + final[1][at, :])
            turned = jnp.concatenate(rows, axis=0).T
            for a in range(16):
                at = a * OUT_ROWS + part * 16 + g * 8
                out_ref[at : at + 8, :] = turned[a * 8 : a * 8 + 8]
            spill += [final[1][pl.ds(base + s * 19 + 16, 8, stride=19), :] for s in (0, 8)]
    turned = jnp.concatenate(spill + spill, axis=0).T
    report = zero[0:1]
    for step in range(ITERS):
        total = jnp.sum(final[2][step * 8 : step * 8 + 8, :])
        report = jnp.where(lane[0:1] == step * 16 + tile, total, report)
    for a in range(16):
        value = turned[a * 8 : a * 8 + 8]
        out_ref[a * OUT_ROWS + 32 : a * OUT_ROWS + 36, :] = jnp.where(lane[0:4] < 64, value[0:4], value[4:8])
        out_ref[a * OUT_ROWS + 36 : a * OUT_ROWS + 37, :] = report


def filter_columns(data):
    def rows(count):
        return pltpu.VMEM((count, LANES), jnp.float32)

    return pl.pallas_call(
        column_kernel,
        out_shape=jax.ShapeDtypeStruct((16 * OUT_ROWS, LANES), jnp.float32),
        in_specs=[pl.BlockSpec(memory_space=pltpu.VMEM)] * 3,
        out_specs=pl.BlockSpec(memory_space=pltpu.VMEM),
        scratch_shapes=[rows(16 * PITCH)] * 2
        + [rows(776)] * 4
        + [rows(520)] * 2
        + [rows(80), rows(544)]
        + ([pltpu.VMEM((272, LANES), jnp.bfloat16)] * 4 + [rows(272)] * 4) * 2
        + [rows(624), rows(624), rows(ITERS * 8)],
        compiler_params=pltpu.CompilerParams(vmem_limit_bytes=16 << 20),
        name="filter_columns",
    )(data, *row_matrices())


def finish_kernel(scale, in_ref, field_ref, profile_ref):
    lane = lax.broadcasted_iota(jnp.int32, (8, LANES), 1)
    extras = []
    sums = jnp.zeros((1, LANES), jnp.float32)
    for c in range(16):
        half = in_ref[c * OUT_ROWS + 32 : c * OUT_ROWS + 36, :]
        extras.append(jnp.concatenate([half, pltpu.roll(half, 64, 1)], axis=0))
        sums = sums + in_ref[c * OUT_ROWS + 36 : c * OUT_ROWS + 37, :]
    for step in range(ITERS):
        profile_ref[step : step + 1, :] = sums[:, step * 16 : step * 16 + 16] * scale
    for part in range(2):
        for g in range(2):
            offset = (part * 2 + g) * 16
            for c in range(16):
                at = c * OUT_ROWS + part * 16 + g * 8
                value = in_ref[at : at + 8, :]
                if c:
                    spill = pltpu.roll(extras[c - 1], LANES - offset, 1) if offset else extras[c - 1]
                    value = value + jnp.where(lane < 16, spill, 0.0)
                field_ref[part, g * 8 : g * 8 + 8, c * LANES : (c + 1) * LANES] = value


def finish(scale, data):
    return pl.pallas_call(
        functools.partial(finish_kernel, scale),
        out_shape=(
            jax.ShapeDtypeStruct((2, 16, 16 * LANES), jnp.float32),
            jax.ShapeDtypeStruct((ITERS, 16), jnp.float32),
        ),
        in_specs=[pl.BlockSpec(memory_space=pltpu.VMEM)],
        out_specs=[pl.BlockSpec(memory_space=pltpu.VMEM)] * 2,
        compiler_params=pltpu.CompilerParams(vmem_limit_bytes=8 << 20),
        name="finish",
    )(data)


def ring_of_blocks(phase, devices, blocks, tiles):
    per_tile = LANES // devices
    ring = tiles * per_tile
    width = phase.shape[1]
    padded = jnp.pad(phase, ((0, 0), (HALO * 16, (ring + HALO) * 16)))
    pieces = []
    for d in range(devices):
        start = d * blocks * 16
        ahead = padded[:, start + HALO * 16 : start + (blocks + 2 * HALO) * 16]
        behind = padded[:, start : start + HALO * 16]
        gap = jnp.zeros((16, (ring - blocks - 2 * HALO) * 16), phase.dtype)
        pieces.append(jnp.concatenate([ahead, gap, behind], axis=1))
    return jnp.stack(pieces)


def per_device(phase):
    devices = lax.axis_size("rows")
    height, width = phase.shape
    blocks = width // (16 * devices)
    per_tile = LANES // devices
    if height != 16 or LANES % devices or blocks * 16 * devices != width or blocks != per_tile:
        raise ValueError("unsupported sizes")
    scale = 1.0 / (height * devices * 128.0)
    if devices == 16:
        data = lax.all_to_all(pack(phase).reshape(16, IN_ROWS, 1, LANES), "rows", 0, 0)
        result = filter_columns(data.reshape(16 * IN_ROWS, LANES))
        result = lax.all_to_all(result.reshape(16, OUT_ROWS, 1, LANES), "rows", 0, 0)
        result = result.reshape(16 * OUT_ROWS, LANES)
        return finish(scale, result)
    tiles = -(-(blocks + 2 * HALO) // per_tile)
    data = lax.all_to_all(ring_of_blocks(phase, devices, blocks, tiles), "rows", 0, 0)
    data = data.reshape(devices, 16, tiles, per_tile, 16).transpose(2, 4, 1, 3, 0)
    result = filter_tiles(devices, blocks, tiles, data.reshape(tiles, 16, 16, LANES))
    field = result[:32].reshape(2, 16, 16, per_tile, devices).transpose(4, 0, 2, 3, 1)
    field = field.reshape(devices, 32, per_tile * 16)
    sums = jnp.broadcast_to(result[32, :ITERS, : per_tile * 16][None], (devices, ITERS, per_tile * 16))
    result = lax.all_to_all(jnp.concatenate([field, sums], axis=1), "rows", 0, 0)
    field = result[:, :32].reshape(devices, 2, 16, per_tile * 16).transpose(1, 2, 0, 3).reshape(2, 16, width)
    profile = result[:, 32:, 0].reshape(width // 128, -1, ITERS).sum(1).T
    return field, profile * scale


def solution(mesh):
    return jax.shard_map(
        per_device,
        mesh=mesh,
        in_specs=(P(("groups", "rows"), None),),
        out_specs=(P(None, ("groups", "rows"), None), P("groups", None)),
        check_vma=False,
    )
```

```python
import functools
import math

import jax
import jax.numpy as jnp
import numpy as np
from jax import lax
from jax.experimental import pallas as pl
from jax.experimental.pallas import tpu as pltpu
from jax.sharding import PartitionSpec as P

ITERS = 3
EPS = 1e-06
LANES = 128
IN_ROWS = 26
OUT_ROWS = 37
PITCH = 41
HALO = 3

SIN = (9.99999996e-01, -1.66666580e-01, 8.33305053e-03, -1.98090400e-04, 2.60515161e-06)
COS = (9.99999953e-01, -4.99999050e-01, 4.16635780e-02, -1.38536600e-03, 2.31530144e-05)


def rotated(value, k, size, sign):
    re, im = value
    half = math.sqrt(0.5)
    if k == 0:
        return re, im
    if 4 * k == size:
        return (im, -re) if sign < 0 else (-im, re)
    if 8 * k == size:
        return ((re + im) * half, (im - re) * half) if sign < 0 else ((re - im) * half, (im + re) * half)
    if 8 * k == 3 * size:
        return ((im - re) * half, (re + im) * -half) if sign < 0 else ((re + im) * -half, (re - im) * half)
    if 2 * k > size:
        return rotated((-re, -im), k - size // 2, size, sign)
    c = math.cos(2 * math.pi * k / size)
    s = sign * math.sin(2 * math.pi * k / size)
    return re * c - im * s, im * c + re * s


def plus(a, b):
    return a[0] + b[0], a[1] + b[1]


def minus(a, b):
    return a[0] - b[0], a[1] - b[1]


def quarter_turn(a, sign):
    return (-a[1], a[0]) if sign > 0 else (a[1], -a[0])


def join(one, three, size, sign):
    quarter = size // 4
    one = [rotated(one[k], k, size, sign) for k in range(quarter)]
    three = [rotated(three[k], 3 * k, size, sign) for k in range(quarter)]
    turned = [quarter_turn(minus(a, b), sign) for a, b in zip(one, three)]
    return [plus(a, b) for a, b in zip(one, three)] + turned


def fft(values, sign):
    size = len(values)
    if size == 1:
        return values
    if size == 2:
        return [plus(*values), minus(*values)]
    even = fft(values[0::2], sign)
    odd = join(fft(values[1::4], sign), fft(values[3::4], sign), size, sign)
    return [plus(e, o) for e, o in zip(even, odd)] + [minus(e, o) for e, o in zip(even, odd)]


def odd_outputs(differences):
    one = []
    three = []
    for k in range(8):
        turned = quarter_turn(differences[k + 8], -1)
        one.append(rotated(plus(differences[k], turned), k, 32, -1))
        three.append(rotated(minus(differences[k], turned), 3 * k, 32, -1))
    pairs = zip(fft(one, -1), fft(three, -1))
    return [value for pair in pairs for value in pair]


def polynomial(coefficients, w):
    result = jnp.full_like(w, coefficients[-1])
    for c in coefficients[-2::-1]:
        result = result * w + c
    return result


def cos_sin(x):
    u = (jnp.abs(x) - jnp.float32(math.pi / 2)) + jnp.float32(4.371139e-08)
    w = u * u
    cosine = -(u * polynomial(SIN, w))
    sine = polynomial(COS, w)
    return cosine, jnp.where(x < 0, -sine, sine)


def ramp(t):
    return 1.0 - abs(t - 15.5) / 16.0


def filter_kernel(
    slabs, blocks, tiles, in_ref, out_ref, zr, zi, yr, yi, ur, ui, vr, vi, wr, wi, pr, pi, qr, qi, energy, gain, sums
):
    tile = lax.axis_index("rows")
    per_tile = LANES // slabs
    ring = tiles * per_tile
    lane = lax.broadcasted_iota(jnp.int32, (8, LANES), 1)
    sub = lax.broadcasted_iota(jnp.int32, (8, LANES), 0)
    not_last = lane % slabs != slabs - 1
    not_first = lane % slabs != 0
    place = lane // slabs

    def inside(h, step):
        position = (h * per_tile + place + step) % ring
        relative = jnp.where(position < blocks + HALO, position, position - ring)
        column = tile * blocks + relative
        return jnp.where((column >= 0) & (column < slabs * blocks), 1.0, 0.0)

    here = [inside(h, 0) for h in range(tiles)]
    both = [here[h] * inside(h, 1) for h in range(tiles)]

    def right(values, active):
        if per_tile == 1:
            return [values[(h + 1) % tiles] for h in active]
        moved = [pltpu.roll(v, LANES - slabs, 1) for v in values]
        return [jnp.where(lane < LANES - slabs, moved[h], moved[(h + 1) % tiles]) for h in active]

    def left(values):
        if per_tile == 1:
            return [values[h - 1] for h in range(tiles)]
        moved = [pltpu.roll(v, slabs, 1) for v in values]
        return [jnp.where(lane < slabs, moved[h - 1], moved[h]) for h in range(tiles)]

    def below(value):
        return jnp.where(not_last, pltpu.roll(value, LANES - 1, 1), 0.0)

    def above(value):
        return jnp.where(not_first, pltpu.roll(value, 1, 1), 0.0)

    def keep(h, s, g, value, power):
        for part, ref in enumerate((zr, zi)):
            ref[h * 16 + s, pl.ds(g * 8, 8), :] = value[part]
            if h == 0 or s == 0:
                ref[h * 16 + s, pl.ds(16 + g, 1), :] = below(value[part])[0:1]
        return power + (value[0] * value[0] + value[1] * value[1])

    for h in range(tiles):
        for g in range(2):
            phases = [in_ref[h, s, g * 8 : g * 8 + 8, :] for s in range(16)]
            power = jnp.zeros((8, LANES), jnp.float32)
            for s in range(16):
                cosine, sine = cos_sin(phases[s])
                power = keep(h, s, g, (cosine * here[h], sine * here[h]), power)
            energy[h * 16 + g * 8 : h * 16 + g * 8 + 8, :] = power

    def sharing(h, needed):
        places = {w % ring - h * per_tile for w in needed}
        places = {p for p in places if 0 <= p < per_tile}
        group = 1
        for k in (2, 4):
            if per_tile % k == 0:
                taken = {(p + j * (per_tile // k)) % per_tile for p in places for j in range(k)}
                group = k if len(taken) == k * len(places) else group
        masks = []
        for k in range(1, group):
            mask = place < 0
            for p in places:
                mask = mask | (place == (p + k * (per_tile // group)) % per_tile)
            masks.append(mask)
        return masks

    def merged(values, masks):
        result = values[0]
        for k, mask in enumerate(masks):
            result = jnp.where(mask, pltpu.roll(values[k + 1], (k + 1) * LANES // (len(masks) + 1), 1), result)
        return result

    def window_gains(plans):
        both_rows = [energy[h * 16 : h * 16 + 8, :] + energy[h * 16 + 8 : h * 16 + 16, :] for h in range(tiles)]
        blockwise = [jnp.broadcast_to(jnp.sum(e, axis=0, keepdims=True), (8, LANES)) for e in both_rows]
        tall = [e + below(e) for e in blockwise]
        for unit, ((h, masks, first, count), wide) in enumerate(zip(plans, right(tall, [p[0] for p in plans]))):
            value = merged([1.0 / ((tall[h] + wide) + EPS)] * 4, masks)
            for j in range(count):
                gain[(first + j) * 8 : (first + j) * 8 + 8, :] = value

    def forward_columns(step, plans, g):
        rows = pl.ds(pl.multiple_of(g * 8, 8), 8)
        under = pl.ds(g * 8 + 1, 8)
        active = [p[0] for p in plans]
        window_gains(plans)
        near = {h: [] for h in active}
        far = {h: [] for h in active}
        for s in range(16):
            re = [zr[h * 16 + s, rows, :] for h in range(tiles)]
            im = [zi[h * 16 + s, rows, :] for h in range(tiles)]
            for h, a, b in zip(active, right(re, active), right(im, active)):
                near[h].append((re[h], im[h]))
                far[h].append((a, b))
        for h, masks, first, count in plans:
            group = len(masks) + 1
            even = fft([plus(a, b) for a, b in zip(near[h], far[h])], -1)
            odd = fft([rotated(minus(a, b), s, 32, -1) for s, (a, b) in enumerate(zip(near[h], far[h]))], -1)
            for row in range(8 * count):
                sources = [(row // 8 * group + k) * 8 + row % 8 for k in range(group)]
                values = [(even, odd)[l % 2][l // 2] for l in sources]
                value = tuple(merged([v[part] for v in values], masks) for part in range(2))
                at = pl.ds((first * 8 + row) * 17 + g * 8, 8)
                if first == 0 and row < 8:
                    following = (below(value[0]), below(value[1]))
                    ur[at, :], ui[at, :] = plus(value, following)
                    vr[at, :], vi[at, :] = minus(value, following)
                else:
                    yr[at, :], yi[at, :] = value

        def corner(s):
            if s < 16:
                return near[0][s], (zr[s, under, :], zi[s, under, :])
            moved = [right([ref[h * 16, under, :] for h in range(tiles)], (0,))[0] for ref in (zr, zi)]
            return far[0][0], tuple(moved)

        def cross(a, b):
            return a[1] * b[0] - a[0] * b[1]

        total = jnp.zeros((8, LANES), jnp.float32)
        here_, under_ = corner(0)
        down = cross(here_, under_)
        for s in range(16):
            next_, next_under = corner(s + 1)
            next_down = cross(next_, next_under)
            loop = (cross(here_, next_) - cross(under_, next_under)) + (next_down - down)
            total = total + loop * loop
            here_, under_, down = next_, next_under, next_down
        sums[pl.ds(pl.multiple_of(step * 16 + g * 8, 8), 8), :] = total

    def split_rows(unit):
        for row in range(8):
            for g in range(2):
                source = pl.ds((unit * 8 + row) * 17 + g * 8, 8)
                at = pl.ds(row * 17 + g * 8, 8)
                value = (yr[source, :], yi[source, :])
                following = (below(value[0]), below(value[1]))
                ur[at, :], ui[at, :] = plus(value, following)
                vr[at, :], vi[at, :] = minus(value, following)

    def join_rows(unit):
        for t in range(16):
            source = pl.ds(t * 9, 8)
            at = pl.ds((unit * 16 + t) * 9, 8)
            wr[at, :] = pr[source, :] + above(qr[source, :])
            wi[at, :] = pi[source, :] + above(qi[source, :])

    def windows(unit):
        join_rows(jnp.maximum(unit - 1, 0))
        scale = gain[pl.ds(pl.multiple_of(unit * 8, 8), 8), :]
        at = [pl.ds(t, 8, stride=17) for t in range(16)]
        back = []
        for parity, (a, b) in enumerate(((ur, ui), (vr, vi))):
            values = [(a[x, :], b[x, :]) for x in at]
            if parity:
                values = [rotated(v, t, 32, -1) for t, v in enumerate(values)]
            filtered = []
            for re, im in fft(values, -1):
                factor = lax.rsqrt(lax.rsqrt((re * re + im * im) * scale))
                filtered.append((re * factor, im * factor))
            back.append(fft(filtered, 1))
        split_rows(unit + 1)
        for t in range(16):
            odd = rotated(back[1][t], t, 32, 1)
            upper = plus(back[0][t], odd)
            lower = minus(back[0][t], odd)
            at = pl.ds(t * 9, 8)
            pr[at, :], pi[at, :] = (v * (ramp(t) / 32) for v in upper)
            qr[at, :], qi[at, :] = (v * (ramp(t + 16) / 32) for v in lower)

    def inverse_columns(plans, units, g):
        rows = pl.ds(pl.multiple_of(g * 8, 8), 8)
        kept = []
        passed = []
        for h, masks, first, count in plans:
            group = len(masks) + 1
            values = [None] * 32
            for row in range(8 * count):
                unit = first + row // 8
                if unit == units - 1:
                    at = pl.ds(g * 72 + row % 8, 8, stride=9)
                    value = (pr[at, :] + above(qr[at, :]), pi[at, :] + above(qi[at, :]))
                else:
                    at = pl.ds(unit * 144 + g * 72 + row % 8, 8, stride=9)
                    value = (wr[at, :], wi[at, :])
                for k in range(group):
                    l = (row // 8 * group + k) * 8 + row % 8
                    values[l] = tuple(pltpu.roll(v, LANES - k * LANES // group, 1) if k else v for v in value)
            even = fft(values[0::2], 1)
            odd = fft(values[1::2], 1)
            own = []
            other = []
            for s in range(16):
                turned = rotated(odd[s], s, 32, 1)
                weight = here[h] * (ramp(s) / 32)
                own.append(tuple(v * weight for v in plus(even[s], turned)))
                weight = both[h] * (ramp(s + 16) / 32)
                other.append(tuple(v * weight for v in minus(even[s], turned)))
            kept.append(own)
            passed.append(other)
        power = [jnp.zeros((8, LANES), jnp.float32) for _ in range(tiles)]
        for s in range(16):
            arrived = [left([passed[h][s][part] for h in range(tiles)]) for part in range(2)]
            for h in range(tiles):
                value = tuple(kept[h][s][part] + arrived[part][h] for part in range(2))
                power[h] = keep(h, s, g, value, power[h])
        for h in range(tiles):
            energy[pl.ds(pl.multiple_of(h * 16 + g * 8, 8), 8), :] = power[h]

    def run(count, body):
        lax.fori_loop(0, count, lambda i, c: (body(i), c)[1], 0)

    for step in range(ITERS):
        needed = range(step - ITERS, blocks + ITERS - 1 - step)
        plans = []
        units = 0
        for h in range(tiles):
            masks = sharing(h, needed)
            plans.append((h, masks, units, 4 // (len(masks) + 1)))
            units += 4 // (len(masks) + 1)
        run(2, functools.partial(forward_columns, step, plans))
        run(units, windows)
        run(2, functools.partial(inverse_columns, plans, units))
    totals = [jnp.sum(sums[step * 16 : step * 16 + 8, :] + sums[step * 16 + 8 : step * 16 + 16, :]) for step in range(ITERS)]

    for step, total in enumerate(totals):
        out_ref[32, step : step + 1, :] = jnp.full((1, LANES), total)
    for part, ref in enumerate((zr, zi)):
        for s in range(16):
            out_ref[part * 16 + s, :, :] = ref[s, 0:16, :]


def filter_tiles(slabs, blocks, tiles, data):
    body = functools.partial(filter_kernel, slabs, blocks, tiles)
    return pl.pallas_call(
        body,
        out_shape=jax.ShapeDtypeStruct((33, 16, LANES), jnp.float32),
        in_specs=[pl.BlockSpec(memory_space=pltpu.VMEM)],
        out_specs=pl.BlockSpec(memory_space=pltpu.VMEM),
        scratch_shapes=[pltpu.VMEM((tiles * 16, 24, LANES), jnp.float32)] * 2
        + [pltpu.VMEM(((tiles * 4 + 1) * 136, LANES), jnp.float32)] * 2
        + [pltpu.VMEM((136, LANES), jnp.float32)] * 4
        + [pltpu.VMEM((tiles * 4 * 144, LANES), jnp.float32)] * 2
        + [pltpu.VMEM((144, LANES), jnp.float32)] * 4
        + [pltpu.VMEM((rows, LANES), jnp.float32) for rows in (tiles * 16, tiles * 32, ITERS * 16)],
        compiler_params=pltpu.CompilerParams(vmem_limit_bytes=16 << 20),
        name="filter_tiles",
    )(data)


def pack_kernel(in_ref, out_ref, turn):
    lane = lax.broadcasted_iota(jnp.int32, (8, LANES), 1)
    zero = jnp.zeros((8, LANES), jnp.float32)
    columns = [[in_ref[g * 8 : g * 8 + 8, c * LANES : (c + 1) * LANES] for g in range(2)] for c in range(16)]
    for c in range(16):
        after = columns[c + 1] if c < 15 else [zero, zero]
        before = columns[c - 1] if c else [zero, zero]
        at = c * IN_ROWS
        out_ref[at : at + 8, :] = columns[c][0]
        out_ref[at + 8 : at + 16, :] = columns[c][1]
        first = jnp.where(lane < 32, after[0], pltpu.roll(before[0], 64, 1))
        second = jnp.where(lane < 96, pltpu.roll(after[1], 64, 1), before[1])
        out_ref[at + 16 : at + 24, :] = jnp.where(lane < 64, first, second)
        turn[c * 8 : c * 8 + 8, :] = jnp.where(lane < 16, pltpu.roll(after[0], 96, 1), pltpu.roll(after[1], 112, 1))
    for q in range(4):
        rows = turn[pl.ds(q * 32, 8, stride=4), :]
        for u in range(1, 4):
            rows = jnp.where(lane // 32 == u, pltpu.roll(turn[pl.ds(q * 32 + u, 8, stride=4), :], 32 * u, 1), rows)
        for k in range(4):
            at = (q * 4 + k) * IN_ROWS + 24
            out_ref[at : at + 2, :] = rows[k * 2 : k * 2 + 2]


def pack(phase):
    return pl.pallas_call(
        pack_kernel,
        out_shape=jax.ShapeDtypeStruct((16 * IN_ROWS, LANES), jnp.float32),
        in_specs=[pl.BlockSpec(memory_space=pltpu.VMEM)],
        out_specs=pl.BlockSpec(memory_space=pltpu.VMEM),
        scratch_shapes=[pltpu.VMEM((128, LANES), jnp.float32)],
        compiler_params=pltpu.CompilerParams(vmem_limit_bytes=8 << 20),
        name="pack",
    )(phase)


def row_matrices():
    k = np.arange(32)
    angle = 2 * np.pi * (k[:, None] * k[None, :] % 32) / 32
    cos, sin = np.cos(angle), np.sin(angle)
    weight = np.array([ramp(t) / 32 for t in range(32)])[:, None]
    result = []
    for matrix in (np.block([[cos, sin], [-sin, cos]]), np.block([[cos * weight, -sin * weight], [sin * weight, cos * weight]])):
        whole = jnp.asarray(matrix, jnp.float32)
        high = whole.astype(jnp.bfloat16)
        low = (whole - high.astype(jnp.float32)).astype(jnp.bfloat16)
        result.append(jnp.concatenate([high, low, high], axis=1))
    return result


def column_kernel(in_ref, forward_ref, inverse_ref, out_ref, *scratch):
    zr, zi, yr, yi, wr, wi, shift_r, shift_i, gain, turn = scratch[:10]
    buffers = [scratch[10 + 8 * k : 18 + 8 * k] for k in range(2)]
    final = scratch[26:29]
    tile = lax.axis_index("rows")
    lane = lax.broadcasted_iota(jnp.int32, (8, LANES), 1)
    sub = lax.broadcasted_iota(jnp.int32, (8, LANES), 0)
    in_slab = lane & 7

    def inside(first):
        column = tile * 8 + (first - 2) + sub // 2
        return jnp.where((column >= 0) & (column < 128), 1.0, 0.0)

    def block(body):
        pl.when(tile >= 0)(body)

    def run(count, body):
        lax.fori_loop(0, count, lambda i, c: (body(i), c)[1], 0)

    zero = jnp.zeros((8, LANES), jnp.float32)
    for part in buffers:
        for ref in part[:4]:
            ref[256:272, :] = jnp.zeros((16, LANES), jnp.bfloat16)
        for ref in part[6:8]:
            ref[0:8, :] = zero
            ref[8:16, :] = zero

    def stacked(offset):
        return jnp.concatenate([in_ref[a * IN_ROWS + offset : a * IN_ROWS + offset + 8, :] for a in range(16)], axis=0)

    for k, offset in enumerate((0, 8, 16)):
        turned = stacked(offset).T
        for b in range(8):
            at = k * 136 + (b % 4 * 2 + b // 4 if k == 2 else b) * 17
            turn[at : at + 16, :] = turned[b * 16 : b * 16 + 16]
    tail = jnp.concatenate([in_ref[a * IN_ROWS + 24 : a * IN_ROWS + 26, :] for a in range(16)], axis=0)
    for q in range(4):
        for u in range(4):
            value = tail[q * 8 : q * 8 + 8]
            turn[pl.ds(408 + q * 32 + u, 8, stride=4), :] = pltpu.roll(value, LANES - 32 * u, 1) if u else value
    turned = turn[408:536, :].T[0:32]
    beyond = jnp.where(tile * 8 + 10 < 128, 1.0, 0.0)
    for ref, v in zip((zr, zi), cos_sin(turned)):
        for k in range(4):
            at = (k % 2) * 8 * PITCH + 24 + k // 2
            ref[pl.ds(at, 8, stride=PITCH), :] = v[k * 8 : k * 8 + 8] * beyond
    for g in range(2):
        for s in range(16):
            value = cos_sin(turn[pl.ds(g * 136 + s, 8, stride=17), :])
            for ref, v in zip((zr, zi), value):
                ref[pl.ds(s * PITCH + 4 + g, 8, stride=2), :] = v
    edge = tile * 8 + jnp.where(sub < 4, 8 + sub // 2, sub // 2 - 4)
    edge = jnp.where((edge >= 0) & (edge < 128), 1.0, 0.0)
    for s in range(16):
        value = cos_sin(turn[pl.ds(272 + s, 8, stride=17), :])
        for ref, v in zip((zr, zi), value):
            v = v * edge
            ref[s * PITCH + 20 : s * PITCH + 24, :] = v[0:4]
            ref[s * PITCH : s * PITCH + 4, :] = v[4:8]

    def forward_columns(first, width, j):
        near = []
        far = []
        power = zero
        for s in range(16):
            at = pl.ds(s * PITCH + 2 * first + j * 8, 8)
            after = pl.ds(s * PITCH + 2 * first + 2 + j * 8, 8)
            near.append((zr[at, :], zi[at, :]))
            far.append((zr[after, :], zi[after, :]))
            a, b = near[-1], far[-1]
            power = power + ((a[0] * a[0] + a[1] * a[1]) + (b[0] * b[0] + b[1] * b[1]))
        gain[pl.ds(pl.multiple_of(48 + j * 8, 8), 8), :] = power
        even = fft([plus(a, b) for a, b in zip(near, far)], -1)
        odd = odd_outputs([minus(a, b) for a, b in zip(near, far)])
        for l in range(32):
            to = pl.ds(j * 256 + l * 8, 8)
            yr[to, :], yi[to, :] = (even, odd)[l % 2][l // 2]

    def split(value):
        high = value.astype(jnp.bfloat16)
        return high, (value - high.astype(jnp.float32)).astype(jnp.bfloat16)

    def turn_in(chunk):
        for part, source in enumerate((yr, yi)):
            halves = []
            for g in range(2):
                parts = [source[pl.ds(chunk * 256 + i * 16 + g, 8, stride=2), :] for i in range(16)]
                halves.append(jnp.concatenate(parts, axis=0).T)
            high, low = buffers[chunk % 2][part], buffers[chunk % 2][2 + part]
            for a in range(16):
                value = jnp.concatenate([v[a * 8 : a * 8 + 8] for v in halves], axis=0)
                high[a * 16 : a * 16 + 16, :], low[a * 16 : a * 16 + 16, :] = split(value)

    def turn_out(chunk):
        pr, pi, qr, qi = buffers[chunk % 2][4:]
        for p, q, target in ((pr, qr, wr), (pi, qi, wi)):
            for g in range(2):
                parts = [p[a * 16 + g * 8 : a * 16 + g * 8 + 8, :] + q[a * 16 + g * 8 : a * 16 + g * 8 + 8, :] for a in range(16)]
                turned = jnp.concatenate(parts, axis=0).T
                for i in range(16):
                    target[pl.ds(chunk * 256 + i * 16 + g, 8, stride=2), :] = turned[i * 8 : i * 8 + 8]

    def window_gains(valid, width):
        count = 2 * width
        power = jnp.concatenate(
            [jnp.where(sub < 2 * valid - 8 * j, gain[48 + j * 8 : 56 + j * 8, :], 0.0) for j in range(count // 8)], axis=0
        )
        row = lax.broadcasted_iota(jnp.int32, (16, LANES), 0)
        slab = lax.broadcasted_iota(jnp.int32, (16, LANES), 1) // 8
        pick = jnp.where((slab == row) | (slab == row + 1), 1.0, 0.0)
        exact = dict(precision=lax.Precision.HIGHEST, preferred_element_type=jnp.float32)
        mean = lax.dot_general(pick, power, (((1,), (1,)), ((), ())), **exact)
        column = lax.broadcasted_iota(jnp.int32, (count, 32 * width), 1)
        column = column // 128 * 4 + column % 4
        spread = jnp.where(column == lax.broadcasted_iota(jnp.int32, (count, 32 * width), 0) // 2, 1.0, 0.0)
        mean = lax.dot_general(mean, spread, (((1,), (0,)), ((), ())), **exact)
        for c in range(width // 4):
            gain[c * 16 : c * 16 + 16, :] = 1.0 / (mean[:, c * 128 : c * 128 + 128] + EPS)

    def residues():
        def corner(s):
            at = s * PITCH + 4 if s < 16 else 6
            result = []
            for ref in (zr, zi):
                top = ref[pl.ds(at, 8, stride=2), :]
                low = ref[pl.ds(at + 1, 8, stride=2), :]
                top_left = pltpu.roll(top, LANES - 1, 1)
                low_left = pltpu.roll(low, LANES - 1, 1)
                top_under = jnp.where(in_slab < 7, top_left, pltpu.roll(low, 7, 1))
                low_under = jnp.where(in_slab < 7, low_left, jnp.where(lane < LANES - 1, top_left, 0.0))
                result.append((top, low, top_under, low_under))
            return [((result[0][g], result[1][g]), (result[0][2 + g], result[1][2 + g])) for g in range(2)]

        def cross(a, b):
            return a[1] * b[0] - a[0] * b[1]

        total = zero
        here = corner(0)
        down = [cross(*pair) for pair in here]
        for s in range(16):
            following = corner(s + 1)
            following_down = [cross(*pair) for pair in following]
            for g in range(2):
                across = cross(here[g][0], following[g][0]) - cross(here[g][1], following[g][1])
                loop = across + (following_down[g] - down[g])
                total = total + loop * loop
            here, down = following, following_down
        return total

    def windows(chunk, pair):
        hr, hi, lr, li, pr, pi, qr, qi = buffers[chunk % 2]
        data = []
        scale = []
        for a in (2 * pair, 2 * pair + 1):
            rows = slice(a * 16, a * 16 + 32)
            data.append(jnp.concatenate([hr[rows, :], hi[rows, :], hr[rows, :], hi[rows, :], lr[rows, :], li[rows, :]], axis=0))
            scale.append(jnp.broadcast_to(gain[chunk * 16 + a : chunk * 16 + a + 1, :], (32, LANES)))
        spectrum = jnp.dot(forward_ref[...], jnp.concatenate(data, axis=1), preferred_element_type=jnp.float32)
        re, im = spectrum[0:32], spectrum[32:64]
        factor = lax.rsqrt(lax.rsqrt((re * re + im * im) * jnp.concatenate(scale, axis=1)))
        high, low = split(jnp.concatenate([re * factor, im * factor], axis=0))
        back = jnp.dot(inverse_ref[...], jnp.concatenate([high, high, low], axis=0), preferred_element_type=jnp.float32)
        for k in range(2):
            at = (2 * pair + k) * 16
            part = back[:, k * LANES : (k + 1) * LANES]
            pr[at : at + 16, :], qr[at + 16 : at + 32, :] = part[0:16], part[16:32]
            pi[at : at + 16, :], qi[at + 16 : at + 32, :] = part[32:48], part[48:64]

    def inverse_columns(first, width, last, j):
        here = inside(first + 4 * j)
        both = here * inside(first + 4 * j + 1)
        values = []
        for l in range(32):
            at = pl.ds(j * 256 + l * 8, 8)
            values.append((wr[at, :], wi[at, :]))
        even = fft(values[0::2], 1)
        odd = join(fft(values[1::4], 1), fft(values[3::4], 1), 32, 1)
        for s in range(16):
            weight = here * (ramp(s) / 32)
            own = [v * weight for v in plus(even[s], odd[s])]
            weight = both * (ramp(s + 16) / 32)
            other = [v * weight for v in minus(even[s], odd[s])]
            for part, (ref, shift) in enumerate(((zr, shift_r), (zi, shift_i))):
                if last:
                    base = part * 304 + s * 19 + 8 * j
                    final[0][pl.ds(base, 8), :] = own[part]
                    final[1][pl.ds(base + 2, 8), :] = other[part]
                else:
                    shift[pl.ds(s * 32 + 8 * j + 2, 8), :] = other[part]
                    value = own[part] + shift[pl.ds(s * 32 + 8 * j, 8), :]
                    ref[pl.ds(s * PITCH + 2 * first + 8 * j, 8), :] = value

    for k in range(32):
        final[1][k * 19 : k * 19 + 2, :] = zero[0:2]

    def iteration(step, width, last):
        chunks = width // 4
        @block
        def _():
            for j in range(chunks):
                forward_columns(step, width, j)
            window_gains(12 - 2 * step, width)
            turn_in(0)
            final[2][pl.ds(step * 8, 8), :] = residues()

        for chunk in range(chunks):

            @block
            def _():
                if chunk + 1 < chunks:
                    turn_in(chunk + 1)
                for pair in range(8):
                    windows(chunk, pair)
                if chunk:
                    turn_out(chunk - 1)

        @block
        def _():
            turn_out(chunks - 1)
            for j in range(chunks):
                inverse_columns(step, width, last, j)

    run(ITERS - 1, lambda step: iteration(step, 12, False))
    iteration(ITERS - 1, 8, True)

    spill = []
    for part in range(2):
        for g in range(2):
            base = part * 304 + g
            rows = []
            for b in range(8):
                for s in (0, 8):
                    at = pl.ds(base + s * 19 + 2 * b, 8, stride=19)
                    rows.append(final[0][at, :] + final[1][at, :])
            turned = jnp.concatenate(rows, axis=0).T
            for a in range(16):
                at = a * OUT_ROWS + part * 16 + g * 8
                out_ref[at : at + 8, :] = turned[a * 8 : a * 8 + 8]
            spill += [final[1][pl.ds(base + s * 19 + 16, 8, stride=19), :] for s in (0, 8)]
    turned = jnp.concatenate(spill + spill, axis=0).T
    report = zero[0:1]
    for step in range(ITERS):
        total = jnp.sum(final[2][step * 8 : step * 8 + 8, :])
        report = jnp.where(lane[0:1] == step * 16 + tile, total, report)
    for a in range(16):
        value = turned[a * 8 : a * 8 + 8]
        out_ref[a * OUT_ROWS + 32 : a * OUT_ROWS + 36, :] = jnp.where(lane[0:4] < 64, value[0:4], value[4:8])
        out_ref[a * OUT_ROWS + 36 : a * OUT_ROWS + 37, :] = report


def filter_columns(data):
    def rows(count):
        return pltpu.VMEM((count, LANES), jnp.float32)

    return pl.pallas_call(
        column_kernel,
        out_shape=jax.ShapeDtypeStruct((16 * OUT_ROWS, LANES), jnp.float32),
        in_specs=[pl.BlockSpec(memory_space=pltpu.VMEM)] * 3,
        out_specs=pl.BlockSpec(memory_space=pltpu.VMEM),
        scratch_shapes=[rows(16 * PITCH)] * 2
        + [rows(776)] * 4
        + [rows(520)] * 2
        + [rows(80), rows(544)]
        + ([pltpu.VMEM((272, LANES), jnp.bfloat16)] * 4 + [rows(272)] * 4) * 2
        + [rows(624), rows(624), rows(ITERS * 8)],
        compiler_params=pltpu.CompilerParams(vmem_limit_bytes=16 << 20),
        name="filter_columns",
    )(data, *row_matrices())


def finish_kernel(scale, in_ref, field_ref, profile_hbm, rows, profile_ref, sent):
    lane = lax.broadcasted_iota(jnp.int32, (8, LANES), 1)
    extras = []
    sums = jnp.zeros((1, LANES), jnp.float32)
    for c in range(16):
        half = in_ref[c * OUT_ROWS + 32 : c * OUT_ROWS + 36, :]
        extras.append(jnp.concatenate([half, pltpu.roll(half, 64, 1)], axis=0))
        sums = sums + in_ref[c * OUT_ROWS + 36 : c * OUT_ROWS + 37, :]
    for step in range(ITERS):
        profile_ref[step : step + 1, :] = sums[:, step * 16 : step * 16 + 16] * scale
    copies = [pltpu.make_async_copy(profile_ref, profile_hbm, sent.at[4])]
    copies[0].start()
    for k in range(4):
        part, g = k // 2, k % 2
        for c in range(16):
            value = in_ref[c * OUT_ROWS + k * 8 : c * OUT_ROWS + k * 8 + 8, :]
            if c:
                spill = pltpu.roll(extras[c - 1], LANES - k * 16, 1) if k else extras[c - 1]
                value = value + jnp.where(lane < 16, spill, 0.0)
            rows[k, :, c * LANES : (c + 1) * LANES] = value
        copies.append(pltpu.make_async_copy(rows.at[k], field_ref.at[part, pl.ds(g * 8, 8)], sent.at[k]))
        copies[-1].start()
    for copy in copies:
        copy.wait()


def finish(scale, data):
    return pl.pallas_call(
        functools.partial(finish_kernel, scale),
        out_shape=(
            jax.ShapeDtypeStruct((2, 16, 16 * LANES), jnp.float32),
            jax.ShapeDtypeStruct((ITERS, 16), jnp.float32),
        ),
        in_specs=[pl.BlockSpec(memory_space=pltpu.VMEM)],
        out_specs=[pl.BlockSpec(memory_space=pl.ANY)] * 2,
        scratch_shapes=[pltpu.VMEM((4, 8, 16 * LANES), jnp.float32), pltpu.VMEM((ITERS, 16), jnp.float32), pltpu.SemaphoreType.DMA((5,))],
        compiler_params=pltpu.CompilerParams(vmem_limit_bytes=8 << 20),
        name="finish",
    )(data)


def ring_of_blocks(phase, devices, blocks, tiles):
    per_tile = LANES // devices
    ring = tiles * per_tile
    width = phase.shape[1]
    padded = jnp.pad(phase, ((0, 0), (HALO * 16, (ring + HALO) * 16)))
    pieces = []
    for d in range(devices):
        start = d * blocks * 16
        ahead = padded[:, start + HALO * 16 : start + (blocks + 2 * HALO) * 16]
        behind = padded[:, start : start + HALO * 16]
        gap = jnp.zeros((16, (ring - blocks - 2 * HALO) * 16), phase.dtype)
        pieces.append(jnp.concatenate([ahead, gap, behind], axis=1))
    return jnp.stack(pieces)


def per_device(phase):
    devices = lax.axis_size("rows")
    height, width = phase.shape
    blocks = width // (16 * devices)
    per_tile = LANES // devices
    if height != 16 or LANES % devices or blocks * 16 * devices != width or blocks != per_tile:
        raise ValueError("unsupported sizes")
    scale = 1.0 / (height * devices * 128.0)
    if devices == 16:
        data = lax.all_to_all(pack(phase).reshape(16, IN_ROWS, 1, LANES), "rows", 0, 0)
        result = filter_columns(data.reshape(16 * IN_ROWS, LANES))
        result = lax.all_to_all(result.reshape(16, OUT_ROWS, 1, LANES), "rows", 0, 0)
        result = result.reshape(16 * OUT_ROWS, LANES)
        return finish(scale, result)
    tiles = -(-(blocks + 2 * HALO) // per_tile)
    data = lax.all_to_all(ring_of_blocks(phase, devices, blocks, tiles), "rows", 0, 0)
    data = data.reshape(devices, 16, tiles, per_tile, 16).transpose(2, 4, 1, 3, 0)
    result = filter_tiles(devices, blocks, tiles, data.reshape(tiles, 16, 16, LANES))
    field = result[:32].reshape(2, 16, 16, per_tile, devices).transpose(4, 0, 2, 3, 1)
    field = field.reshape(devices, 32, per_tile * 16)
    sums = jnp.broadcast_to(result[32, :ITERS, : per_tile * 16][None], (devices, ITERS, per_tile * 16))
    result = lax.all_to_all(jnp.concatenate([field, sums], axis=1), "rows", 0, 0)
    field = result[:, :32].reshape(devices, 2, 16, per_tile * 16).transpose(1, 2, 0, 3).reshape(2, 16, width)
    profile = result[:, 32:, 0].reshape(width // 128, -1, ITERS).sum(1).T
    return field, profile * scale


def solution(mesh):
    return jax.shard_map(
        per_device,
        mesh=mesh,
        in_specs=(P(("groups", "rows"), None),),
        out_specs=(P(None, ("groups", "rows"), None), P("groups", None)),
        check_vma=False,
    )
```
